32 devices in a mesh: dp: 16 (over z, x, core), tile: 2 (over y).
Axes of the slice: x: 2, y: 2, z: 4, core: 2. Of those that a mesh axis runs over, the one named last changes fastest.
Arguments:
- proposal_boxes: int32 [16, 4, 512], P('dp'), may hold values from 0 to 672, as said below
- level_plan: int32 [16, 512], P('dp'), may hold values from 0 to 1
- fine_map: bfloat16 [16, 84, 168, 128], P('dp', 'tile'), may hold values from -6 to 6
- coarse_map: bfloat16 [16, 42, 84, 128], P('dp', 'tile'), may hold values from -6 to 6
- first_weight: bfloat16 [6272, 1024], P('tile', 'dp'), may hold values from -0.078125 to 0.078125
- second_weight: bfloat16 [1024, 1024], P('tile', 'dp'), may hold values from -0.1875 to 0.1875
- upstream: bfloat16 [16, 512, 1024], P('dp'), may hold values from -6 to 6
Outputs:
- first_grad: float32 [6272, 1024], P('tile', 'dp')
- second_grad: float32 [1024, 1024], P('tile', 'dp')
The draws below stay inside these ranges and needn't reach their ends.
Inputs may be any that keep to these rules, and one draw needn't show every extreme that they name: `proposal_boxes`: with s = 4 where level_plan is 0 and s = 8 where it is 1: h >= 1, w >= 1, y0 + h <= 336, x0 + w <= 672, (y0 mod s) + h <= 14 * s and (x0 mod s) + w <= 14 * s. Band b holds the proposals with b * 168 <= y0 < (b + 1) * 168; at most 256 of an image's proposals lie in one band, and in every image some band holds exactly 256.
All inputs are finite; a program needn't handle non-finite values.
Results may differ from the reference program's by a relative error of at most 0.017.
Values may be sent and summed in bfloat16 or wider, within the bound.
A program may use at most 64 MiB of HBM per device.

```python
import jax
import jax.numpy as jnp
from jax import lax

CH = 128
HIDDEN_SIZE = 1024
FEATS = 6272
WIN = 16
ROWS2 = 42
COLS2 = 168
ROWS3 = 21
COLS3 = 84
PROPS = 512
CAP = 256
IMAGES = 16
BAND_PX = 168
HEIGHT_PX = 336
WIDTH_PX = 672
N_TILE = 2


def proposal_plan(key):
    base_key = jax.random.fold_in(key, 11)
    key_level, key_busy, key_order, key_top, key_height, key_left, key_width = jax.random.split(base_key, 7)
    grid_shape = (IMAGES, PROPS)
    level_draw = jax.random.randint(key_level, grid_shape, 0, 2)
    busy_band = jax.random.randint(key_busy, (IMAGES, 1), 0, N_TILE)
    slot_index = jnp.arange(PROPS)[None, :]
    other_bands = max(N_TILE - 1, 1)
    spread_band = (busy_band + 1 + jnp.maximum(slot_index - CAP, 0) % other_bands) % N_TILE
    listed_band = jnp.where(slot_index < CAP, busy_band, spread_band)
    shuffles = jax.vmap(lambda order_key: jax.random.permutation(order_key, PROPS))(jax.random.split(key_order, IMAGES))
    owner_band = jnp.take_along_axis(listed_band, shuffles, axis=1)
    stride = jnp.where(level_draw == 0, 4, 8)
    top_pixel = owner_band * BAND_PX + jax.random.randint(key_top, grid_shape, 0, BAND_PX)
    height_most = jnp.minimum(14 * stride - top_pixel % stride, HEIGHT_PX - top_pixel)
    height_draw = jax.random.randint(key_height, grid_shape, jnp.minimum(stride, height_most), height_most + 1)
    left_pixel = jax.random.randint(key_left, grid_shape, 0, WIDTH_PX)
    width_most = jnp.minimum(14 * stride - left_pixel % stride, WIDTH_PX - left_pixel)
    width_draw = jax.random.randint(key_width, grid_shape, jnp.minimum(stride, width_most), width_most + 1)
    box_array = jnp.stack([top_pixel, left_pixel, height_draw, width_draw], axis=1).astype(jnp.int32)
    return (box_array, level_draw.astype(jnp.int32))


def draw_proposal_boxes(key, part):
    return proposal_plan(key)[0]


def draw_level_plan(key, part):
    return proposal_plan(key)[1]


def block_scale(stream_key, shape, shards, low, high):
    gain, own = 1.0, jax.random.fold_in(stream_key, 6)
    for axis_at, shards_of in shards:
        draws = jnp.exp(jax.random.uniform(jax.random.fold_in(own, axis_at), (shards_of,), jnp.float32, low / len(shards), high / len(shards)))
        gain = gain * jnp.repeat(draws, shape[axis_at] // shards_of).reshape([-1 if axis == axis_at else 1 for axis in range(len(shape))])
    return gain


def gaussian(own_key, dims, scale, limit, cuts=(), held_as=jnp.bfloat16):
    entries = jax.random.normal(own_key, dims, jnp.float32) * scale
    if len(cuts) > 0:
        entries = block_scale(own_key, dims, cuts, -0.22, 0.18) * entries
    return jnp.clip(entries, min=-limit, max=limit).astype(held_as)


def setup_inputs(seed: int = 0) -> dict:
    key_of = jax.random.split(jax.random.key(seed), 8)
    proposal_boxes = draw_proposal_boxes(jax.random.fold_in(key_of[7], 71), 0)
    level_plan = draw_level_plan(jax.random.fold_in(key_of[7], 71), 0)
    fine_map = gaussian(key_of[2], (IMAGES, ROWS2 * N_TILE, COLS2, CH), 1.0, 6.0, ((0, 16), (1, 2)))
    coarse_map = gaussian(key_of[3], (IMAGES, ROWS3 * N_TILE, COLS3, CH), 1.0, 6.0, ((0, 16), (1, 2)))
    first_weight = gaussian(key_of[4], (FEATS, HIDDEN_SIZE), FEATS ** -0.5, 0.078125, ((0, 2), (1, 16)))
    second_weight = gaussian(key_of[5], (HIDDEN_SIZE, HIDDEN_SIZE), HIDDEN_SIZE ** -0.5, 0.1875, ((0, 2), (1, 16)))
    upstream = gaussian(key_of[6], (IMAGES, PROPS, HIDDEN_SIZE), 1.0, 6.0, ((0, 16),))
    return {"proposal_boxes": proposal_boxes, "level_plan": level_plan, "fine_map": fine_map, "coarse_map": coarse_map, "first_weight": first_weight, "second_weight": second_weight, "upstream": upstream}


def gelu_parts(hidden):
    factor = 0.7978845608028654
    cubic_term = 0.044715
    inner_term = factor * (hidden + cubic_term * hidden * hidden * hidden)
    tangent = jnp.tanh(inner_term)
    gelu_value = 0.5 * hidden * (1.0 + tangent)
    gelu_slope = 0.5 * (1.0 + tangent) + 0.5 * hidden * (1.0 - tangent * tangent) * factor * (1.0 + 3.0 * cubic_term * hidden * hidden)
    return gelu_value, gelu_slope


def block_size(num_items):
    return 32 if num_items % 32 == 0 else num_items


def axis_weights(begin_px, extent, first_cell, stride):
    stride_float = stride.astype(jnp.float32)[:, None]
    bin_index = jnp.arange(7, dtype=jnp.float32)[None, :]
    sample_pos = begin_px.astype(jnp.float32)[:, None] / stride_float + (bin_index + 0.5) * extent.astype(jnp.float32)[:, None] / (7.0 * stride_float)
    cell_pos = first_cell.astype(jnp.float32)[:, None, None] + jnp.arange(WIN, dtype=jnp.float32)[None, None, :]
    return jnp.maximum(0.0, 1.0 - jnp.abs(sample_pos[:, :, None] - cell_pos))


def crop_block(combined, fields, levels_blk, shift_fine, shift_coarse, limit_fine, limit_coarse, offset):
    top_pixel = fields[0]
    left_pixel = fields[1]
    height = fields[2]
    box_width = fields[3]
    stride = jnp.where(levels_blk == 0, 4, 8).astype(jnp.int32)
    first_row = (top_pixel // stride).astype(jnp.int32)
    first_col = jnp.minimum(left_pixel // stride, jnp.where(levels_blk == 0, limit_fine, limit_coarse) - WIN).astype(jnp.int32)
    start_row = jnp.where(levels_blk == 0, first_row - shift_fine, offset + first_row - shift_coarse).astype(jnp.int32)
    channels = combined.shape[2]
    zero_index = jnp.zeros((), jnp.int32)

    def window(row_start, col_start):
        return lax.dynamic_slice(combined, (row_start.astype(jnp.int32), col_start.astype(jnp.int32), zero_index), (WIN, WIN, channels))

    windows = jax.vmap(window)(start_row, first_col).astype(jnp.float32)
    row_low = lax.optimization_barrier(axis_weights(top_pixel, height, first_row, stride).astype(jnp.bfloat16))
    col_low = lax.optimization_barrier(axis_weights(left_pixel, box_width, first_col, stride).astype(jnp.bfloat16))
    row_weights = row_low.astype(jnp.float32)
    col_weights = col_low.astype(jnp.float32)
    partial_rows = jnp.einsum("bia,baqc->biqc", row_weights, windows, precision=lax.Precision.HIGHEST)
    crop_rows = jnp.einsum("bjq,biqc->bijc", col_weights, partial_rows, precision=lax.Precision.HIGHEST)
    return crop_rows.reshape(crop_rows.shape[0], 49 * channels).astype(jnp.bfloat16)


def image_crops(inputs):
    fields, levels_img, fine_tile, coarse = inputs
    fine_rows, fine_cols, channels = fine_tile.shape
    coarse_cols = coarse.shape[1]
    fine_pad = jnp.pad(fine_tile, ((0, WIN), (0, WIN), (0, 0)))
    coarse_pad = jnp.pad(coarse, ((0, WIN), (0, fine_cols + WIN - coarse_cols), (0, 0)))
    combined = jnp.concatenate([fine_pad, coarse_pad], axis=0)
    num_props = levels_img.shape[0]
    block_len = block_size(num_props)
    grouped_fields = fields.reshape(4, num_props // block_len, block_len).transpose(1, 0, 2)
    grouped_levels = levels_img.reshape(num_props // block_len, block_len)

    def crop_group(pieces):
        part_fields, part_levels = pieces
        return crop_block(combined, part_fields, part_levels, 0, 0, fine_cols + WIN, coarse_cols + WIN, fine_rows + WIN)

    grouped = lax.map(crop_group, (grouped_fields, grouped_levels))
    return grouped.reshape(num_props, 49 * channels)


def reference(proposal_boxes, level_plan, fine_map, coarse_map, first_weight, second_weight, upstream):
    crop_all = lax.map(image_crops, (proposal_boxes, level_plan, fine_map, coarse_map))
    flat_crops = crop_all.reshape(-1, crop_all.shape[2])
    upstream_rows = upstream.reshape(-1, upstream.shape[2])
    hidden = jnp.dot(flat_crops, first_weight, preferred_element_type=jnp.float32)
    gelu_value, gelu_slope = gelu_parts(hidden)
    activated = gelu_value.astype(jnp.bfloat16)
    second_grad = jnp.dot(activated.T, upstream_rows, preferred_element_type=jnp.float32)
    back_grad = jnp.dot(upstream_rows, second_weight.T, preferred_element_type=jnp.float32)
    pre_grad = (back_grad * gelu_slope).astype(jnp.bfloat16)
    first_grad = jnp.dot(flat_crops.T, pre_grad, preferred_element_type=jnp.float32)
    return first_grad, second_grad
```

```python
import functools

import jax
import jax.numpy as jnp
from jax import lax
from jax.experimental import pallas as pl
from jax.experimental.pallas import tpu as pltpu
from jax.sharding import PartitionSpec as P

WIN = 16
BINS = 7
ROWS_PAD = 56
GROUP = 16


def from_ahead(block, axis, distance):
    if distance == 0:
        return block
    size = lax.axis_size(axis)
    return lax.ppermute(block, axis, [(i, (i - distance) % size) for i in range(size)])


def halo_from_next(block, axis):
    size = lax.axis_size(axis)
    return lax.ppermute(block, axis, [(i + 1, i) for i in range(size - 1)])


def gelu_parts(hidden):
    factor = 0.7978845608028654
    cubic_term = 0.044715
    inner_term = factor * (hidden + cubic_term * hidden * hidden * hidden)
    tangent = jnp.tanh(inner_term)
    gelu_value = 0.5 * hidden * (1.0 + tangent)
    gelu_slope = 0.5 * (1.0 + tangent) + 0.5 * hidden * (1.0 - tangent * tangent) * factor * (
        1.0 + 3.0 * cubic_term * hidden * hidden
    )
    return (gelu_value, gelu_slope)


def crop_kernel(starts, width, cells_ref, geo_ref, maps_ref, out_ref, wide, stage):
    step = pl.program_id(0)

    @pl.when(step == 0)
    def _():
        def widen(r, carry):
            wide[r] = maps_ref[r].astype(jnp.float32)
            return carry

        lax.fori_loop(0, maps_ref.shape[0], widen, 0)

    shape = (ROWS_PAD, WIN * WIN)
    k = lax.broadcasted_iota(jnp.int32, shape, 0).astype(jnp.float32)
    i_bin = jnp.floor((k + 0.5) * (1.0 / BINS))
    j_bin = k - BINS * i_bin
    i_mid = i_bin + 0.5
    j_mid = j_bin + 0.5
    lane = lax.broadcasted_iota(jnp.int32, shape, 1)
    r_cell = (lane >> 4).astype(jnp.float32)
    q_cell = (lane & 15).astype(jnp.float32)
    for p in range(GROUP):
        n = step * GROUP + p
        row = cells_ref[0, n]
        col = cells_ref[1, n]
        row_w = jnp.maximum(0.0, 1.0 - jnp.abs(i_mid * geo_ref[1, n] + geo_ref[0, n] - r_cell))
        col_w = jnp.maximum(0.0, 1.0 - jnp.abs(j_mid * geo_ref[3, n] + geo_ref[2, n] - q_cell))
        weights = (row_w * col_w).astype(jnp.bfloat16)
        window = jnp.concatenate(
            [wide[row + r, pl.ds(col, WIN), :] for r in range(WIN)], axis=0
        ).astype(jnp.bfloat16)
        crop = jnp.dot(weights, window, preferred_element_type=jnp.float32)
        stage[pl.ds(p, ROWS_PAD, stride=GROUP), :] = crop
    for t, first in enumerate(starts):
        for m in range(width):
            at = (first + m) * GROUP
            out_ref[t, :, m * 128 : (m + 1) * 128] = stage[at : at + GROUP, :].astype(jnp.bfloat16)


def make_crops(cells, geo, maps, starts, width, capacity):
    tiles = len(starts)
    lanes = width * 128
    return pl.pallas_call(
        functools.partial(crop_kernel, starts, width),
        grid=(capacity // GROUP,),
        out_shape=jax.ShapeDtypeStruct((tiles, capacity, lanes), jnp.bfloat16),
        in_specs=[
            pl.BlockSpec(memory_space=pltpu.SMEM),
            pl.BlockSpec(memory_space=pltpu.SMEM),
            pl.BlockSpec(maps.shape, lambda g: (0, 0, 0)),
        ],
        out_specs=pl.BlockSpec((tiles, GROUP, lanes), lambda g: (0, g, 0)),
        scratch_shapes=[
            pltpu.VMEM(maps.shape, jnp.float32),
            pltpu.VMEM((ROWS_PAD * GROUP, 128), jnp.float32),
        ],
        compiler_params=pltpu.CompilerParams(
            dimension_semantics=("arbitrary",), vmem_limit_bytes=48 * 1024 * 1024
        ),
        cost_estimate=pl.CostEstimate(
            flops=capacity * ROWS_PAD * WIN * WIN * 128 * 16,
            bytes_accessed=2 * maps.size + 2 * tiles * capacity * lanes,
            transcendentals=0,
        ),
        name="crops",
    )(cells, geo, maps)


def per_device_by_bands(
    proposal_boxes, level_plan, fine_map, coarse_map, first_weight, second_weight, upstream
):
    tile_count = lax.axis_size("tile")
    band = lax.axis_index("tile")
    num_props = level_plan.shape[1]
    capacity = max(num_props // 4, num_props // tile_count)
    fine_tile = fine_map[0]
    coarse = coarse_map[0]
    fine_rows, fine_cols, channels = fine_tile.shape
    coarse_rows, coarse_cols = (coarse.shape[0], coarse.shape[1])

    top_rows = jnp.concatenate([fine_tile[:WIN], coarse[:WIN]], axis=1)
    below_rows = halo_from_next(top_rows, "tile")

    share_feats = first_weight.shape[0]
    feats = share_feats * tile_count
    width = max(
        -(-((t + 1) * share_feats) // 128) - t * share_feats // 128 for t in range(tile_count)
    )
    starts = [min(t * share_feats // 128, feats // 128 - width) for t in range(tile_count)]
    lanes = width * 128
    feat_off = band * share_feats - 128 * jnp.minimum(
        band * share_feats // 128, feats // 128 - width
    )

    first_rows = lax.dynamic_update_slice(
        jnp.zeros((first_weight.shape[1], lanes), jnp.bfloat16),
        first_weight.T,
        (0, feat_off),
    )
    both = lax.all_gather(
        jnp.concatenate([first_rows, second_weight.T], axis=1), "dp", axis=0, tiled=True
    )
    first_all = both[:, :lanes]
    second_all = both[:, lanes:]

    fields = proposal_boxes[0]
    levels = level_plan[0]
    owner = fields[0] // (4 * fine_rows)
    members = (owner[:, None] == jnp.arange(tile_count, dtype=jnp.int32)[None, :]).astype(jnp.int32)
    rank = jnp.sum((jnp.cumsum(members, axis=0) - 1) * members, axis=1)
    relative = lax.rem(owner - band + tile_count, tile_count)
    slot_id = relative * capacity + rank
    slots = tile_count * capacity
    chosen = slot_id[None, :] == jnp.arange(slots, dtype=jnp.int32)[:, None]
    upstream_slots = jnp.dot(
        chosen.astype(jnp.bfloat16), upstream[0], preferred_element_type=jnp.float32
    ).astype(jnp.bfloat16)
    mine = chosen[:capacity].astype(jnp.int32)
    top, left, height, box_width = (
        jnp.sum(mine * fields[f][None, :], axis=1) for f in range(4)
    )
    level = jnp.sum(mine * levels[None, :], axis=1)

    stride = jnp.where(level == 0, 4, 8).astype(jnp.int32)
    is_fine = level == 0
    first_row = top // stride
    local_row = jnp.clip(
        first_row - band * jnp.where(is_fine, fine_rows, coarse_rows),
        0,
        jnp.where(is_fine, fine_rows, coarse_rows) - 1,
    )
    first_col = jnp.minimum(left // stride, jnp.where(is_fine, fine_cols, coarse_cols) - WIN)
    cells = jnp.stack(
        [local_row + jnp.where(is_fine, 0, fine_rows + WIN), first_col], axis=0
    ).astype(jnp.int32)
    stride_float = stride.astype(jnp.float32)
    geo = jnp.stack(
        [
            top.astype(jnp.float32) / stride_float - first_row.astype(jnp.float32),
            height.astype(jnp.float32) / (7.0 * stride_float),
            left.astype(jnp.float32) / stride_float - first_col.astype(jnp.float32),
            box_width.astype(jnp.float32) / (7.0 * stride_float),
        ],
        axis=0,
    )

    side = ((0, 0), (0, fine_cols - coarse_cols), (0, 0))
    maps = jnp.concatenate(
        [
            fine_tile,
            below_rows[:, :fine_cols],
            jnp.pad(coarse, side),
            jnp.pad(below_rows[:, fine_cols:], side),
        ],
        axis=0,
    )
    crop_blocks = make_crops(cells, geo, maps, starts, width, capacity)
    own_feats = jnp.concatenate(
        [
            from_ahead(
                lax.dynamic_index_in_dim(
                    crop_blocks, lax.rem(band - d + tile_count, tile_count), 0, keepdims=False
                ),
                "tile",
                d,
            )
            for d in range(tile_count)
        ],
        axis=0,
    )

    partial_hidden = lax.dot_general(
        own_feats, first_all, (((1,), (1,)), ((), ())), preferred_element_type=jnp.float32
    ).astype(jnp.bfloat16)
    share = second_weight.shape[0]

    def in_my_order(block, d):
        return jnp.roll(block, d * capacity, axis=0) if d else block

    hidden_own = 0.0
    for d in range(tile_count):
        to = lax.rem(band - d + tile_count, tile_count)
        piece = lax.dynamic_slice_in_dim(partial_hidden, to * share, share, axis=1)
        hidden_own = hidden_own + in_my_order(from_ahead(piece, "tile", d), d).astype(jnp.float32)
    gelu_value, gelu_slope = gelu_parts(hidden_own)
    activated = gelu_value.astype(jnp.bfloat16)
    back_grad = jnp.dot(upstream_slots, second_all, preferred_element_type=jnp.float32)
    pre_own = (back_grad * gelu_slope).astype(jnp.bfloat16)
    ahead = [in_my_order(from_ahead(pre_own, "tile", d), d) for d in range(tile_count)]
    twice = jnp.concatenate(ahead + ahead[:-1], axis=1)
    pre_grad = lax.dynamic_slice_in_dim(
        twice, lax.rem(tile_count - band, tile_count) * share, tile_count * share, axis=1
    )
    over_rows = (((0,), (0,)), ((), ()))
    second_part = lax.dot_general(
        upstream_slots, activated, over_rows, preferred_element_type=jnp.float32
    ).astype(jnp.bfloat16)
    first_part = lax.dot_general(
        pre_grad, own_feats, over_rows, preferred_element_type=jnp.float32
    ).astype(jnp.bfloat16)
    summed = lax.psum_scatter(
        jnp.concatenate([first_part, second_part], axis=1), "dp", scatter_dimension=0, tiled=True
    ).astype(jnp.float32)
    first_grad = lax.dynamic_slice_in_dim(summed[:, :lanes], feat_off, share_feats, axis=1).T
    second_grad = summed[:, lanes:].T
    return (first_grad, second_grad)


MESH = pl.DeviceIdType.MESH
REACH = 15
HALO = REACH - 1
NT = (((1,), (1,)), ((), ()))
NN = (((1,), (0,)), ((), ()))


def chip_grid(mesh):
    chips = [getattr(device, "coords", None) for device in mesh.devices[:, 0]]
    if chips[0] is None:
        return None
    cores = sum(1 for c in chips if tuple(c) == tuple(chips[0]))
    chips = [tuple(c) for c in chips[::cores]]
    if len(chips) == 1:
        return (1, 1, cores)
    axis = [a != b for a, b in zip(chips[0], chips[1])].index(True)
    fast = 1
    while fast < len(chips) and all(
        a == b or i == axis for i, (a, b) in enumerate(zip(chips[0], chips[fast]))
    ):
        fast += 1
    return (len(chips) // fast, fast, cores)


def offsets(size):
    if size == 1:
        return [0]
    if size == 2:
        return [0, 1]
    return [0] + [s * d for d in range(1, size) for s in (-1, 1)]


def steps_of(size):
    return {1: [], 2: [1]}.get(size, [-1, 1])


def moved(position, size, rel):
    if rel == 0 or size == 1:
        return position
    return 1 - position if size == 2 else position + rel


def last_axis(order, rel):
    used = [j for j in range(3) if rel[order[j]]]
    return used[-1] if used else -1


def onward(sizes, order, rel):
    last = last_axis(order, rel)
    hops = []
    if last >= 0:
        axis = order[last]
        if sizes[axis] > 2 and abs(rel[axis]) < sizes[axis] - 1:
            hops.append((last, axis, -1 if rel[axis] > 0 else 1))
    for j in range(last + 1, 3):
        hops.extend((j, order[j], step) for step in steps_of(sizes[order[j]]))
    return hops


def arrival_order(sizes, routes, extra):
    import heapq
    import itertools

    places = list(itertools.product(*(range(n) for n in sizes)))
    queue, waiting, busy = [], {}, set()
    seen, tick = {}, itertools.count()

    def start(link, now):
        if link not in busy and waiting.get(link):
            busy.add(link)
            load, arrival = waiting[link].pop(0)
            heapq.heappush(queue, (now + load, next(tick), link, arrival))

    def arrive(place, route, rel, now):
        seen.setdefault((route, rel), []).append(now)
        for _, axis, step in onward(sizes, routes[route][0], rel):
            target = list(place)
            target[axis] = moved(place[axis], sizes[axis], step)
            if not 0 <= target[axis] < sizes[axis]:
                continue
            there = list(rel)
            there[axis] = rel[axis] - step if sizes[axis] > 2 else 1
            link = (place, axis, step)
            waiting.setdefault(link, []).append(
                (routes[route][1], (tuple(target), route, tuple(there)))
            )
            start(link, now)

    first = {}
    for place in places:
        for route in extra[1]:
            arrive(place, route, (0, 0, 0), 0.0)
        if extra[0] and place[2] == 1:
            waiting.setdefault((place, 2, 1), []).append((extra[0], None))
            start((place, 2, 1), 0.0)
        for route in range(len(routes)):
            if route not in extra[1]:
                arrive(place, route, (0, 0, 0), 0.0)
    end = 0.0
    while queue:
        now, _, link, arrival = heapq.heappop(queue)
        end = now
        busy.discard(link)
        if arrival is not None:
            arrive(*arrival, now)
        start(link, now)
    key = {event: sum(t) / len(t) for event, t in seen.items()}
    for _ in range(sum(sizes)):
        for (route, rel) in list(key):
            for _, axis, step in onward(sizes, routes[route][0], rel):
                there = list(rel)
                there[axis] = rel[axis] - step if sizes[axis] > 2 else 1
                event = (route, tuple(there))
                if event in key:
                    key[event] = max(key[event], key[(route, rel)] + 1e-3)
    return sorted(key, key=lambda e: (key[e], e)), key, end


def slots_of(sizes, order):
    counts, before = [], 1
    for j in range(3):
        n = sizes[order[j]]
        counts.append(before * (2 * n if n > 2 else 1))
        before *= n
    return counts


def when(conds, body):
    if not conds:
        body()
        return
    total = conds[0]
    for cond in conds[1:]:
        total = jnp.logical_and(total, cond)
    pl.when(total)(body)


class Routes:
    def __init__(self, sizes, position, core, cores, orders):
        self.sizes, self.position = sizes, position
        self.core, self.cores = core, cores
        self.orders = orders
        self.slot_counts = [slots_of(sizes, order) for order in orders]

    def inside(self, axis, rel):
        if rel == 0 or self.sizes[axis] <= 2:
            return []
        p = self.position[axis]
        return [p < self.sizes[axis] - rel] if rel > 0 else [p >= -rel]

    def valid(self, rel):
        return sum((self.inside(axis, rel[axis]) for axis in range(3)), [])

    def at(self, rel):
        return [moved(self.position[a], self.sizes[a], rel[a]) for a in range(3)]

    def device(self, axis, step):
        there = list(self.position)
        there[axis] = moved(there[axis], self.sizes[axis], step)
        return ((there[0] * self.sizes[1] + there[1]) * self.cores + self.core, there[2])

    def back_step(self, order, rel):
        axis = order[last_axis(order, rel)]
        return axis, (1 if self.sizes[axis] == 2 or rel[axis] > 0 else -1)

    def number(self, place):
        return (place[0] * self.sizes[1] + place[1]) * self.sizes[2] + place[2]

    def direction(self, axis, step):
        return 2 * axis + (1 if step > 0 else 0)

    def gather(self, route, rel, ref_of, send_sems, recv_sems, drain=False):
        order = self.orders[route]

        def body():
            place = self.at(rel)
            ref = ref_of(place)
            q = self.number(place)

            def hop(axis, step):
                return pltpu.make_async_remote_copy(
                    src_ref=ref,
                    dst_ref=ref,
                    send_sem=send_sems.at[route, q, self.direction(axis, step)],
                    recv_sem=recv_sems.at[route, q],
                    device_id=self.device(axis, step),
                    device_id_type=MESH,
                )

            if last_axis(order, rel) >= 0 and not drain:
                hop(*self.back_step(order, rel)).wait_recv()
            for _, axis, step in onward(self.sizes, order, rel):
                copy = hop(axis, step)
                when(self.inside(axis, step), copy.wait_send if drain else copy.start)

        when(self.valid(rel), body)

    def slot(self, route, phase, side, place):
        order, counts = self.orders[route], self.slot_counts[route]
        index = 0
        for j in range(phase):
            index = index * self.sizes[order[j]] + place[order[j]]
        n = self.sizes[order[phase]]
        if n > 2:
            index = (index * n + place[order[phase]]) * 2 + (1 if side > 0 else 0)
        return sum(counts[:phase]) + index

    def scatter(self, route, rel, ref_of, slots, add, send_sems, recv_sems, drain=False):
        order = self.orders[route]

        def body():
            place = self.at(rel)
            ref = ref_of(place)
            q = self.number(place)
            if not drain:
                for phase, axis, step in onward(self.sizes, order, rel):
                    slot = self.slot(route, phase, step, place)

                    def take(axis=axis, step=step, slot=slot):
                        pltpu.make_async_remote_copy(
                            src_ref=ref,
                            dst_ref=slots.at[slot],
                            send_sem=send_sems.at[route, q],
                            recv_sem=recv_sems.at[route, slot],
                            device_id=self.device(axis, step),
                            device_id_type=MESH,
                        ).wait_recv()
                        add(ref, slots.at[slot])

                    when(self.inside(axis, step), take)
            phase = last_axis(order, rel)
            if phase >= 0:
                axis, step = self.back_step(order, rel)
                slot = self.slot(route, phase, 1 if self.sizes[axis] == 2 else -step, place)
                copy = pltpu.make_async_remote_copy(
                    src_ref=ref,
                    dst_ref=slots.at[slot],
                    send_sem=send_sems.at[route, q],
                    recv_sem=recv_sems.at[route, slot],
                    device_id=self.device(axis, step),
                    device_id_type=MESH,
                )
                if drain:
                    copy.wait_send()
                else:
                    copy.start()

        when(self.valid(rel), body)


def cut(bins, shares):
    edges = [0]
    for i in range(1, len(shares) + 1):
        edges.append(round(bins * sum(shares[:i]) / sum(shares)))
    return [(a, b - a) for a, b in zip(edges, edges[1:])]


ORDERS = ((2, 0, 1), (0, 1, 2), (1, 2, 0), (2, 0, 1))
GATHER_SHARES = (10, 11, 4)
SCATTER_SHARES = (6, 16, 3)


def step_kernel(
    grid,
    cells_ref,
    geo_ref,
    w1_ref,
    w2_ref,
    up_ref,
    upt_ref,
    fine_ref,
    coarse_ref,
    first_ref,
    second_ref,
    w_in,
    wbuf,
    w2buf,
    fine_low,
    coarse_low,
    wide,
    stage,
    crops,
    upb,
    uptb,
    back,
    hidden,
    acts,
    pres,
    grads,
    seconds,
    slots_a,
    slots_b,
    slots_c,
    slots_d,
    out_first,
    out_second,
    swap,
    local_sems,
    send_sems,
    recv_sems,
    sum_send_sems,
    sum_recv_sems,
    core_send,
    core_recv,
    crop_send,
    crop_recv,
):
    nz, nx, ny, cores = grid
    sizes = (nz, nx, ny)
    chips = nz * nx
    dp = lax.axis_index("dp")
    y = lax.axis_index("tile")
    core = dp % cores
    chip = dp // cores
    x = chip % nx
    z = chip // nx
    position = (z, x, y)
    other = 1 - core
    partner = (chip * cores + other, y)
    routes = Routes(sizes, position, core, cores, ORDERS)
    share, h = w1_ref.shape
    lanes = wbuf.shape[2]
    bins = lanes // 128
    fine_rows, fine_cols, _ = fine_ref.shape
    coarse_rows, coarse_cols, _ = coarse_ref.shape
    capacity = up_ref.shape[0]
    depth = w2_ref.shape[2]
    pair = 2 * h
    feat_bins = crops.shape[1] // 128
    starts = [min(t * share // 128, feat_bins - bins) for t in range(ny)]
    start_bin = starts[0] + y * (starts[1] - starts[0])
    shift = y * share - 128 * start_bin
    first_parts = cut(bins, GATHER_SHARES)
    sum_parts = cut(bins, SCATTER_SHARES)

    barrier = pltpu.get_barrier_semaphore()
    pl.semaphore_signal(barrier, inc=1, device_id=partner, device_id_type=MESH)
    peers = 1
    for axis in range(3):
        for step in steps_of(sizes[axis]):
            def greet(axis=axis, step=step):
                pl.semaphore_signal(
                    barrier, inc=1, device_id=routes.device(axis, step), device_id_type=MESH
                )
            near = routes.inside(axis, step)
            when(near, greet)
            peers = peers + (near[0].astype(jnp.int32) if near else 1)
    pl.semaphore_wait(barrier, peers)

    def rows(start, size):
        return pl.ds(pl.multiple_of(start, size), size)

    w_copy = pltpu.make_async_copy(
        w1_ref, w_in.at[pl.ds(pl.multiple_of(shift, 16), share), :], local_sems.at[0]
    )
    w_copy.start()
    w2_rows = rows(chip * pair + core * h, h)
    w2_copy = pltpu.make_async_copy(w2_ref.at[core], w2buf.at[y, w2_rows, :], local_sems.at[1])
    w2_copy.start()
    w2_swap = pltpu.make_async_remote_copy(
        src_ref=w2_ref.at[other],
        dst_ref=w2buf.at[y, w2_rows, :],
        send_sem=core_send.at[0],
        recv_sem=core_recv.at[0],
        device_id=partner,
        device_id_type=MESH,
    )
    w2_swap.start()
    fine_copy = pltpu.make_async_copy(
        fine_ref, fine_low.at[pl.ds(0, fine_rows)], local_sems.at[2]
    )
    coarse_copy = pltpu.make_async_copy(
        coarse_ref, coarse_low.at[pl.ds(0, coarse_rows)], local_sems.at[3]
    )
    fine_copy.start()
    coarse_copy.start()

    gather_routes = [
        (ORDERS[i], first_parts[i][1] if i < 3 else depth * pair // (h * 128)) for i in range(4)
    ]
    halo_load = HALO * (fine_cols + coarse_cols) // h
    events, times, _ = arrival_order(sizes, gather_routes, (halo_load, (0, 2)))

    def gather_ref(route):
        if route == 3:
            return lambda q: w2buf.at[q[2], rows((q[0] * nx + q[1]) * pair, pair), :]
        first, count = first_parts[route]
        return lambda q: wbuf.at[
            q[2], rows((q[0] * nx + q[1]) * h, h), pl.ds(first * 128, count * 128)
        ]

    def gather(event, drain=False):
        route, rel = event
        routes.gather(route, rel, gather_ref(route), send_sems, recv_sems, drain)

    own_rows = rows(chip * h, h)
    w_copy.wait()
    pad = lanes - share
    w_in[pl.ds(pl.multiple_of((1 - y) * share, 16), pad), :] = jnp.zeros((pad, h), jnp.bfloat16)
    for i in range(bins):
        block = w_in[128 * i : 128 * (i + 1), :].astype(jnp.float32)
        wbuf[y, own_rows, 128 * i : 128 * (i + 1)] = block.T.astype(jnp.bfloat16)

    gather((0, (0, 0, 0)))
    gather((2, (0, 0, 0)))
    below = routes.device(2, 1)
    fine_halo = pltpu.make_async_remote_copy(
        src_ref=fine_ref.at[pl.ds(0, HALO)],
        dst_ref=fine_low.at[pl.ds(fine_rows, HALO)],
        send_sem=core_send.at[1],
        recv_sem=core_recv.at[1],
        device_id=below,
        device_id_type=MESH,
    )
    coarse_halo = pltpu.make_async_remote_copy(
        src_ref=coarse_ref.at[pl.ds(0, HALO)],
        dst_ref=coarse_low.at[pl.ds(coarse_rows, HALO)],
        send_sem=core_send.at[2],
        recv_sem=core_recv.at[2],
        device_id=below,
        device_id_type=MESH,
    )

    @pl.when(y == 1)
    def _():
        fine_halo.start()
        coarse_halo.start()

    gather((1, (0, 0, 0)))
    w2_copy.wait()
    w2_swap.wait()
    gather((3, (0, 0, 0)))
    todo = [e for e in events if e[1] != (0, 0, 0)]

    half = rows(core * capacity, capacity)
    ups = []
    for i, (src, dst) in enumerate(((up_ref, upb.at[half, :]), (upt_ref, uptb.at[core]))):
        ups.append(pltpu.make_async_copy(src, dst, local_sems.at[4 + i]))
        ups.append(
            pltpu.make_async_remote_copy(
                src_ref=src,
                dst_ref=dst,
                send_sem=core_send.at[3 + i],
                recv_sem=core_recv.at[3 + i],
                device_id=partner,
                device_id_type=MESH,
            )
        )
    for copy in ups:
        copy.start()

    coarse_base = fine_rows + HALO

    def widen(low, first, count, base, cols):
        def one(r, carry):
            wide[base + r, 0:cols, :] = low[r].astype(jnp.float32)
            return carry

        lax.fori_loop(first, first + count, one, 0)

    fine_copy.wait()
    coarse_copy.wait()
    widen(fine_low, 0, fine_rows, 0, fine_cols)
    widen(coarse_low, 0, coarse_rows, coarse_base, coarse_cols)

    scale = max(times.values())
    early = [e for e in todo if times[e] < HALO_TIME * scale]
    for event in early:
        gather(event)
    todo = todo[len(early) :]

    @pl.when(y == 0)
    def _():
        fine_halo.wait_recv()
        coarse_halo.wait_recv()
        widen(fine_low, fine_rows, HALO, 0, fine_cols)
        widen(coarse_low, coarse_rows, HALO, coarse_base, coarse_cols)

    @pl.when(y == 1)
    def _():
        def clear(r, carry):
            wide[r] = jnp.zeros(wide.shape[1:], jnp.float32)
            return carry

        lax.fori_loop(fine_rows, fine_rows + HALO, clear, 0)
        lax.fori_loop(coarse_base + coarse_rows, coarse_base + coarse_rows + HALO, clear, 0)

    groups = capacity // GROUP
    during = [e for e in todo if times[e] < CROP_TIME * scale]
    todo = todo[len(during) :]
    shape = (ROWS_PAD, REACH * WIN)
    k = lax.broadcasted_iota(jnp.int32, shape, 0).astype(jnp.float32)
    i_bin = jnp.floor((k + 0.5) * (1.0 / BINS))
    j_bin = k - BINS * i_bin
    i_mid = i_bin + 0.5
    j_mid = j_bin + 0.5
    lane = lax.broadcasted_iota(jnp.int32, shape, 1)
    r_cell = (lane >> 4).astype(jnp.float32)
    q_cell = (lane & 15).astype(jnp.float32)

    def crop_copy(g):
        group_rows = rows(core * capacity + g * GROUP, GROUP)
        return pltpu.make_async_remote_copy(
            src_ref=crops.at[group_rows, :],
            dst_ref=crops.at[group_rows, :],
            send_sem=crop_send.at[g],
            recv_sem=crop_recv.at[g],
            device_id=partner,
            device_id_type=MESH,
        )

    def crop_group(g, carry):
        for n, event in enumerate(during):
            pl.when(g == n * groups // len(during))(functools.partial(gather, event))
        for p in range(GROUP):
            n = g * GROUP + p
            row = cells_ref[0, n]
            col = cells_ref[1, n]
            row_w = jnp.maximum(0.0, 1.0 - jnp.abs(i_mid * geo_ref[1, n] + geo_ref[0, n] - r_cell))
            col_w = jnp.maximum(0.0, 1.0 - jnp.abs(j_mid * geo_ref[3, n] + geo_ref[2, n] - q_cell))
            weights = (row_w * col_w).astype(jnp.bfloat16)
            window = jnp.concatenate(
                [wide[row + r, pl.ds(col, WIN), :] for r in range(REACH)], axis=0
            ).astype(jnp.bfloat16)
            crop = jnp.dot(weights, window, preferred_element_type=jnp.float32)
            stage[pl.ds(p, ROWS_PAD, stride=GROUP), :] = crop
        group_rows = rows(core * capacity + g * GROUP, GROUP)
        for m in range(feat_bins):
            crops[group_rows, m * 128 : (m + 1) * 128] = stage[
                m * GROUP : (m + 1) * GROUP, :
            ].astype(jnp.bfloat16)

        @pl.when(g > 0)
        def _():
            crop_copy(g - 1).start()

        return carry

    lax.fori_loop(0, groups, crop_group, 0)
    crop_copy(groups - 1).start()

    for copy in ups:
        copy.wait()
    for event in todo:
        gather(event)
    for g in range(groups):
        crop_copy(g).wait()

    for t in range(ny):
        part = jnp.dot(upb[...], w2buf[t], preferred_element_type=jnp.float32)
        back[t * depth : (t + 1) * depth, :] = part.T

    hidden[...] = jnp.zeros_like(hidden)
    chunk = 640 if lanes % 640 == 0 else 128
    for t in range(ny):
        def hide(i, carry, t=t):
            at = pl.multiple_of(i * chunk, 128)
            from_at = pl.multiple_of(starts[t] * 128 + i * chunk, 128)
            hidden[...] += lax.dot_general(
                wbuf[t, :, pl.ds(at, chunk)],
                crops[:, pl.ds(from_at, chunk)],
                NT,
                preferred_element_type=jnp.float32,
            )
            return carry

        lax.fori_loop(0, lanes // chunk, hide, 0)

    def gelu(i, carry):
        at = rows(i * 32, 32)
        value, slope = gelu_parts(hidden[at, :])
        acts[at, :] = value.astype(jnp.bfloat16)
        pres[at, :] = (back[at, :] * slope).astype(jnp.bfloat16)
        return carry

    lax.fori_loop(0, hidden.shape[0] // 32, gelu, 0)
    for event in events:
        gather(event, drain=True)

    sum_routes = [
        (ORDERS[i], sum_parts[i][1] if i < 3 else depth * pair // (h * 128)) for i in range(4)
    ]
    sum_events, _, _ = arrival_order(sizes, sum_routes, (0, ()))
    sum_events = sum_events[::-1]
    slot_refs = (slots_a, slots_b, slots_c, slots_d)

    def sum_ref(route):
        if route == 3:
            return lambda q: seconds.at[q[2], rows((q[0] * nx + q[1]) * pair, pair), :]
        first, count = sum_parts[route]
        return lambda q: grads.at[
            q[2], rows((q[0] * nx + q[1]) * h, h), pl.ds(first * 128, count * 128)
        ]

    def add(ref, more):
        def one(i, carry):
            at = rows(i * 16, 16)
            total = ref[at, :].astype(jnp.float32) + more[at, :].astype(jnp.float32)
            ref[at, :] = total.astype(jnp.bfloat16)
            return carry

        lax.fori_loop(0, ref.shape[0] // 16, one, 0)

    def scatter(event, drain=False):
        route, rel = event
        routes.scatter(
            route, rel, sum_ref(route), slot_refs[route], add, sum_send_sems, sum_recv_sems, drain
        )

    def make_grads(t, part):
        first, count = sum_parts[part]
        step = max(c for c in range(1, 6) if count % c == 0)

        def one(i, carry):
            at = pl.multiple_of((first + i * step) * 128, 128)
            base = starts[0] + t * (starts[1] - starts[0])
            from_at = pl.multiple_of(base * 128 + at, 128)
            grads[t, :, pl.ds(at, step * 128)] = jnp.dot(
                pres[...], crops[:, pl.ds(from_at, step * 128)], preferred_element_type=jnp.float32
            ).astype(jnp.bfloat16)
            return carry

        lax.fori_loop(0, count // step, one, 0)

    def leaf(route):
        order = ORDERS[route]
        return [
            e
            for e in sum_events
            if e[0] == route and not onward(sizes, order, e[1])
        ]

    done = []

    def run(chosen):
        for event in chosen:
            scatter(event)
            done.append(event)

    make_grads(1 - y, 1)
    run(leaf(1))
    make_grads(1 - y, 0)
    make_grads(y, 0)
    run(leaf(0))
    for part in range(2):
        for t in range(ny):
            total = lax.dot_general(
                uptb[part],
                acts[t * depth : (t + 1) * depth, part * capacity : (part + 1) * capacity],
                NT,
                preferred_element_type=jnp.float32,
            )
            if part:
                total = total + stash[t]
            if part == 0:
                stash = (stash if t else []) + [total]
            else:
                seconds[t] = total.astype(jnp.bfloat16)
    run(leaf(3))
    make_grads(1 - y, 2)
    make_grads(y, 2)
    run(leaf(2))
    make_grads(y, 1)
    run([e for e in sum_events if e not in done])

    swap[0] = seconds[y, rows(chip * pair + other * h, h), :]
    second_swap = pltpu.make_async_remote_copy(
        src_ref=swap.at[0],
        dst_ref=swap.at[1],
        send_sem=core_send.at[5],
        recv_sem=core_recv.at[5],
        device_id=partner,
        device_id_type=MESH,
    )
    second_swap.start()
    for i in range(bins):
        block = grads[y, own_rows, 128 * i : 128 * (i + 1)].astype(jnp.float32)
        out_first[128 * i : 128 * (i + 1), :] = block.T
    first_out = pltpu.make_async_copy(
        out_first.at[pl.ds(pl.multiple_of(shift, 16), share), :], first_ref, local_sems.at[6]
    )
    first_out.start()
    out_second[core] = seconds[y, rows(chip * pair + core * h, h), :].astype(jnp.float32)
    second_swap.wait()
    out_second[other] = swap[1].astype(jnp.float32)
    second_out = pltpu.make_async_copy(out_second, second_ref, local_sems.at[7])
    second_out.start()
    for event in sum_events:
        scatter(event, drain=True)

    @pl.when(y == 1)
    def _():
        fine_halo.wait_send()
        coarse_halo.wait_send()

    first_out.wait()
    second_out.wait()


HALO_TIME = 0.4
CROP_TIME = 0.62


def per_device_by_chips(
    grid, proposal_boxes, level_plan, fine_map, coarse_map, first_weight, second_weight, upstream
):
    nz, nx, ny, cores = grid
    chips = nz * nx
    band = lax.axis_index("tile")
    core = lax.axis_index("dp") % cores
    num_props = level_plan.shape[1]
    capacity = num_props // ny
    fine_tile, coarse = fine_map[0], coarse_map[0]
    fine_rows, fine_cols, channels = fine_tile.shape
    coarse_rows, coarse_cols = coarse.shape[:2]
    share, h = first_weight.shape
    feats = share * ny
    bins = max(-(-((t + 1) * share) // 128) - t * share // 128 for t in range(ny))
    lanes = bins * 128
    hidden_size = upstream.shape[2]
    depth = second_weight.shape[0] // cores
    pair = cores * h

    fields, levels = proposal_boxes[0], level_plan[0]
    member = (fields[0] // (4 * fine_rows) == band).astype(jnp.int32)
    rank = jnp.cumsum(member) - 1
    slot = jnp.where(member == 1, rank, -1)
    chosen = slot[None, :] == jnp.arange(capacity, dtype=jnp.int32)[:, None]
    picks = chosen.astype(jnp.bfloat16)
    up = jnp.dot(picks, upstream[0], preferred_element_type=jnp.float32).astype(jnp.bfloat16)
    up_turned = lax.dot_general(
        upstream[0], picks, (((0,), (1,)), ((), ())), preferred_element_type=jnp.float32
    ).astype(jnp.bfloat16)
    mine = chosen.astype(jnp.int32)
    top, left, height, box_width = (
        jnp.sum(mine * fields[f][None, :], axis=1) for f in range(4)
    )
    level = jnp.sum(mine * levels[None, :], axis=1)
    is_fine = level == 0
    stride = jnp.where(is_fine, 4, 8).astype(jnp.int32)
    first_row = top // stride
    band_rows = jnp.where(is_fine, fine_rows, coarse_rows)
    local_row = jnp.clip(first_row - band * band_rows, 0, band_rows - 1)
    first_col = jnp.minimum(left // stride, jnp.where(is_fine, fine_cols, coarse_cols) - WIN)
    cells = jnp.stack(
        [local_row + jnp.where(is_fine, 0, fine_rows + HALO), first_col], axis=0
    ).astype(jnp.int32)
    stride_float = stride.astype(jnp.float32)
    geo = jnp.stack(
        [
            top.astype(jnp.float32) / stride_float - first_row.astype(jnp.float32),
            height.astype(jnp.float32) / (7.0 * stride_float),
            left.astype(jnp.float32) / stride_float - first_col.astype(jnp.float32),
            box_width.astype(jnp.float32) / (7.0 * stride_float),
        ],
        axis=0,
    )
    second_sets = (
        second_weight.T.reshape(h, depth // h, cores, h).transpose(2, 0, 1, 3).reshape(cores, h, depth)
    )

    low, f32 = jnp.bfloat16, jnp.float32
    sizes = (nz, nx, ny)
    sum_parts = cut(bins, SCATTER_SHARES)
    slot_counts = [sum(slots_of(sizes, order)) for order in ORDERS]
    rows_all = chips * h
    batch = cores * capacity
    q = chips * ny
    dma = pltpu.SemaphoreType.DMA
    anywhere = pl.BlockSpec(memory_space=pl.ANY)
    smem = pl.BlockSpec(memory_space=pltpu.SMEM)
    first, second = pl.pallas_call(
        functools.partial(step_kernel, grid),
        out_shape=(
            jax.ShapeDtypeStruct((share, h), f32),
            jax.ShapeDtypeStruct((cores, h, depth), f32),
        ),
        in_specs=[smem, smem] + [anywhere] * 6,
        out_specs=(anywhere, anywhere),
        scratch_shapes=[
            pltpu.VMEM((lanes, h), low),
            pltpu.VMEM((ny, rows_all, lanes), low),
            pltpu.VMEM((ny, hidden_size, depth), low),
            pltpu.VMEM((fine_rows + HALO, fine_cols, channels), low),
            pltpu.VMEM((coarse_rows + HALO, coarse_cols, channels), low),
            pltpu.VMEM((fine_rows + coarse_rows + 2 * HALO, fine_cols, channels), f32),
            pltpu.VMEM((ROWS_PAD * GROUP, 128), f32),
            pltpu.VMEM((batch, feats), low),
            pltpu.VMEM((batch, hidden_size), low),
            pltpu.VMEM((cores, hidden_size, capacity), low),
            pltpu.VMEM((rows_all, batch), f32),
            pltpu.VMEM((rows_all, batch), f32),
            pltpu.VMEM((rows_all, batch), low),
            pltpu.VMEM((rows_all, batch), low),
            pltpu.VMEM((ny, rows_all, lanes), low),
            pltpu.VMEM((ny, hidden_size, depth), low),
            pltpu.VMEM((slot_counts[0], h, sum_parts[0][1] * 128), low),
            pltpu.VMEM((slot_counts[1], h, sum_parts[1][1] * 128), low),
            pltpu.VMEM((slot_counts[2], h, sum_parts[2][1] * 128), low),
            pltpu.VMEM((slot_counts[3], pair, depth), low),
            pltpu.VMEM((lanes, h), f32),
            pltpu.VMEM((cores, h, depth), f32),
            pltpu.VMEM((2, h, depth), low),
            dma((8,)),
            dma((4, q, 6)),
            dma((4, q)),
            dma((4, q)),
            dma((4, max(slot_counts))),
            dma((6,)),
            dma((6,)),
            dma((capacity // GROUP,)),
            dma((capacity // GROUP,)),
        ],
        compiler_params=pltpu.CompilerParams(
            collective_id=0, has_side_effects=True, vmem_limit_bytes=64000 * 1024
        ),
        name="step",
    )(cells, geo, first_weight, second_sets, up, up_turned, fine_tile, coarse)
    turned = second.reshape(cores, h, depth // h, h).transpose(2, 0, 3, 1)
    return (first, turned.reshape(cores * depth, h))


def solution(mesh):
    placed = (
        P("dp", None, None),
        P("dp", None),
        P("dp", "tile", None, None),
        P("dp", "tile", None, None),
        P("tile", "dp"),
        P("tile", "dp"),
        P("dp", None, None),
    )
    grid = chip_grid(mesh)
    tiles = mesh.shape["tile"]
    body = per_device_by_bands
    if grid is not None and tiles == 2 and grid[1] <= 2 and grid[2] == 2:
        body = functools.partial(per_device_by_chips, (grid[0], grid[1], tiles, grid[2]))
    return jax.shard_map(
        body,
        mesh=mesh,
        in_specs=placed,
        out_specs=(P("tile", "dp"), P("tile", "dp")),
        check_vma=False,
    )
```

```python
import functools

import jax
import jax.numpy as jnp
from jax import lax
from jax.experimental import pallas as pl
from jax.experimental.pallas import tpu as pltpu
from jax.sharding import PartitionSpec as P

WIN = 16
BINS = 7
ROWS_PAD = 56
GROUP = 16


def from_ahead(block, axis, distance):
    if distance == 0:
        return block
    size = lax.axis_size(axis)
    return lax.ppermute(block, axis, [(i, (i - distance) % size) for i in range(size)])


def halo_from_next(block, axis):
    size = lax.axis_size(axis)
    return lax.ppermute(block, axis, [(i + 1, i) for i in range(size - 1)])


def gelu_parts(hidden):
    factor = 0.7978845608028654
    cubic_term = 0.044715
    inner_term = factor * (hidden + cubic_term * hidden * hidden * hidden)
    tangent = jnp.tanh(inner_term)
    gelu_value = 0.5 * hidden * (1.0 + tangent)
    gelu_slope = 0.5 * (1.0 + tangent) + 0.5 * hidden * (1.0 - tangent * tangent) * factor * (
        1.0 + 3.0 * cubic_term * hidden * hidden
    )
    return (gelu_value, gelu_slope)


def crop_kernel(starts, width, cells_ref, geo_ref, maps_ref, out_ref, wide, stage):
    step = pl.program_id(0)

    @pl.when(step == 0)
    def _():
        def widen(r, carry):
            wide[r] = maps_ref[r].astype(jnp.float32)
            return carry

        lax.fori_loop(0, maps_ref.shape[0], widen, 0)

    shape = (ROWS_PAD, WIN * WIN)
    k = lax.broadcasted_iota(jnp.int32, shape, 0).astype(jnp.float32)
    i_bin = jnp.floor((k + 0.5) * (1.0 / BINS))
    j_bin = k - BINS * i_bin
    i_mid = i_bin + 0.5
    j_mid = j_bin + 0.5
    lane = lax.broadcasted_iota(jnp.int32, shape, 1)
    r_cell = (lane >> 4).astype(jnp.float32)
    q_cell = (lane & 15).astype(jnp.float32)
    for p in range(GROUP):
        n = step * GROUP + p
        row = cells_ref[0, n]
        col = cells_ref[1, n]
        row_w = jnp.maximum(0.0, 1.0 - jnp.abs(i_mid * geo_ref[1, n] + geo_ref[0, n] - r_cell))
        col_w = jnp.maximum(0.0, 1.0 - jnp.abs(j_mid * geo_ref[3, n] + geo_ref[2, n] - q_cell))
        weights = (row_w * col_w).astype(jnp.bfloat16)
        window = jnp.concatenate(
            [wide[row + r, pl.ds(col, WIN), :] for r in range(WIN)], axis=0
        ).astype(jnp.bfloat16)
        crop = jnp.dot(weights, window, preferred_element_type=jnp.float32)
        stage[pl.ds(p, ROWS_PAD, stride=GROUP), :] = crop
    for t, first in enumerate(starts):
        for m in range(width):
            at = (first + m) * GROUP
            out_ref[t, :, m * 128 : (m + 1) * 128] = stage[at : at + GROUP, :].astype(jnp.bfloat16)


def make_crops(cells, geo, maps, starts, width, capacity):
    tiles = len(starts)
    lanes = width * 128
    return pl.pallas_call(
        functools.partial(crop_kernel, starts, width),
        grid=(capacity // GROUP,),
        out_shape=jax.ShapeDtypeStruct((tiles, capacity, lanes), jnp.bfloat16),
        in_specs=[
            pl.BlockSpec(memory_space=pltpu.SMEM),
            pl.BlockSpec(memory_space=pltpu.SMEM),
            pl.BlockSpec(maps.shape, lambda g: (0, 0, 0)),
        ],
        out_specs=pl.BlockSpec((tiles, GROUP, lanes), lambda g: (0, g, 0)),
        scratch_shapes=[
            pltpu.VMEM(maps.shape, jnp.float32),
            pltpu.VMEM((ROWS_PAD * GROUP, 128), jnp.float32),
        ],
        compiler_params=pltpu.CompilerParams(
            dimension_semantics=("arbitrary",), vmem_limit_bytes=48 * 1024 * 1024
        ),
        cost_estimate=pl.CostEstimate(
            flops=capacity * ROWS_PAD * WIN * WIN * 128 * 16,
            bytes_accessed=2 * maps.size + 2 * tiles * capacity * lanes,
            transcendentals=0,
        ),
        name="crops",
    )(cells, geo, maps)


def per_device_by_bands(
    proposal_boxes, level_plan, fine_map, coarse_map, first_weight, second_weight, upstream
):
    tile_count = lax.axis_size("tile")
    band = lax.axis_index("tile")
    num_props = level_plan.shape[1]
    capacity = max(num_props // 4, num_props // tile_count)
    fine_tile = fine_map[0]
    coarse = coarse_map[0]
    fine_rows, fine_cols, channels = fine_tile.shape
    coarse_rows, coarse_cols = (coarse.shape[0], coarse.shape[1])

    top_rows = jnp.concatenate([fine_tile[:WIN], coarse[:WIN]], axis=1)
    below_rows = halo_from_next(top_rows, "tile")

    share_feats = first_weight.shape[0]
    feats = share_feats * tile_count
    width = max(
        -(-((t + 1) * share_feats) // 128) - t * share_feats // 128 for t in range(tile_count)
    )
    starts = [min(t * share_feats // 128, feats // 128 - width) for t in range(tile_count)]
    lanes = width * 128
    feat_off = band * share_feats - 128 * jnp.minimum(
        band * share_feats // 128, feats // 128 - width
    )

    first_rows = lax.dynamic_update_slice(
        jnp.zeros((first_weight.shape[1], lanes), jnp.bfloat16),
        first_weight.T,
        (0, feat_off),
    )
    both = lax.all_gather(
        jnp.concatenate([first_rows, second_weight.T], axis=1), "dp", axis=0, tiled=True
    )
    first_all = both[:, :lanes]
    second_all = both[:, lanes:]

    fields = proposal_boxes[0]
    levels = level_plan[0]
    owner = fields[0] // (4 * fine_rows)
    members = (owner[:, None] == jnp.arange(tile_count, dtype=jnp.int32)[None, :]).astype(jnp.int32)
    rank = jnp.sum((jnp.cumsum(members, axis=0) - 1) * members, axis=1)
    relative = lax.rem(owner - band + tile_count, tile_count)
    slot_id = relative * capacity + rank
    slots = tile_count * capacity
    chosen = slot_id[None, :] == jnp.arange(slots, dtype=jnp.int32)[:, None]
    upstream_slots = jnp.dot(
        chosen.astype(jnp.bfloat16), upstream[0], preferred_element_type=jnp.float32
    ).astype(jnp.bfloat16)
    mine = chosen[:capacity].astype(jnp.int32)
    top, left, height, box_width = (
        jnp.sum(mine * fields[f][None, :], axis=1) for f in range(4)
    )
    level = jnp.sum(mine * levels[None, :], axis=1)

    stride = jnp.where(level == 0, 4, 8).astype(jnp.int32)
    is_fine = level == 0
    first_row = top // stride
    local_row = jnp.clip(
        first_row - band * jnp.where(is_fine, fine_rows, coarse_rows),
        0,
        jnp.where(is_fine, fine_rows, coarse_rows) - 1,
    )
    first_col = jnp.minimum(left // stride, jnp.where(is_fine, fine_cols, coarse_cols) - WIN)
    cells = jnp.stack(
        [local_row + jnp.where(is_fine, 0, fine_rows + WIN), first_col], axis=0
    ).astype(jnp.int32)
    stride_float = stride.astype(jnp.float32)
    geo = jnp.stack(
        [
            top.astype(jnp.float32) / stride_float - first_row.astype(jnp.float32),
            height.astype(jnp.float32) / (7.0 * stride_float),
            left.astype(jnp.float32) / stride_float - first_col.astype(jnp.float32),
            box_width.astype(jnp.float32) / (7.0 * stride_float),
        ],
        axis=0,
    )

    side = ((0, 0), (0, fine_cols - coarse_cols), (0, 0))
    maps = jnp.concatenate(
        [
            fine_tile,
            below_rows[:, :fine_cols],
            jnp.pad(coarse, side),
            jnp.pad(below_rows[:, fine_cols:], side),
        ],
        axis=0,
    )
    crop_blocks = make_crops(cells, geo, maps, starts, width, capacity)
    own_feats = jnp.concatenate(
        [
            from_ahead(
                lax.dynamic_index_in_dim(
                    crop_blocks, lax.rem(band - d + tile_count, tile_count), 0, keepdims=False
                ),
                "tile",
                d,
            )
            for d in range(tile_count)
        ],
        axis=0,
    )

    partial_hidden = lax.dot_general(
        own_feats, first_all, (((1,), (1,)), ((), ())), preferred_element_type=jnp.float32
    ).astype(jnp.bfloat16)
    share = second_weight.shape[0]

    def in_my_order(block, d):
        return jnp.roll(block, d * capacity, axis=0) if d else block

    hidden_own = 0.0
    for d in range(tile_count):
        to = lax.rem(band - d + tile_count, tile_count)
        piece = lax.dynamic_slice_in_dim(partial_hidden, to * share, share, axis=1)
        hidden_own = hidden_own + in_my_order(from_ahead(piece, "tile", d), d).astype(jnp.float32)
    gelu_value, gelu_slope = gelu_parts(hidden_own)
    activated = gelu_value.astype(jnp.bfloat16)
    back_grad = jnp.dot(upstream_slots, second_all, preferred_element_type=jnp.float32)
    pre_own = (back_grad * gelu_slope).astype(jnp.bfloat16)
    ahead = [in_my_order(from_ahead(pre_own, "tile", d), d) for d in range(tile_count)]
    twice = jnp.concatenate(ahead + ahead[:-1], axis=1)
    pre_grad = lax.dynamic_slice_in_dim(
        twice, lax.rem(tile_count - band, tile_count) * share, tile_count * share, axis=1
    )
    over_rows = (((0,), (0,)), ((), ()))
    second_part = lax.dot_general(
        upstream_slots, activated, over_rows, preferred_element_type=jnp.float32
    ).astype(jnp.bfloat16)
    first_part = lax.dot_general(
        pre_grad, own_feats, over_rows, preferred_element_type=jnp.float32
    ).astype(jnp.bfloat16)
    summed = lax.psum_scatter(
        jnp.concatenate([first_part, second_part], axis=1), "dp", scatter_dimension=0, tiled=True
    ).astype(jnp.float32)
    first_grad = lax.dynamic_slice_in_dim(summed[:, :lanes], feat_off, share_feats, axis=1).T
    second_grad = summed[:, lanes:].T
    return (first_grad, second_grad)


MESH = pl.DeviceIdType.MESH
REACH = 15
HALO = REACH - 1
NT = (((1,), (1,)), ((), ()))
NN = (((1,), (0,)), ((), ()))


def chip_grid(mesh):
    chips = [getattr(device, "coords", None) for device in mesh.devices[:, 0]]
    if chips[0] is None:
        return None
    cores = sum(1 for c in chips if tuple(c) == tuple(chips[0]))
    chips = [tuple(c) for c in chips[::cores]]
    if len(chips) == 1:
        return (1, 1, cores)
    axis = [a != b for a, b in zip(chips[0], chips[1])].index(True)
    fast = 1
    while fast < len(chips) and all(
        a == b or i == axis for i, (a, b) in enumerate(zip(chips[0], chips[fast]))
    ):
        fast += 1
    return (len(chips) // fast, fast, cores)


def offsets(size):
    if size == 1:
        return [0]
    if size == 2:
        return [0, 1]
    return [0] + [s * d for d in range(1, size) for s in (-1, 1)]


def steps_of(size):
    return {1: [], 2: [1]}.get(size, [-1, 1])


def moved(position, size, rel):
    if rel == 0 or size == 1:
        return position
    return 1 - position if size == 2 else position + rel


def last_axis(order, rel):
    used = [j for j in range(3) if rel[order[j]]]
    return used[-1] if used else -1


def onward(sizes, order, rel):
    last = last_axis(order, rel)
    hops = []
    if last >= 0:
        axis = order[last]
        if sizes[axis] > 2 and abs(rel[axis]) < sizes[axis] - 1:
            hops.append((last, axis, -1 if rel[axis] > 0 else 1))
    for j in range(last + 1, 3):
        hops.extend((j, order[j], step) for step in steps_of(sizes[order[j]]))
    return hops


def arrival_order(sizes, routes, extra):
    import heapq
    import itertools

    places = list(itertools.product(*(range(n) for n in sizes)))
    queue, waiting, busy = [], {}, set()
    seen, tick = {}, itertools.count()

    def start(link, now):
        if link not in busy and waiting.get(link):
            busy.add(link)
            load, arrival = waiting[link].pop(0)
            heapq.heappush(queue, (now + load, next(tick), link, arrival))

    def arrive(place, route, rel, now):
        seen.setdefault((route, rel), []).append(now)
        for _, axis, step in onward(sizes, routes[route][0], rel):
            target = list(place)
            target[axis] = moved(place[axis], sizes[axis], step)
            if not 0 <= target[axis] < sizes[axis]:
                continue
            there = list(rel)
            there[axis] = rel[axis] - step if sizes[axis] > 2 else 1
            link = (place, axis, step)
            waiting.setdefault(link, []).append(
                (routes[route][1], (tuple(target), route, tuple(there)))
            )
            start(link, now)

    first = {}
    for place in places:
        for route in extra[1]:
            arrive(place, route, (0, 0, 0), 0.0)
        if extra[0] and place[2] == 1:
            waiting.setdefault((place, 2, 1), []).append((extra[0], None))
            start((place, 2, 1), 0.0)
        for route in range(len(routes)):
            if route not in extra[1]:
                arrive(place, route, (0, 0, 0), 0.0)
    end = 0.0
    while queue:
        now, _, link, arrival = heapq.heappop(queue)
        end = now
        busy.discard(link)
        if arrival is not None:
            arrive(*arrival, now)
        start(link, now)
    key = {event: sum(t) / len(t) for event, t in seen.items()}
    for _ in range(sum(sizes)):
        for (route, rel) in list(key):
            for _, axis, step in onward(sizes, routes[route][0], rel):
                there = list(rel)
                there[axis] = rel[axis] - step if sizes[axis] > 2 else 1
                event = (route, tuple(there))
                if event in key:
                    key[event] = max(key[event], key[(route, rel)] + 1e-3)
    return sorted(key, key=lambda e: (key[e], e)), key, end


def slots_of(sizes, order):
    counts, before = [], 1
    for j in range(3):
        n = sizes[order[j]]
        counts.append(before * (2 * n if n > 2 else 1))
        before *= n
    return counts


def when(conds, body):
    if not conds:
        body()
        return
    total = conds[0]
    for cond in conds[1:]:
        total = jnp.logical_and(total, cond)
    pl.when(total)(body)


class Routes:
    def __init__(self, sizes, position, core, cores, orders):
        self.sizes, self.position = sizes, position
        self.core, self.cores = core, cores
        self.orders = orders
        self.slot_counts = [slots_of(sizes, order) for order in orders]
        self.slot_base = [sum(sum(c) for c in self.slot_counts[:i]) for i in range(len(orders))]

    def inside(self, axis, rel):
        if rel == 0 or self.sizes[axis] <= 2:
            return []
        p = self.position[axis]
        return [p < self.sizes[axis] - rel] if rel > 0 else [p >= -rel]

    def valid(self, rel):
        return sum((self.inside(axis, rel[axis]) for axis in range(3)), [])

    def at(self, rel):
        return [moved(self.position[a], self.sizes[a], rel[a]) for a in range(3)]

    def device(self, axis, step):
        there = list(self.position)
        there[axis] = moved(there[axis], self.sizes[axis], step)
        return ((there[0] * self.sizes[1] + there[1]) * self.cores + self.core, there[2])

    def back_step(self, order, rel):
        axis = order[last_axis(order, rel)]
        return axis, (1 if self.sizes[axis] == 2 or rel[axis] > 0 else -1)

    def number(self, place):
        return (place[0] * self.sizes[1] + place[1]) * self.sizes[2] + place[2]

    def direction(self, axis, step):
        return 2 * axis + (1 if step > 0 else 0)

    def drain(self, route, whole, unit, sems):
        order, before = self.orders[route], 1
        for axis in order:
            n, p = self.sizes[axis], self.position[axis]
            for step in steps_of(n):
                for at in range(n) if n > 2 else [0]:
                    sent = before * ((at + 1 if step > 0 else n - at) if n > 2 else 1)
                    if n > 2 and not 0 <= at + step < n:
                        continue

                    def wait(axis=axis, step=step, sent=sent):
                        part = whole(sent * unit)
                        pltpu.make_async_copy(
                            part, part, sems.at[route, self.direction(axis, step)]
                        ).wait()

                    when([p == at] if n > 2 else [], wait)
            before *= n

    def gather(self, route, rel, ref_of, send_sems, recv_sems):
        order = self.orders[route]

        def body():
            place = self.at(rel)
            ref = ref_of(place)
            q = self.number(place)

            def hop(axis, step):
                return pltpu.make_async_remote_copy(
                    src_ref=ref,
                    dst_ref=ref,
                    send_sem=send_sems.at[route, self.direction(axis, step)],
                    recv_sem=recv_sems.at[route, q],
                    device_id=self.device(axis, step),
                    device_id_type=MESH,
                )

            if last_axis(order, rel) >= 0:
                hop(*self.back_step(order, rel)).wait_recv()
            for _, axis, step in onward(self.sizes, order, rel):
                copy = hop(axis, step)
                when(self.inside(axis, step), copy.start)

        when(self.valid(rel), body)

    def slot(self, route, phase, side, place):
        order, counts = self.orders[route], self.slot_counts[route]
        index = 0
        for j in range(phase):
            index = index * self.sizes[order[j]] + place[order[j]]
        n = self.sizes[order[phase]]
        if n > 2:
            index = (index * n + place[order[phase]]) * 2 + (1 if side > 0 else 0)
        return sum(counts[:phase]) + index

    def scatter(self, route, rel, ref_of, slots, add, send_sems, recv_sems):
        order = self.orders[route]

        def body():
            place = self.at(rel)
            ref = ref_of(place)
            base = self.slot_base[route]
            for phase, axis, step in onward(self.sizes, order, rel):
                slot = self.slot(route, phase, step, place)

                def take(axis=axis, step=step, slot=slot):
                    pltpu.make_async_remote_copy(
                        src_ref=ref,
                        dst_ref=slots.at[slot],
                        send_sem=send_sems.at[route],
                        recv_sem=recv_sems.at[base + slot],
                        device_id=self.device(axis, step),
                        device_id_type=MESH,
                    ).wait_recv()
                    add(ref, slots.at[slot])

                when(self.inside(axis, step), take)
            phase = last_axis(order, rel)
            if phase >= 0:
                axis, step = self.back_step(order, rel)
                slot = self.slot(route, phase, 1 if self.sizes[axis] == 2 else -step, place)
                pltpu.make_async_remote_copy(
                    src_ref=ref,
                    dst_ref=slots.at[slot],
                    send_sem=send_sems.at[route],
                    recv_sem=recv_sems.at[base + slot],
                    device_id=self.device(axis, step),
                    device_id_type=MESH,
                ).start()

        when(self.valid(rel), body)


def cut(bins, shares):
    edges = [0]
    for i in range(1, len(shares) + 1):
        edges.append(round(bins * sum(shares[:i]) / sum(shares)))
    return [(a, b - a) for a, b in zip(edges, edges[1:])]


GATHER_ORDERS = ((2, 0, 1), (0, 1, 2), (1, 2, 0), (2, 0, 1))
GATHER_SHARES = (10, 11, 4)
SCATTER_ORDERS = ((2, 0, 1), (0, 1, 2), (1, 2, 0), (2, 0, 1))
SCATTER_SHARES = (6, 16, 3)
HALO_AFTER = 4
EARLY, DURING, LAST = 18, 30, 8
GATHER_CODES = {
    (4, 2, 2): (
        84, 0, 56, 28, 1, 85, 58, 88, 4, 8, 57, 89, 29, 9, 36, 92, 32, 5, 86, 40, 64, 93, 97,
        16, 59, 12, 30, 38, 44, 65, 100, 37, 90, 24, 87, 17, 48, 13, 10, 61, 101, 63, 50, 34,
        18, 7, 66, 20, 42, 73, 96, 3, 2, 62, 6, 49, 26, 31, 60, 52, 39, 45, 104, 33, 95, 46, 69,
        25, 108, 21, 67, 91, 14, 68, 105, 109, 106, 41, 77, 54, 82, 76, 74, 71, 72, 53, 23, 94,
        75, 11, 111, 22, 70, 102, 19, 81, 107, 110, 27, 35, 99, 47, 98, 103, 15, 80, 79, 51, 78,
        43, 55, 83
    ),
}
SCATTER_CODES = {
    (4, 2, 2): (
        111, 26, 78, 23, 94, 51, 47, 106, 43, 35, 55, 99, 82, 37, 22, 80, 107, 110, 77, 81, 103,
        79, 18, 74, 27, 53, 109, 98, 11, 69, 73, 76, 83, 45, 24, 108, 7, 102, 101, 87, 61, 19,
        90, 95, 49, 75, 54, 66, 68, 25, 15, 100, 71, 63, 39, 104, 20, 70, 50, 72, 105, 10, 16,
        14, 91, 46, 65, 42, 41, 17, 2, 67, 92, 97, 31, 64, 33, 93, 29, 88, 21, 96, 6, 3, 52, 34,
        13, 48, 89, 9, 5, 12, 62, 40, 4, 38, 85, 60, 44, 8, 59, 1, 30, 32, 36, 58, 57, 86, 0,
        56, 28, 84
    ),
}


def unpack(codes, sizes):
    spans = [offsets(n) for n in sizes]
    events = []
    for code in codes:
        code, k = divmod(code, len(spans[2]))
        code, j = divmod(code, len(spans[1]))
        route, i = divmod(code, len(spans[0]))
        events.append((route, (spans[0][i], spans[1][j], spans[2][k])))
    return events


def step_kernel(grid, *refs):
    fields_ref, levels_ref, w1_ref, w2_ref, up_ref, fine_ref, coarse_ref = refs[:7]
    first_ref, second_ref = refs[7:9]
    (
        w_in,
        w2_in,
        w2_sets,
        wbuf,
        w2buf,
        fine_low,
        coarse_low,
        wide,
        stage,
        crops,
        up_all,
        upb,
        uptb,
        back,
        hidden,
        acts,
        pres,
        grads,
        seconds,
        out_first,
        out_second,
        swap,
        cells_v,
        geo_v,
        cells_ref,
        geo_ref,
        local_sems,
        send_sems,
        recv_sems,
        sum_send_sems,
        sum_recv_sems,
        core_send,
        core_recv,
    ) = refs[9:42]
    slot_refs = refs[42:]
    nz, nx, ny, cores = grid
    sizes = (nz, nx, ny)
    dp = lax.axis_index("dp")
    y = lax.axis_index("tile")
    core = dp % cores
    chip = dp // cores
    x = chip % nx
    z = chip // nx
    position = (z, x, y)
    other = 1 - core
    partner = (chip * cores + other, y)
    ways_in = Routes(sizes, position, core, cores, GATHER_ORDERS)
    ways_out = Routes(sizes, position, core, cores, SCATTER_ORDERS)
    h, share = w1_ref.shape
    lanes = wbuf.shape[1]
    bins = lanes // 128
    all_rows = nz * nx * h
    fine_rows, fine_cols, _ = fine_ref.shape
    coarse_rows, coarse_cols, _ = coarse_ref.shape
    batch, feats = crops.shape
    capacity = batch // cores
    depth = w2buf.shape[1]
    hidden_size = up_ref.shape[1]
    pair = cores * h
    starts = [min(t * share // 128, feats // 128 - bins) for t in range(ny)]
    shift = share - 128 * starts[1]
    parts_in = cut(bins, GATHER_SHARES)
    parts_out = cut(bins, SCATTER_SHARES)
    f32, low = jnp.float32, jnp.bfloat16

    barrier = pltpu.get_barrier_semaphore()
    pl.semaphore_signal(barrier, inc=1, device_id=partner, device_id_type=MESH)
    peers = 1
    for axis in range(3):
        for step in steps_of(sizes[axis]):

            def greet(axis=axis, step=step):
                pl.semaphore_signal(
                    barrier, inc=1, device_id=ways_in.device(axis, step), device_id_type=MESH
                )

            near = ways_in.inside(axis, step)
            when(near, greet)
            peers = peers + (near[0].astype(jnp.int32) if near else 1)

    def rows(start, size):
        return pl.ds(pl.multiple_of(start, size), size)

    def local(src, dst, i):
        copy = pltpu.make_async_copy(src, dst, local_sems.at[i])
        copy.start()
        return copy

    def remote(src, dst, i, device):
        return pltpu.make_async_remote_copy(
            src_ref=src,
            dst_ref=dst,
            send_sem=core_send.at[i],
            recv_sem=core_recv.at[i],
            device_id=device,
            device_id_type=MESH,
        )

    w_copy = local(w1_ref, w_in, 0)
    w2_copy = local(w2_ref, w2_in, 1)
    fine_copy = local(fine_ref, fine_low.at[pl.ds(0, fine_rows)], 2)
    coarse_copy = local(coarse_ref, coarse_low.at[pl.ds(0, coarse_rows)], 3)
    up_copy = local(up_ref, up_all, 4)
    halves = lax.broadcasted_iota(jnp.int32, (h, 128), 1)

    w_copy.wait()
    own_rows = pl.ds(pl.multiple_of(y * all_rows + chip * h, h), h)
    before = jnp.zeros((h, 128), f32)
    for i in range(bins):
        width = min(128, share - 128 * i)
        now = w_in[:, 128 * i : 128 * i + width].astype(f32)
        if width < 128:
            now = jnp.concatenate([now, jnp.zeros((h, 128 - width), f32)], axis=1)
        turned = pltpu.roll(now, shift, axis=1) if shift else now
        late = jnp.where(halves < shift, before, turned)
        before = turned
        wbuf[own_rows, 128 * i : 128 * (i + 1)] = jnp.where(y == 0, now, late).astype(low)

    w2_copy.wait()
    for m in range(depth // 128):
        a = w2_in[:, 256 * m : 256 * m + 128].astype(f32)
        b = w2_in[:, 256 * m + 128 : 256 * m + 256].astype(f32)
        at = slice(128 * m, 128 * (m + 1))
        w2_sets[0, :, at] = jnp.where(halves < h, a, pltpu.roll(b, h, axis=1)).astype(low)
        w2_sets[1, :, at] = jnp.where(halves < h, pltpu.roll(a, h, axis=1), b).astype(low)
    w2_rows = pl.ds(pl.multiple_of(y * hidden_size + chip * pair + core * h, h), h)
    w2buf[w2_rows, :] = w2_sets[core]

    pl.semaphore_wait(barrier, peers)
    w2_swap = remote(w2_sets.at[other], w2buf.at[w2_rows, :], 0, partner)

    last_in = len(GATHER_SHARES)
    last_out = len(SCATTER_SHARES)
    loads_in = [
        (order, parts_in[i][1] if i < last_in else depth * pair // (h * 128))
        for i, order in enumerate(GATHER_ORDERS)
    ]
    loads_out = [
        (order, parts_out[i][1] if i < last_out else depth * pair // (h * 128))
        for i, order in enumerate(SCATTER_ORDERS)
    ]
    halo_load = HALO * (fine_cols + coarse_cols) // h
    if sizes in GATHER_CODES:
        events = unpack(GATHER_CODES[sizes], sizes)
        sum_events = unpack(SCATTER_CODES[sizes], sizes)
    else:
        events = arrival_order(sizes, loads_in, (halo_load, (0,)))[0]
        sum_events = arrival_order(sizes, loads_out, (0, ()))[0][::-1]

    def gather_ref(route):
        if route == last_in:
            return lambda q: w2buf.at[
                rows(q[2] * hidden_size + (q[0] * nx + q[1]) * pair, pair), :
            ]
        first, count = parts_in[route]
        return lambda q: wbuf.at[
            rows(q[2] * all_rows + (q[0] * nx + q[1]) * h, h), pl.ds(first * 128, count * 128)
        ]

    def gather(event):
        route, rel = event
        ways_in.gather(route, rel, gather_ref(route), send_sems, recv_sems)

    w2_swap.start()
    below = ways_in.device(2, 1)
    fine_halo = remote(
        fine_ref.at[pl.ds(0, HALO)], fine_low.at[pl.ds(fine_rows, HALO)], 1, below
    )
    coarse_halo = remote(
        coarse_ref.at[pl.ds(0, HALO)], coarse_low.at[pl.ds(coarse_rows, HALO)], 2, below
    )
    own = [e for e in events if e[1] == (0, 0, 0)]
    todo = [e for e in events if e[1] != (0, 0, 0)]
    for n, event in enumerate(own):
        if event[0] == last_in:
            w2_swap.wait()
        gather(event)
        if n + 1 == HALO_AFTER:

            @pl.when(y == 1)
            def _():
                fine_halo.start()
                coarse_halo.start()

    member = jnp.logical_and(
        fields_ref[0:1, :] >= y * (4 * fine_rows), fields_ref[0:1, :] < (y + 1) * (4 * fine_rows)
    )
    props = fields_ref.shape[1]
    ones = jnp.broadcast_to(jnp.where(member, 1.0, 0.0), (8, props)).astype(low)
    upto = lax.broadcasted_iota(jnp.int32, (props, props), 0) <= lax.broadcasted_iota(
        jnp.int32, (props, props), 1
    )
    rank = jnp.dot(ones, jnp.where(upto, 1.0, 0.0).astype(low), preferred_element_type=f32)
    slot = jnp.where(member, rank[0:1, :] - 1.0, -1.0)
    slot_ids = lax.broadcasted_iota(jnp.int32, (capacity, props), 0).astype(f32)
    picks = jnp.where(slot == slot_ids, 1.0, 0.0).astype(low)

    def pick(ints):
        return lax.dot_general(
            ints.astype(f32).astype(low), picks, NT, preferred_element_type=f32
        )

    boxes = jnp.concatenate([fields_ref[...], fields_ref[...]], axis=0)
    values = 8.0 * pick(boxes >> 3) + pick(boxes & 7)
    level = pick(jnp.broadcast_to(levels_ref[...], (8, props)))[0:1, :]
    top, left, height, box_width = (values[i : i + 1, :] for i in range(4))
    is_fine = level < 0.5
    inverse = jnp.where(is_fine, 0.25, 0.125)
    span = jnp.where(is_fine, 28.0, 56.0)
    first_row = jnp.floor(top * inverse)
    band_rows = jnp.where(is_fine, 1.0 * fine_rows, 1.0 * coarse_rows)
    local_row = jnp.clip(first_row - y.astype(f32) * band_rows, 0.0, band_rows - 1.0)
    first_col = jnp.minimum(
        jnp.floor(left * inverse), jnp.where(is_fine, 1.0 * fine_cols, 1.0 * coarse_cols) - WIN
    )
    cells_v[0:1, :] = (local_row + jnp.where(is_fine, 0.0, 1.0 * (fine_rows + HALO))).astype(
        jnp.int32
    )
    cells_v[1:2, :] = first_col.astype(jnp.int32)
    geo_v[0:1, :] = top * inverse - first_row
    geo_v[1:2, :] = height / span
    geo_v[2:3, :] = left * inverse - first_col
    geo_v[3:4, :] = box_width / span
    up_copy.wait()
    half = rows(core * capacity, capacity)
    upb[half, :] = jnp.dot(picks, up_all[...], preferred_element_type=f32).astype(low)
    cells_copy = local(cells_v, cells_ref, 5)
    geo_copy = local(geo_v, geo_ref, 6)

    coarse_base = fine_rows + HALO

    def widen(source, first, count, base, cols):
        def one(r, carry):
            wide[base + r, 0:cols, :] = source[r].astype(f32)
            return carry

        lax.fori_loop(first, first + count, one, 0)

    fine_copy.wait()
    coarse_copy.wait()
    widen(fine_low, 0, fine_rows, 0, fine_cols)
    widen(coarse_low, 0, coarse_rows, coarse_base, coarse_cols)
    up_swap = remote(upb.at[half, :], upb.at[half, :], 3, partner)
    up_swap.start()

    for event in todo[:EARLY]:
        gather(event)

    @pl.when(y == 0)
    def _():
        fine_halo.wait_recv()
        coarse_halo.wait_recv()
        widen(fine_low, fine_rows, HALO, 0, fine_cols)
        widen(coarse_low, coarse_rows, HALO, coarse_base, coarse_cols)

    @pl.when(y == 1)
    def _():
        def clear(r, carry):
            wide[r] = jnp.zeros(wide.shape[1:], f32)
            return carry

        lax.fori_loop(fine_rows, fine_rows + HALO, clear, 0)
        lax.fori_loop(coarse_base + coarse_rows, coarse_base + coarse_rows + HALO, clear, 0)

    cells_copy.wait()
    geo_copy.wait()

    groups = capacity // GROUP
    during = todo[EARLY : EARLY + DURING]
    todo = todo[EARLY + DURING :]
    shape = (ROWS_PAD, REACH * WIN)
    k = lax.broadcasted_iota(jnp.int32, shape, 0).astype(f32)
    i_bin = jnp.floor((k + 0.5) * (1.0 / BINS))
    j_bin = k - BINS * i_bin
    i_mid = i_bin + 0.5
    j_mid = j_bin + 0.5
    lane = lax.broadcasted_iota(jnp.int32, shape, 1)
    r_cell = (lane >> 4).astype(f32)
    q_cell = (lane & 15).astype(f32)

    def crop_copy(first, count):
        crop_rows = pl.ds(pl.multiple_of(core * capacity + first, GROUP), count)
        return remote(crops.at[crop_rows, :], crops.at[crop_rows, :], 4, partner)

    def crop_group(g, carry):
        for n, event in enumerate(during):
            pl.when(g == n * groups // len(during))(functools.partial(gather, event))
        for p in range(GROUP):
            n = g * GROUP + p
            row = jnp.clip(cells_ref[0, n], 0, wide.shape[0] - REACH)
            col = jnp.clip(cells_ref[1, n], 0, fine_cols - WIN)
            row_w = jnp.maximum(0.0, 1.0 - jnp.abs(i_mid * geo_ref[1, n] + geo_ref[0, n] - r_cell))
            col_w = jnp.maximum(0.0, 1.0 - jnp.abs(j_mid * geo_ref[3, n] + geo_ref[2, n] - q_cell))
            weights = (row_w * col_w).astype(low)
            window = jnp.concatenate(
                [wide[row + r, pl.ds(col, WIN), :] for r in range(REACH)], axis=0
            ).astype(low)
            crop = jnp.dot(weights, window, preferred_element_type=f32)
            stage[pl.ds(p, ROWS_PAD, stride=GROUP), :] = crop
        group_rows = rows(core * capacity + g * GROUP, GROUP)
        for m in range(feats // 128):
            crops[group_rows, m * 128 : (m + 1) * 128] = stage[
                m * GROUP : (m + 1) * GROUP, :
            ].astype(low)

        @pl.when(g > 0)
        def _():
            crop_copy((g - 1) * GROUP, GROUP).start()

        return carry

    lax.fori_loop(0, groups, crop_group, 0)
    crop_copy((groups - 1) * GROUP, GROUP).start()

    for event in todo[:-LAST]:
        gather(event)
    up_swap.wait()

    def turn_up(i, carry):
        at = rows(i * 128, 128)
        uptb[at, :] = upb[:, at].astype(f32).T.astype(low)
        return carry

    lax.fori_loop(0, hidden_size // 128, turn_up, 0)
    for event in todo[-LAST:]:
        gather(event)
    for t in range(ny):
        part = jnp.dot(
            upb[...], w2buf[t * hidden_size : (t + 1) * hidden_size, :], preferred_element_type=f32
        )
        back[t * depth : (t + 1) * depth, :] = part.T
    crop_copy(0, capacity).wait()

    chunk = 640 if lanes % 640 == 0 else 128
    hidden[...] = jnp.zeros_like(hidden)
    for t in range(ny):

        def hide(i, carry, t=t):
            at = pl.multiple_of(i * chunk, 128)
            from_at = pl.multiple_of(starts[t] * 128 + i * chunk, 128)
            hidden[...] += lax.dot_general(
                wbuf[t * all_rows : (t + 1) * all_rows, pl.ds(at, chunk)],
                crops[:, pl.ds(from_at, chunk)],
                NT,
                preferred_element_type=f32,
            )
            return carry

        lax.fori_loop(0, lanes // chunk, hide, 0)

    def gelu(i, carry):
        at = rows(i * 32, 32)
        value, slope = gelu_parts(hidden[at, :])
        acts[at, :] = value.astype(low)
        pres[at, :] = (back[at, :] * slope).astype(low)
        return carry

    lax.fori_loop(0, hidden.shape[0] // 32, gelu, 0)

    def sum_ref(route):
        if route == last_out:
            return lambda q: seconds.at[
                rows(q[2] * hidden_size + (q[0] * nx + q[1]) * pair, pair), :
            ]
        first, count = parts_out[route]
        return lambda q: grads.at[
            rows(q[2] * all_rows + (q[0] * nx + q[1]) * h, h), pl.ds(first * 128, count * 128)
        ]

    def add(ref, more):
        def one(i, carry):
            at = rows(i * 16, 16)
            ref[at, :] = (ref[at, :].astype(f32) + more[at, :].astype(f32)).astype(low)
            return carry

        lax.fori_loop(0, ref.shape[0] // 16, one, 0)

    def make_grads(t, part):
        first, count = parts_out[part]
        step = max(c for c in range(1, 7) if count % c == 0)

        def one(i, carry):
            at = pl.multiple_of((first + i * step) * 128, 128)
            from_at = pl.multiple_of((starts[0] + t * (starts[1] - starts[0])) * 128 + at, 128)
            grads[rows(t * all_rows, all_rows), pl.ds(at, step * 128)] = jnp.dot(
                pres[...], crops[:, pl.ds(from_at, step * 128)], preferred_element_type=f32
            ).astype(low)
            return carry

        lax.fori_loop(0, count // step, one, 0)

    def make_seconds():
        for t in range(ny):
            seconds[t * hidden_size : (t + 1) * hidden_size, :] = lax.dot_general(
                uptb[...], acts[t * depth : (t + 1) * depth, :], NT, preferred_element_type=f32
            ).astype(low)

    made = set()
    for route, rel in sum_events:
        need = (route, rel[2] if route < last_out else 0)
        if need not in made:
            made.add(need)
            if route == last_out:
                make_seconds()
            else:
                make_grads(y if rel[2] == 0 else 1 - y, route)
        ways_out.scatter(
            route, rel, sum_ref(route), slot_refs[route], add, sum_send_sems, sum_recv_sems
        )

    own_second = y * hidden_size + chip * pair
    swap[0] = seconds[pl.ds(pl.multiple_of(own_second + other * h, h), h), :]
    second_swap = remote(swap.at[0], swap.at[1], 5, partner)
    second_swap.start()
    tile = grads[own_rows, 0:128].astype(f32)
    back_shift = (128 - shift) % 128
    now_turned = pltpu.roll(tile, back_shift, axis=1)
    for i in range(bins):
        width = min(128, share - 128 * i)
        following, next_turned = tile, now_turned
        if i + 1 < bins:
            following = grads[own_rows, 128 * (i + 1) : 128 * (i + 2)].astype(f32)
            next_turned = pltpu.roll(following, back_shift, axis=1)
        late = jnp.where(halves < 128 - shift, now_turned, next_turned)
        out_first[:, 128 * i : 128 * i + width] = jnp.where(y == 0, tile, late)[:, :width]
        tile, now_turned = following, next_turned
    first_out = local(out_first, first_ref, 0)
    second_swap.wait()
    for m in range(depth // 128):
        at = slice(128 * m, 128 * (m + 1))
        mine = seconds[pl.ds(pl.multiple_of(own_second + core * h, h), h), at].astype(f32)
        theirs = swap[1, :, at].astype(f32)
        set_0 = jnp.where(core == 0, mine, theirs)
        set_1 = jnp.where(core == 0, theirs, mine)
        out_second[:, 256 * m : 256 * m + 128] = jnp.where(
            halves < h, set_0, pltpu.roll(set_1, h, axis=1)
        )
        out_second[:, 256 * m + 128 : 256 * m + 256] = jnp.where(
            halves < h, pltpu.roll(set_0, h, axis=1), set_1
        )
    second_out = local(out_second, second_ref, 1)

    def whole(route, buf, other_buf, parts, last):
        if route == last:
            return lambda n: other_buf.at[pl.ds(0, n), :]
        first, count = parts[route]
        return lambda n: buf.at[pl.ds(0, n), pl.ds(first * 128, count * 128)]

    for route in range(last_in + 1):
        unit = pair if route == last_in else h
        ways_in.drain(route, whole(route, wbuf, w2buf, parts_in, last_in), unit, send_sems)
    for route in range(last_out + 1):
        unit = pair if route == last_out else h
        sent = whole(route, grads, seconds, parts_out, last_out)((nz * nx * ny - 1) * unit)
        pltpu.make_async_copy(sent, sent, sum_send_sems.at[route]).wait()

    @pl.when(y == 1)
    def _():
        fine_halo.wait_send()
        coarse_halo.wait_send()

    first_out.wait()
    second_out.wait()


def per_device_by_chips(
    grid, proposal_boxes, level_plan, fine_map, coarse_map, first_weight, second_weight, upstream
):
    nz, nx, ny, cores = grid
    chips = nz * nx
    props = level_plan.shape[1]
    capacity = props // ny
    fine_tile, coarse = fine_map[0], coarse_map[0]
    fine_rows, fine_cols, channels = fine_tile.shape
    coarse_rows = coarse.shape[0]
    share, h = first_weight.shape
    feats = share * ny
    bins = max(-(-((t + 1) * share) // 128) - t * share // 128 for t in range(ny))
    lanes = bins * 128
    hidden_size = upstream.shape[2]
    depth = second_weight.shape[0] // cores
    pair = cores * h
    low, f32 = jnp.bfloat16, jnp.float32
    sizes = (nz, nx, ny)
    parts_out = cut(bins, SCATTER_SHARES)
    slot_counts = [sum(slots_of(sizes, order)) for order in SCATTER_ORDERS]
    rows_all = chips * h
    batch = cores * capacity
    q = chips * ny
    dma = pltpu.SemaphoreType.DMA
    anywhere = pl.BlockSpec(memory_space=pl.ANY)
    vmem = pl.BlockSpec(memory_space=pltpu.VMEM)
    slot_shapes = [
        (n, h, parts_out[i][1] * 128) if i < len(parts_out) else (n, pair, depth)
        for i, n in enumerate(slot_counts)
    ]
    first, second = pl.pallas_call(
        functools.partial(step_kernel, grid),
        out_shape=(
            jax.ShapeDtypeStruct((h, share), f32),
            jax.ShapeDtypeStruct((h, cores * depth), f32),
        ),
        in_specs=[vmem, vmem] + [anywhere] * 5,
        out_specs=(anywhere, anywhere),
        scratch_shapes=[
            pltpu.VMEM((h, share), low),
            pltpu.VMEM((h, cores * depth), low),
            pltpu.VMEM((cores, h, depth), low),
            pltpu.VMEM((ny * rows_all, lanes), low),
            pltpu.VMEM((ny * hidden_size, depth), low),
            pltpu.VMEM((fine_rows + HALO, fine_cols, channels), low),
            pltpu.VMEM((coarse_rows + HALO, coarse.shape[1], channels), low),
            pltpu.VMEM((fine_rows + coarse_rows + 2 * HALO, fine_cols, channels), f32),
            pltpu.VMEM((ROWS_PAD * GROUP, 128), f32),
            pltpu.VMEM((batch, feats), low),
            pltpu.VMEM((props, hidden_size), low),
            pltpu.VMEM((batch, hidden_size), low),
            pltpu.VMEM((hidden_size, batch), low),
            pltpu.VMEM((rows_all, batch), f32),
            pltpu.VMEM((rows_all, batch), f32),
            pltpu.VMEM((rows_all, batch), low),
            pltpu.VMEM((rows_all, batch), low),
            pltpu.VMEM((ny * rows_all, lanes), low),
            pltpu.VMEM((ny * hidden_size, depth), low),
            pltpu.VMEM((h, share), f32),
            pltpu.VMEM((h, cores * depth), f32),
            pltpu.VMEM((2, h, depth), low),
            pltpu.VMEM((8, capacity), jnp.int32),
            pltpu.VMEM((8, capacity), f32),
            pltpu.SMEM((8, capacity), jnp.int32),
            pltpu.SMEM((8, capacity), f32),
            dma((7,)),
            dma((len(GATHER_ORDERS), 6)),
            dma((len(GATHER_ORDERS), q)),
            dma((len(SCATTER_ORDERS),)),
            dma((sum(slot_counts),)),
            dma((6,)),
            dma((6,)),
        ]
        + [pltpu.VMEM(shape, low) for shape in slot_shapes],
        compiler_params=pltpu.CompilerParams(
            collective_id=0, has_side_effects=True, vmem_limit_bytes=64000 * 1024
        ),
        name="step",
    )(
        proposal_boxes[0],
        level_plan,
        first_weight.T,
        second_weight.T,
        upstream[0],
        fine_tile,
        coarse,
    )
    return (first.T, second.T)


def solution(mesh):
    placed = (
        P("dp", None, None),
        P("dp", None),
        P("dp", "tile", None, None),
        P("dp", "tile", None, None),
        P("tile", "dp"),
        P("tile", "dp"),
        P("dp", None, None),
    )
    grid = chip_grid(mesh)
    tiles = mesh.shape["tile"]
    body = per_device_by_bands
    if grid is not None and tiles == 2 and grid[1] <= 2 and grid[2] == 2:
        body = functools.partial(per_device_by_chips, (grid[0], grid[1], tiles, grid[2]))
    return jax.shard_map(
        body,
        mesh=mesh,
        in_specs=placed,
        out_specs=(P("tile", "dp"), P("tile", "dp")),
        check_vma=False,
    )
```

```python
import functools

import jax
import jax.numpy as jnp
from jax import lax
from jax.experimental import pallas as pl
from jax.experimental.pallas import tpu as pltpu
from jax.sharding import PartitionSpec as P

WIN = 16
BINS = 7
ROWS_PAD = 56
GROUP = 16


def from_ahead(block, axis, distance):
    if distance == 0:
        return block
    size = lax.axis_size(axis)
    return lax.ppermute(block, axis, [(i, (i - distance) % size) for i in range(size)])


def halo_from_next(block, axis):
    size = lax.axis_size(axis)
    return lax.ppermute(block, axis, [(i + 1, i) for i in range(size - 1)])


def gelu_parts(hidden):
    factor = 0.7978845608028654
    cubic_term = 0.044715
    inner_term = factor * (hidden + cubic_term * hidden * hidden * hidden)
    tangent = jnp.tanh(inner_term)
    gelu_value = 0.5 * hidden * (1.0 + tangent)
    gelu_slope = 0.5 * (1.0 + tangent) + 0.5 * hidden * (1.0 - tangent * tangent) * factor * (
        1.0 + 3.0 * cubic_term * hidden * hidden
    )
    return (gelu_value, gelu_slope)


def crop_kernel(starts, width, cells_ref, geo_ref, maps_ref, out_ref, wide, stage):
    step = pl.program_id(0)

    @pl.when(step == 0)
    def _():
        def widen(r, carry):
            wide[r] = maps_ref[r].astype(jnp.float32)
            return carry

        lax.fori_loop(0, maps_ref.shape[0], widen, 0)

    shape = (ROWS_PAD, WIN * WIN)
    k = lax.broadcasted_iota(jnp.int32, shape, 0).astype(jnp.float32)
    i_bin = jnp.floor((k + 0.5) * (1.0 / BINS))
    j_bin = k - BINS * i_bin
    i_mid = i_bin + 0.5
    j_mid = j_bin + 0.5
    lane = lax.broadcasted_iota(jnp.int32, shape, 1)
    r_cell = (lane >> 4).astype(jnp.float32)
    q_cell = (lane & 15).astype(jnp.float32)
    for p in range(GROUP):
        n = step * GROUP + p
        row = cells_ref[0, n]
        col = cells_ref[1, n]
        row_w = jnp.maximum(0.0, 1.0 - jnp.abs(i_mid * geo_ref[1, n] + geo_ref[0, n] - r_cell))
        col_w = jnp.maximum(0.0, 1.0 - jnp.abs(j_mid * geo_ref[3, n] + geo_ref[2, n] - q_cell))
        weights = (row_w * col_w).astype(jnp.bfloat16)
        window = jnp.concatenate(
            [wide[row + r, pl.ds(col, WIN), :] for r in range(WIN)], axis=0
        ).astype(jnp.bfloat16)
        crop = jnp.dot(weights, window, preferred_element_type=jnp.float32)
        stage[pl.ds(p, ROWS_PAD, stride=GROUP), :] = crop
    for t, first in enumerate(starts):
        for m in range(width):
            at = (first + m) * GROUP
            out_ref[t, :, m * 128 : (m + 1) * 128] = stage[at : at + GROUP, :].astype(jnp.bfloat16)


def make_crops(cells, geo, maps, starts, width, capacity):
    tiles = len(starts)
    lanes = width * 128
    return pl.pallas_call(
        functools.partial(crop_kernel, starts, width),
        grid=(capacity // GROUP,),
        out_shape=jax.ShapeDtypeStruct((tiles, capacity, lanes), jnp.bfloat16),
        in_specs=[
            pl.BlockSpec(memory_space=pltpu.SMEM),
            pl.BlockSpec(memory_space=pltpu.SMEM),
            pl.BlockSpec(maps.shape, lambda g: (0, 0, 0)),
        ],
        out_specs=pl.BlockSpec((tiles, GROUP, lanes), lambda g: (0, g, 0)),
        scratch_shapes=[
            pltpu.VMEM(maps.shape, jnp.float32),
            pltpu.VMEM((ROWS_PAD * GROUP, 128), jnp.float32),
        ],
        compiler_params=pltpu.CompilerParams(
            dimension_semantics=("arbitrary",), vmem_limit_bytes=48 * 1024 * 1024
        ),
        cost_estimate=pl.CostEstimate(
            flops=capacity * ROWS_PAD * WIN * WIN * 128 * 16,
            bytes_accessed=2 * maps.size + 2 * tiles * capacity * lanes,
            transcendentals=0,
        ),
        name="crops",
    )(cells, geo, maps)


def per_device_by_bands(
    proposal_boxes, level_plan, fine_map, coarse_map, first_weight, second_weight, upstream
):
    tile_count = lax.axis_size("tile")
    band = lax.axis_index("tile")
    num_props = level_plan.shape[1]
    capacity = max(num_props // 4, num_props // tile_count)
    fine_tile = fine_map[0]
    coarse = coarse_map[0]
    fine_rows, fine_cols, channels = fine_tile.shape
    coarse_rows, coarse_cols = (coarse.shape[0], coarse.shape[1])

    top_rows = jnp.concatenate([fine_tile[:WIN], coarse[:WIN]], axis=1)
    below_rows = halo_from_next(top_rows, "tile")

    share_feats = first_weight.shape[0]
    feats = share_feats * tile_count
    width = max(
        -(-((t + 1) * share_feats) // 128) - t * share_feats // 128 for t in range(tile_count)
    )
    starts = [min(t * share_feats // 128, feats // 128 - width) for t in range(tile_count)]
    lanes = width * 128
    feat_off = band * share_feats - 128 * jnp.minimum(
        band * share_feats // 128, feats // 128 - width
    )

    first_rows = lax.dynamic_update_slice(
        jnp.zeros((first_weight.shape[1], lanes), jnp.bfloat16),
        first_weight.T,
        (0, feat_off),
    )
    both = lax.all_gather(
        jnp.concatenate([first_rows, second_weight.T], axis=1), "dp", axis=0, tiled=True
    )
    first_all = both[:, :lanes]
    second_all = both[:, lanes:]

    fields = proposal_boxes[0]
    levels = level_plan[0]
    owner = fields[0] // (4 * fine_rows)
    members = (owner[:, None] == jnp.arange(tile_count, dtype=jnp.int32)[None, :]).astype(jnp.int32)
    rank = jnp.sum((jnp.cumsum(members, axis=0) - 1) * members, axis=1)
    relative = lax.rem(owner - band + tile_count, tile_count)
    slot_id = relative * capacity + rank
    slots = tile_count * capacity
    chosen = slot_id[None, :] == jnp.arange(slots, dtype=jnp.int32)[:, None]
    upstream_slots = jnp.dot(
        chosen.astype(jnp.bfloat16), upstream[0], preferred_element_type=jnp.float32
    ).astype(jnp.bfloat16)
    mine = chosen[:capacity].astype(jnp.int32)
    top, left, height, box_width = (
        jnp.sum(mine * fields[f][None, :], axis=1) for f in range(4)
    )
    level = jnp.sum(mine * levels[None, :], axis=1)

    stride = jnp.where(level == 0, 4, 8).astype(jnp.int32)
    is_fine = level == 0
    first_row = top // stride
    local_row = jnp.clip(
        first_row - band * jnp.where(is_fine, fine_rows, coarse_rows),
        0,
        jnp.where(is_fine, fine_rows, coarse_rows) - 1,
    )
    first_col = jnp.minimum(left // stride, jnp.where(is_fine, fine_cols, coarse_cols) - WIN)
    cells = jnp.stack(
        [local_row + jnp.where(is_fine, 0, fine_rows + WIN), first_col], axis=0
    ).astype(jnp.int32)
    stride_float = stride.astype(jnp.float32)
    geo = jnp.stack(
        [
            top.astype(jnp.float32) / stride_float - first_row.astype(jnp.float32),
            height.astype(jnp.float32) / (7.0 * stride_float),
            left.astype(jnp.float32) / stride_float - first_col.astype(jnp.float32),
            box_width.astype(jnp.float32) / (7.0 * stride_float),
        ],
        axis=0,
    )

    side = ((0, 0), (0, fine_cols - coarse_cols), (0, 0))
    maps = jnp.concatenate(
        [
            fine_tile,
            below_rows[:, :fine_cols],
            jnp.pad(coarse, side),
            jnp.pad(below_rows[:, fine_cols:], side),
        ],
        axis=0,
    )
    crop_blocks = make_crops(cells, geo, maps, starts, width, capacity)
    own_feats = jnp.concatenate(
        [
            from_ahead(
                lax.dynamic_index_in_dim(
                    crop_blocks, lax.rem(band - d + tile_count, tile_count), 0, keepdims=False
                ),
                "tile",
                d,
            )
            for d in range(tile_count)
        ],
        axis=0,
    )

    partial_hidden = lax.dot_general(
        own_feats, first_all, (((1,), (1,)), ((), ())), preferred_element_type=jnp.float32
    ).astype(jnp.bfloat16)
    share = second_weight.shape[0]

    def in_my_order(block, d):
        return jnp.roll(block, d * capacity, axis=0) if d else block

    hidden_own = 0.0
    for d in range(tile_count):
        to = lax.rem(band - d + tile_count, tile_count)
        piece = lax.dynamic_slice_in_dim(partial_hidden, to * share, share, axis=1)
        hidden_own = hidden_own + in_my_order(from_ahead(piece, "tile", d), d).astype(jnp.float32)
    gelu_value, gelu_slope = gelu_parts(hidden_own)
    activated = gelu_value.astype(jnp.bfloat16)
    back_grad = jnp.dot(upstream_slots, second_all, preferred_element_type=jnp.float32)
    pre_own = (back_grad * gelu_slope).astype(jnp.bfloat16)
    ahead = [in_my_order(from_ahead(pre_own, "tile", d), d) for d in range(tile_count)]
    twice = jnp.concatenate(ahead + ahead[:-1], axis=1)
    pre_grad = lax.dynamic_slice_in_dim(
        twice, lax.rem(tile_count - band, tile_count) * share, tile_count * share, axis=1
    )
    over_rows = (((0,), (0,)), ((), ()))
    second_part = lax.dot_general(
        upstream_slots, activated, over_rows, preferred_element_type=jnp.float32
    ).astype(jnp.bfloat16)
    first_part = lax.dot_general(
        pre_grad, own_feats, over_rows, preferred_element_type=jnp.float32
    ).astype(jnp.bfloat16)
    summed = lax.psum_scatter(
        jnp.concatenate([first_part, second_part], axis=1), "dp", scatter_dimension=0, tiled=True
    ).astype(jnp.float32)
    first_grad = lax.dynamic_slice_in_dim(summed[:, :lanes], feat_off, share_feats, axis=1).T
    second_grad = summed[:, lanes:].T
    return (first_grad, second_grad)


MESH = pl.DeviceIdType.MESH
REACH = 15
HALO = REACH - 1
NT = (((1,), (1,)), ((), ()))
NN = (((1,), (0,)), ((), ()))


def chip_grid(mesh):
    chips = [getattr(device, "coords", None) for device in mesh.devices[:, 0]]
    if chips[0] is None:
        return None
    cores = sum(1 for c in chips if tuple(c) == tuple(chips[0]))
    chips = [tuple(c) for c in chips[::cores]]
    if len(chips) == 1:
        return (1, 1, cores)
    axis = [a != b for a, b in zip(chips[0], chips[1])].index(True)
    fast = 1
    while fast < len(chips) and all(
        a == b or i == axis for i, (a, b) in enumerate(zip(chips[0], chips[fast]))
    ):
        fast += 1
    return (len(chips) // fast, fast, cores)


def offsets(size):
    if size == 1:
        return [0]
    if size == 2:
        return [0, 1]
    return [0] + [s * d for d in range(1, size) for s in (-1, 1)]


def steps_of(size):
    return {1: [], 2: [1]}.get(size, [-1, 1])


def moved(position, size, rel):
    if rel == 0 or size == 1:
        return position
    return 1 - position if size == 2 else position + rel


def last_axis(order, rel):
    used = [j for j in range(3) if rel[order[j]]]
    return used[-1] if used else -1


def onward(sizes, order, rel):
    last = last_axis(order, rel)
    hops = []
    if last >= 0:
        axis = order[last]
        if sizes[axis] > 2 and abs(rel[axis]) < sizes[axis] - 1:
            hops.append((last, axis, -1 if rel[axis] > 0 else 1))
    for j in range(last + 1, 3):
        hops.extend((j, order[j], step) for step in steps_of(sizes[order[j]]))
    return hops


def arrival_order(sizes, routes, extra):
    import heapq
    import itertools

    places = list(itertools.product(*(range(n) for n in sizes)))
    queue, waiting, busy = [], {}, set()
    seen, tick = {}, itertools.count()

    def start(link, now):
        if link not in busy and waiting.get(link):
            busy.add(link)
            load, arrival = waiting[link].pop(0)
            heapq.heappush(queue, (now + load, next(tick), link, arrival))

    def arrive(place, route, rel, now):
        seen.setdefault((route, rel), []).append(now)
        for _, axis, step in onward(sizes, routes[route][0], rel):
            target = list(place)
            target[axis] = moved(place[axis], sizes[axis], step)
            if not 0 <= target[axis] < sizes[axis]:
                continue
            there = list(rel)
            there[axis] = rel[axis] - step if sizes[axis] > 2 else 1
            link = (place, axis, step)
            waiting.setdefault(link, []).append(
                (routes[route][1], (tuple(target), route, tuple(there)))
            )
            start(link, now)

    first = {}
    for place in places:
        for route in extra[1]:
            arrive(place, route, (0, 0, 0), 0.0)
        if extra[0] and place[2] == 1:
            waiting.setdefault((place, 2, 1), []).append((extra[0], None))
            start((place, 2, 1), 0.0)
        for route in range(len(routes)):
            if route not in extra[1]:
                arrive(place, route, (0, 0, 0), 0.0)
    end = 0.0
    while queue:
        now, _, link, arrival = heapq.heappop(queue)
        end = now
        busy.discard(link)
        if arrival is not None:
            arrive(*arrival, now)
        start(link, now)
    key = {event: sum(t) / len(t) for event, t in seen.items()}
    for _ in range(sum(sizes)):
        for (route, rel) in list(key):
            for _, axis, step in onward(sizes, routes[route][0], rel):
                there = list(rel)
                there[axis] = rel[axis] - step if sizes[axis] > 2 else 1
                event = (route, tuple(there))
                if event in key:
                    key[event] = max(key[event], key[(route, rel)] + 1e-3)
    return sorted(key, key=lambda e: (key[e], e)), key, end


def slots_of(sizes, order):
    counts, before = [], 1
    for j in range(3):
        n = sizes[order[j]]
        counts.append(before * (2 * n if n > 2 else 1))
        before *= n
    return counts


def when(conds, body):
    if not conds:
        body()
        return
    total = conds[0]
    for cond in conds[1:]:
        total = jnp.logical_and(total, cond)
    pl.when(total)(body)


class Routes:
    def __init__(self, sizes, position, core, cores, orders):
        self.sizes, self.position = sizes, position
        self.core, self.cores = core, cores
        self.orders = orders
        self.slot_counts = [slots_of(sizes, order) for order in orders]
        self.slot_base = [sum(sum(c) for c in self.slot_counts[:i]) for i in range(len(orders))]

    def inside(self, axis, rel):
        if rel == 0 or self.sizes[axis] <= 2:
            return []
        p = self.position[axis]
        return [p < self.sizes[axis] - rel] if rel > 0 else [p >= -rel]

    def valid(self, rel):
        return sum((self.inside(axis, rel[axis]) for axis in range(3)), [])

    def at(self, rel):
        return [moved(self.position[a], self.sizes[a], rel[a]) for a in range(3)]

    def device(self, axis, step):
        there = list(self.position)
        there[axis] = moved(there[axis], self.sizes[axis], step)
        return ((there[0] * self.sizes[1] + there[1]) * self.cores + self.core, there[2])

    def back_step(self, order, rel):
        axis = order[last_axis(order, rel)]
        return axis, (1 if self.sizes[axis] == 2 or rel[axis] > 0 else -1)

    def number(self, place):
        return (place[0] * self.sizes[1] + place[1]) * self.sizes[2] + place[2]

    def direction(self, axis, step):
        return 2 * axis + (1 if step > 0 else 0)

    def drain(self, route, whole, unit, sems):
        order, before = self.orders[route], 1
        for axis in order:
            n, p = self.sizes[axis], self.position[axis]
            for step in steps_of(n):
                for at in range(n) if n > 2 else [0]:
                    sent = before * ((at + 1 if step > 0 else n - at) if n > 2 else 1)
                    if n > 2 and not 0 <= at + step < n:
                        continue

                    def wait(axis=axis, step=step, sent=sent):
                        part = whole(sent * unit)
                        pltpu.make_async_copy(
                            part, part, sems.at[route, self.direction(axis, step)]
                        ).wait()

                    when([p == at] if n > 2 else [], wait)
            before *= n

    def gather(self, route, rel, ref_of, send_sems, recv_sems):
        order = self.orders[route]

        def body():
            place = self.at(rel)
            ref = ref_of(place)
            q = self.number(place)

            def hop(axis, step):
                return pltpu.make_async_remote_copy(
                    src_ref=ref,
                    dst_ref=ref,
                    send_sem=send_sems.at[route, self.direction(axis, step)],
                    recv_sem=recv_sems.at[route, q],
                    device_id=self.device(axis, step),
                    device_id_type=MESH,
                )

            if last_axis(order, rel) >= 0:
                hop(*self.back_step(order, rel)).wait_recv()
            for _, axis, step in onward(self.sizes, order, rel):
                copy = hop(axis, step)
                when(self.inside(axis, step), copy.start)

        when(self.valid(rel), body)

    def slot(self, route, phase, side, place):
        order, counts = self.orders[route], self.slot_counts[route]
        index = 0
        for j in range(phase):
            index = index * self.sizes[order[j]] + place[order[j]]
        n = self.sizes[order[phase]]
        if n > 2:
            index = (index * n + place[order[phase]]) * 2 + (1 if side > 0 else 0)
        return sum(counts[:phase]) + index

    def scatter(self, route, rel, ref_of, slots, add, send_sems, recv_sems):
        order = self.orders[route]

        def body():
            place = self.at(rel)
            ref = ref_of(place)
            base = self.slot_base[route]
            for phase, axis, step in onward(self.sizes, order, rel):
                slot = self.slot(route, phase, step, place)

                def take(axis=axis, step=step, slot=slot):
                    pltpu.make_async_remote_copy(
                        src_ref=ref,
                        dst_ref=slots.at[slot],
                        send_sem=send_sems.at[route],
                        recv_sem=recv_sems.at[base + slot],
                        device_id=self.device(axis, step),
                        device_id_type=MESH,
                    ).wait_recv()
                    add(ref, slots.at[slot])

                when(self.inside(axis, step), take)
            phase = last_axis(order, rel)
            if phase >= 0:
                axis, step = self.back_step(order, rel)
                slot = self.slot(route, phase, 1 if self.sizes[axis] == 2 else -step, place)
                pltpu.make_async_remote_copy(
                    src_ref=ref,
                    dst_ref=slots.at[slot],
                    send_sem=send_sems.at[route],
                    recv_sem=recv_sems.at[base + slot],
                    device_id=self.device(axis, step),
                    device_id_type=MESH,
                ).start()

        when(self.valid(rel), body)


def cut(bins, shares):
    edges = [0]
    for i in range(1, len(shares) + 1):
        edges.append(round(bins * sum(shares[:i]) / sum(shares)))
    return [(a, b - a) for a, b in zip(edges, edges[1:])]


GATHER_ORDERS = ((2, 0, 1), (0, 1, 2), (1, 2, 0), (2, 0, 1))
GATHER_SHARES = (10, 11, 4)
SCATTER_ORDERS = ((2, 0, 1), (0, 1, 2), (1, 2, 0), (2, 0, 1))
SCATTER_SHARES = (6, 16, 3)
HALO_AFTER = 4
EARLY, DURING = 18, 30
GATHER_CODES = {
    (4, 2, 2): (
        84, 0, 56, 28, 1, 85, 58, 88, 4, 8, 57, 89, 29, 9, 36, 92, 32, 5, 86, 40, 64, 93, 97,
        16, 59, 12, 30, 38, 44, 65, 100, 37, 90, 24, 87, 17, 48, 13, 10, 61, 101, 63, 50, 34,
        18, 7, 66, 20, 42, 73, 96, 3, 2, 62, 6, 49, 26, 31, 60, 52, 39, 45, 104, 33, 95, 46, 69,
        25, 108, 21, 67, 91, 14, 68, 105, 109, 106, 41, 77, 54, 82, 76, 74, 71, 72, 53, 23, 94,
        75, 11, 111, 22, 70, 102, 19, 81, 107, 110, 27, 35, 99, 47, 98, 103, 15, 80, 79, 51, 78,
        43, 55, 83
    ),
}
SCATTER_CODES = {
    (4, 2, 2): (
        111, 26, 78, 23, 94, 51, 47, 106, 43, 35, 55, 99, 82, 37, 22, 80, 107, 110, 77, 81, 103,
        79, 18, 74, 27, 53, 109, 98, 11, 69, 73, 76, 83, 45, 24, 108, 7, 102, 101, 87, 61, 19,
        90, 95, 49, 75, 54, 66, 68, 25, 15, 100, 71, 63, 39, 104, 20, 70, 50, 72, 105, 10, 16,
        14, 91, 46, 65, 42, 41, 17, 2, 67, 92, 97, 31, 64, 33, 93, 29, 88, 21, 96, 6, 3, 52, 34,
        13, 48, 89, 9, 5, 12, 62, 40, 4, 38, 85, 60, 44, 8, 59, 1, 30, 32, 36, 58, 57, 86, 0,
        56, 28, 84
    ),
}


def unpack(codes, sizes):
    spans = [offsets(n) for n in sizes]
    events = []
    for code in codes:
        code, k = divmod(code, len(spans[2]))
        code, j = divmod(code, len(spans[1]))
        route, i = divmod(code, len(spans[0]))
        events.append((route, (spans[0][i], spans[1][j], spans[2][k])))
    return events


def step_kernel(grid, *refs):
    fields_ref, levels_ref, w1_ref, w2_ref, up_ref, fine_ref, coarse_ref = refs[:7]
    first_ref, second_ref = refs[7:9]
    (
        w_in,
        w2_in,
        w2_sets,
        wbuf,
        w2buf,
        fine_low,
        coarse_low,
        wide,
        stage,
        crops,
        up_all,
        upb,
        uptb,
        back,
        hidden,
        acts,
        pres,
        grads,
        seconds,
        swap,
        cells_v,
        geo_v,
        cells_ref,
        geo_ref,
        local_sems,
        send_sems,
        recv_sems,
        sum_send_sems,
        sum_recv_sems,
        core_send,
        core_recv,
    ) = refs[9:40]
    slot_refs = refs[40:]
    nz, nx, ny, cores = grid
    sizes = (nz, nx, ny)
    dp = lax.axis_index("dp")
    y = lax.axis_index("tile")
    core = dp % cores
    chip = dp // cores
    x = chip % nx
    z = chip // nx
    position = (z, x, y)
    other = 1 - core
    partner = (chip * cores + other, y)
    ways_in = Routes(sizes, position, core, cores, GATHER_ORDERS)
    ways_out = Routes(sizes, position, core, cores, SCATTER_ORDERS)
    h, share = w1_ref.shape
    lanes = wbuf.shape[1]
    bins = lanes // 128
    all_rows = nz * nx * h
    fine_rows, fine_cols, _ = fine_ref.shape
    coarse_rows, coarse_cols, _ = coarse_ref.shape
    batch, feats = crops.shape
    capacity = batch // cores
    depth = w2buf.shape[1]
    hidden_size = up_ref.shape[1]
    pair = cores * h
    starts = [min(t * share // 128, feats // 128 - bins) for t in range(ny)]
    shift = share - 128 * starts[1]
    parts_in = cut(bins, GATHER_SHARES)
    parts_out = cut(bins, SCATTER_SHARES)
    f32, low = jnp.float32, jnp.bfloat16

    barrier = pltpu.get_barrier_semaphore()
    pl.semaphore_signal(barrier, inc=1, device_id=partner, device_id_type=MESH)
    peers = 1
    for axis in range(3):
        for step in steps_of(sizes[axis]):

            def greet(axis=axis, step=step):
                pl.semaphore_signal(
                    barrier, inc=1, device_id=ways_in.device(axis, step), device_id_type=MESH
                )

            near = ways_in.inside(axis, step)
            when(near, greet)
            peers = peers + (near[0].astype(jnp.int32) if near else 1)

    def rows(start, size):
        return pl.ds(pl.multiple_of(start, size), size)

    def local(src, dst, i):
        copy = pltpu.make_async_copy(src, dst, local_sems.at[i])
        copy.start()
        return copy

    def remote(src, dst, i, device):
        return pltpu.make_async_remote_copy(
            src_ref=src,
            dst_ref=dst,
            send_sem=core_send.at[i],
            recv_sem=core_recv.at[i],
            device_id=device,
            device_id_type=MESH,
        )

    w_copy = local(w1_ref, w_in, 0)
    w2_copy = local(w2_ref, w2_in, 1)
    fine_copy = local(fine_ref, fine_low.at[pl.ds(0, fine_rows)], 2)
    coarse_copy = local(coarse_ref, coarse_low.at[pl.ds(0, coarse_rows)], 3)
    up_copy = local(up_ref, up_all, 4)
    halves = lax.broadcasted_iota(jnp.int32, (h, 128), 1)

    w_copy.wait()
    own_rows = pl.ds(pl.multiple_of(y * all_rows + chip * h, h), h)
    before = jnp.zeros((h, 128), f32)
    for i in range(bins):
        width = min(128, share - 128 * i)
        now = w_in[:, 128 * i : 128 * i + width].astype(f32)
        if width < 128:
            now = jnp.concatenate([now, jnp.zeros((h, 128 - width), f32)], axis=1)
        turned = pltpu.roll(now, shift, axis=1) if shift else now
        late = jnp.where(halves < shift, before, turned)
        before = turned
        wbuf[own_rows, 128 * i : 128 * (i + 1)] = jnp.where(y == 0, now, late).astype(low)

    w2_copy.wait()
    for m in range(depth // 128):
        a = w2_in[:, 256 * m : 256 * m + 128].astype(f32)
        b = w2_in[:, 256 * m + 128 : 256 * m + 256].astype(f32)
        at = slice(128 * m, 128 * (m + 1))
        w2_sets[0, :, at] = jnp.where(halves < h, a, pltpu.roll(b, h, axis=1)).astype(low)
        w2_sets[1, :, at] = jnp.where(halves < h, pltpu.roll(a, h, axis=1), b).astype(low)
    w2_rows = pl.ds(pl.multiple_of(y * hidden_size + chip * pair + core * h, h), h)
    w2buf[w2_rows, :] = w2_sets[core]

    pl.semaphore_wait(barrier, peers)
    w2_swap = remote(w2_sets.at[other], w2buf.at[w2_rows, :], 0, partner)

    last_in = len(GATHER_SHARES)
    last_out = len(SCATTER_SHARES)
    cols_in = depth // (len(GATHER_ORDERS) - last_in)
    cols_out = depth // (len(SCATTER_ORDERS) - last_out)
    loads_in = [
        (order, parts_in[i][1] if i < last_in else cols_in * pair // (h * 128))
        for i, order in enumerate(GATHER_ORDERS)
    ]
    loads_out = [
        (order, parts_out[i][1] if i < last_out else cols_out * pair // (h * 128))
        for i, order in enumerate(SCATTER_ORDERS)
    ]
    halo_load = HALO * (fine_cols + coarse_cols) // h
    if sizes in GATHER_CODES:
        events = unpack(GATHER_CODES[sizes], sizes)
        sum_events = unpack(SCATTER_CODES[sizes], sizes)
    else:
        events = arrival_order(sizes, loads_in, (halo_load, (0,)))[0]
        sum_events = arrival_order(sizes, loads_out, (0, ()))[0][::-1]

    def gather_ref(route):
        if route >= last_in:
            return lambda q: w2buf.at[
                rows(q[2] * hidden_size + (q[0] * nx + q[1]) * pair, pair),
                pl.ds((route - last_in) * cols_in, cols_in),
            ]
        first, count = parts_in[route]
        return lambda q: wbuf.at[
            rows(q[2] * all_rows + (q[0] * nx + q[1]) * h, h), pl.ds(first * 128, count * 128)
        ]

    def gather(event):
        route, rel = event
        ways_in.gather(route, rel, gather_ref(route), send_sems, recv_sems)

    w2_swap.start()
    below = ways_in.device(2, 1)
    fine_halo = remote(
        fine_ref.at[pl.ds(0, HALO)], fine_low.at[pl.ds(fine_rows, HALO)], 1, below
    )
    coarse_halo = remote(
        coarse_ref.at[pl.ds(0, HALO)], coarse_low.at[pl.ds(coarse_rows, HALO)], 2, below
    )
    own = [e for e in events if e[1] == (0, 0, 0)]
    todo = [e for e in events if e[1] != (0, 0, 0)]
    events = own + todo
    swapped = False
    for n, event in enumerate(own):
        if event[0] >= last_in and not swapped:
            swapped = True
            w2_swap.wait()
        gather(event)
        if n + 1 == HALO_AFTER:

            @pl.when(y == 1)
            def _():
                fine_halo.start()
                coarse_halo.start()

    member = jnp.logical_and(
        fields_ref[0:1, :] >= y * (4 * fine_rows), fields_ref[0:1, :] < (y + 1) * (4 * fine_rows)
    )
    props = fields_ref.shape[1]
    ones = jnp.broadcast_to(jnp.where(member, 1.0, 0.0), (8, props)).astype(low)
    upto = lax.broadcasted_iota(jnp.int32, (props, props), 0) <= lax.broadcasted_iota(
        jnp.int32, (props, props), 1
    )
    rank = jnp.dot(ones, jnp.where(upto, 1.0, 0.0).astype(low), preferred_element_type=f32)
    slot = jnp.where(member, rank[0:1, :] - 1.0, -1.0)
    slot_ids = lax.broadcasted_iota(jnp.int32, (capacity, props), 0).astype(f32)
    picks = jnp.where(slot == slot_ids, 1.0, 0.0).astype(low)

    def pick(ints):
        return lax.dot_general(
            ints.astype(f32).astype(low), picks, NT, preferred_element_type=f32
        )

    boxes = jnp.concatenate([fields_ref[...], fields_ref[...]], axis=0)
    values = 8.0 * pick(boxes >> 3) + pick(boxes & 7)
    level = pick(jnp.broadcast_to(levels_ref[...], (8, props)))[0:1, :]
    top, left, height, box_width = (values[i : i + 1, :] for i in range(4))
    is_fine = level < 0.5
    inverse = jnp.where(is_fine, 0.25, 0.125)
    span = jnp.where(is_fine, 28.0, 56.0)
    first_row = jnp.floor(top * inverse)
    band_rows = jnp.where(is_fine, 1.0 * fine_rows, 1.0 * coarse_rows)
    local_row = jnp.clip(first_row - y.astype(f32) * band_rows, 0.0, band_rows - 1.0)
    first_col = jnp.minimum(
        jnp.floor(left * inverse), jnp.where(is_fine, 1.0 * fine_cols, 1.0 * coarse_cols) - WIN
    )
    cells_v[0:1, :] = (local_row + jnp.where(is_fine, 0.0, 1.0 * (fine_rows + HALO))).astype(
        jnp.int32
    )
    cells_v[1:2, :] = first_col.astype(jnp.int32)
    geo_v[0:1, :] = top * inverse - first_row
    geo_v[1:2, :] = height / span
    geo_v[2:3, :] = left * inverse - first_col
    geo_v[3:4, :] = box_width / span
    up_copy.wait()
    half = rows(core * capacity, capacity)
    upb[half, :] = jnp.dot(picks, up_all[...], preferred_element_type=f32).astype(low)
    cells_copy = local(cells_v, cells_ref, 5)
    geo_copy = local(geo_v, geo_ref, 6)

    coarse_base = fine_rows + HALO

    def widen(source, first, count, base, cols):
        def one(r, carry):
            wide[base + r, 0:cols, :] = source[r].astype(f32)
            return carry

        lax.fori_loop(first, first + count, one, 0)

    fine_copy.wait()
    coarse_copy.wait()
    widen(fine_low, 0, fine_rows, 0, fine_cols)
    widen(coarse_low, 0, coarse_rows, coarse_base, coarse_cols)
    up_swap = remote(upb.at[half, :], upb.at[half, :], 3, partner)
    up_swap.start()

    for event in todo[:EARLY]:
        gather(event)
    up_swap.wait()

    def turn_up(i, carry):
        at = rows(i * 128, 128)
        uptb[at, :] = upb[:, at].astype(f32).T.astype(low)
        return carry

    lax.fori_loop(0, hidden_size // 128, turn_up, 0)

    @pl.when(y == 0)
    def _():
        fine_halo.wait_recv()
        coarse_halo.wait_recv()
        widen(fine_low, fine_rows, HALO, 0, fine_cols)
        widen(coarse_low, coarse_rows, HALO, coarse_base, coarse_cols)

    @pl.when(y == 1)
    def _():
        def clear(r, carry):
            wide[r] = jnp.zeros(wide.shape[1:], f32)
            return carry

        lax.fori_loop(fine_rows, fine_rows + HALO, clear, 0)
        lax.fori_loop(coarse_base + coarse_rows, coarse_base + coarse_rows + HALO, clear, 0)

    cells_copy.wait()
    geo_copy.wait()

    groups = capacity // GROUP
    during = todo[EARLY : EARLY + DURING]
    shape = (ROWS_PAD, REACH * WIN)
    k = lax.broadcasted_iota(jnp.int32, shape, 0).astype(f32)
    i_bin = jnp.floor((k + 0.5) * (1.0 / BINS))
    j_bin = k - BINS * i_bin
    i_mid = i_bin + 0.5
    j_mid = j_bin + 0.5
    lane = lax.broadcasted_iota(jnp.int32, shape, 1)
    r_cell = (lane >> 4).astype(f32)
    q_cell = (lane & 15).astype(f32)

    def crop_copy(first, count):
        crop_rows = pl.ds(pl.multiple_of(core * capacity + first, GROUP), count)
        return remote(crops.at[crop_rows, :], crops.at[crop_rows, :], 4, partner)

    def crop_group(g, carry):
        for n, event in enumerate(during):
            pl.when(g == n * groups // len(during))(functools.partial(gather, event))
        for p in range(GROUP):
            n = g * GROUP + p
            row = jnp.clip(cells_ref[0, n], 0, wide.shape[0] - REACH)
            col = jnp.clip(cells_ref[1, n], 0, fine_cols - WIN)
            row_w = jnp.maximum(0.0, 1.0 - jnp.abs(i_mid * geo_ref[1, n] + geo_ref[0, n] - r_cell))
            col_w = jnp.maximum(0.0, 1.0 - jnp.abs(j_mid * geo_ref[3, n] + geo_ref[2, n] - q_cell))
            weights = (row_w * col_w).astype(low)
            window = jnp.concatenate(
                [wide[row + r, pl.ds(col, WIN), :] for r in range(REACH)], axis=0
            ).astype(low)
            crop = jnp.dot(weights, window, preferred_element_type=f32)
            stage[pl.ds(p, ROWS_PAD, stride=GROUP), :] = crop
        group_rows = rows(core * capacity + g * GROUP, GROUP)
        for m in range(feats // 128):
            crops[group_rows, m * 128 : (m + 1) * 128] = stage[
                m * GROUP : (m + 1) * GROUP, :
            ].astype(low)

        @pl.when(g > 0)
        def _():
            crop_copy((g - 1) * GROUP, GROUP).start()

        return carry

    lax.fori_loop(0, groups, crop_group, 0)
    crop_copy((groups - 1) * GROUP, GROUP).start()

    def hide(ahead, route, begun):
        t = y if ahead == 0 else 1 - y
        first, count = parts_in[route]
        from_at = (starts[0] + t * (starts[1] - starts[0]) + first) * 128
        part = lax.dot_general(
            wbuf[rows(t * all_rows, all_rows), first * 128 : (first + count) * 128],
            crops[:, pl.ds(pl.multiple_of(from_at, 128), count * 128)],
            NT,
            preferred_element_type=f32,
        )
        hidden[...] = hidden[...] + part if begun else part

    ends = {(rel[2], route): i for i, (route, rel) in enumerate(events) if route < last_in}
    ready = [(i, key) for key, i in ends.items()]
    passed = len(own) + EARLY + DURING
    waited, begun = False, False
    for i in range(passed - 1, len(events)):
        if i >= passed:
            gather(events[i])
        for key in [k for end, k in sorted(ready) if end == i or (i == passed - 1 and end < i)]:
            if not waited:
                waited = True
                crop_copy(0, capacity).wait()
            hide(*key, begun)
            begun = True
    for t in range(ny):
        part = jnp.dot(
            upb[...], w2buf[t * hidden_size : (t + 1) * hidden_size, :], preferred_element_type=f32
        )
        back[t * depth : (t + 1) * depth, :] = part.T

    def gelu(i, carry):
        at = rows(i * 32, 32)
        value, slope = gelu_parts(hidden[at, :])
        acts[at, :] = value.astype(low)
        pres[at, :] = (back[at, :] * slope).astype(low)
        return carry

    lax.fori_loop(0, hidden.shape[0] // 32, gelu, 0)

    def sum_ref(route):
        if route >= last_out:
            return lambda q: seconds.at[
                rows(q[2] * hidden_size + (q[0] * nx + q[1]) * pair, pair),
                pl.ds((route - last_out) * cols_out, cols_out),
            ]
        first, count = parts_out[route]
        return lambda q: grads.at[
            rows(q[2] * all_rows + (q[0] * nx + q[1]) * h, h), pl.ds(first * 128, count * 128)
        ]

    def add(ref, more):
        def one(i, carry):
            at = rows(i * 16, 16)
            ref[at, :] = (ref[at, :].astype(f32) + more[at, :].astype(f32)).astype(low)
            return carry

        lax.fori_loop(0, ref.shape[0] // 16, one, 0)

    def make_grads(t, part):
        first, count = parts_out[part]
        step = max(c for c in range(1, 7) if count % c == 0)

        def one(i, carry):
            at = pl.multiple_of((first + i * step) * 128, 128)
            from_at = pl.multiple_of((starts[0] + t * (starts[1] - starts[0])) * 128 + at, 128)
            grads[rows(t * all_rows, all_rows), pl.ds(at, step * 128)] = jnp.dot(
                pres[...], crops[:, pl.ds(from_at, step * 128)], preferred_element_type=f32
            ).astype(low)
            return carry

        lax.fori_loop(0, count // step, one, 0)

    def make_seconds():
        for t in range(ny):
            seconds[t * hidden_size : (t + 1) * hidden_size, :] = lax.dot_general(
                uptb[...], acts[t * depth : (t + 1) * depth, :], NT, preferred_element_type=f32
            ).astype(low)

    made = set()
    for route, rel in sum_events:
        need = (route, rel[2]) if route < last_out else last_out
        if need not in made:
            made.add(need)
            if route >= last_out:
                make_seconds()
            else:
                make_grads(y if rel[2] == 0 else 1 - y, route)
        ways_out.scatter(
            route, rel, sum_ref(route), slot_refs[route], add, sum_send_sems, sum_recv_sems
        )

    first_out = local(grads.at[own_rows, :], first_ref, 0)
    own_second = y * hidden_size + chip * pair
    swap[0] = seconds[pl.ds(pl.multiple_of(own_second + other * h, h), h), :]
    second_swap = remote(swap.at[0], swap.at[1], 5, partner)
    second_swap.start()
    mine_out = local(
        seconds.at[pl.ds(pl.multiple_of(own_second + core * h, h), h), :], second_ref.at[core], 1
    )

    def whole(route, buf, other_buf, parts, last, cols):
        if route >= last:
            return lambda n: other_buf.at[pl.ds(0, n), pl.ds((route - last) * cols, cols)]
        first, count = parts[route]
        return lambda n: buf.at[pl.ds(0, n), pl.ds(first * 128, count * 128)]

    for route in range(len(GATHER_ORDERS)):
        unit = pair if route >= last_in else h
        part = whole(route, wbuf, w2buf, parts_in, last_in, cols_in)
        ways_in.drain(route, part, unit, send_sems)
    for route in range(len(SCATTER_ORDERS)):
        unit = pair if route >= last_out else h
        part = whole(route, grads, seconds, parts_out, last_out, cols_out)
        sent = part((nz * nx * ny - 1) * unit)
        pltpu.make_async_copy(sent, sent, sum_send_sems.at[route]).wait()

    @pl.when(y == 1)
    def _():
        fine_halo.wait_send()
        coarse_halo.wait_send()

    second_swap.wait()
    theirs_out = local(swap.at[1], second_ref.at[other], 2)
    first_out.wait()
    mine_out.wait()
    theirs_out.wait()


def finish_kernel(shift, sums_ref, sets_ref, first_ref, second_ref):
    y = lax.axis_index("tile")
    h, share = first_ref.shape
    depth = sets_ref.shape[2]
    bins = sums_ref.shape[1] // 128
    f32 = jnp.float32
    halves = lax.broadcasted_iota(jnp.int32, (h, 128), 1)
    back_shift = (128 - shift) % 128

    def turned(i):
        tile = sums_ref[:, 128 * i : 128 * (i + 1)].astype(f32)
        return tile, pltpu.roll(tile, back_shift, axis=1)

    now = turned(0)
    for i in range(bins):
        width = min(128, share - 128 * i)
        following = turned(i + 1) if i + 1 < bins else now
        late = jnp.where(halves < 128 - shift, now[1], following[1])
        first_ref[:, 128 * i : 128 * i + width] = jnp.where(y == 0, now[0], late)[:, :width]
        now = following
    for m in range(depth // 128):
        at = slice(128 * m, 128 * (m + 1))
        set_0 = sets_ref[0, :, at].astype(f32)
        set_1 = sets_ref[1, :, at].astype(f32)
        second_ref[:, 256 * m : 256 * m + 128] = jnp.where(
            halves < h, set_0, pltpu.roll(set_1, h, axis=1)
        )
        second_ref[:, 256 * m + 128 : 256 * m + 256] = jnp.where(
            halves < h, pltpu.roll(set_0, h, axis=1), set_1
        )


def per_device_by_chips(
    grid, proposal_boxes, level_plan, fine_map, coarse_map, first_weight, second_weight, upstream
):
    nz, nx, ny, cores = grid
    chips = nz * nx
    props = level_plan.shape[1]
    capacity = props // ny
    fine_tile, coarse = fine_map[0], coarse_map[0]
    fine_rows, fine_cols, channels = fine_tile.shape
    coarse_rows = coarse.shape[0]
    share, h = first_weight.shape
    feats = share * ny
    bins = max(-(-((t + 1) * share) // 128) - t * share // 128 for t in range(ny))
    lanes = bins * 128
    hidden_size = upstream.shape[2]
    depth = second_weight.shape[0] // cores
    pair = cores * h
    low, f32 = jnp.bfloat16, jnp.float32
    sizes = (nz, nx, ny)
    parts_out = cut(bins, SCATTER_SHARES)
    slot_counts = [sum(slots_of(sizes, order)) for order in SCATTER_ORDERS]
    rows_all = chips * h
    batch = cores * capacity
    q = chips * ny
    dma = pltpu.SemaphoreType.DMA
    anywhere = pl.BlockSpec(memory_space=pl.ANY)
    vmem = pl.BlockSpec(memory_space=pltpu.VMEM)
    slot_shapes = [
        (n, h, parts_out[i][1] * 128)
        if i < len(parts_out)
        else (n, pair, depth // (len(SCATTER_ORDERS) - len(parts_out)))
        for i, n in enumerate(slot_counts)
    ]
    sums, sets = pl.pallas_call(
        functools.partial(step_kernel, grid),
        out_shape=(
            jax.ShapeDtypeStruct((h, lanes), low),
            jax.ShapeDtypeStruct((cores, h, depth), low),
        ),
        in_specs=[vmem, vmem] + [anywhere] * 5,
        out_specs=(anywhere, anywhere),
        scratch_shapes=[
            pltpu.VMEM((h, share), low),
            pltpu.VMEM((h, cores * depth), low),
            pltpu.VMEM((cores, h, depth), low),
            pltpu.VMEM((ny * rows_all, lanes), low),
            pltpu.VMEM((ny * hidden_size, depth), low),
            pltpu.VMEM((fine_rows + HALO, fine_cols, channels), low),
            pltpu.VMEM((coarse_rows + HALO, coarse.shape[1], channels), low),
            pltpu.VMEM((fine_rows + coarse_rows + 2 * HALO, fine_cols, channels), f32),
            pltpu.VMEM((ROWS_PAD * GROUP, 128), f32),
            pltpu.VMEM((batch, feats), low),
            pltpu.VMEM((props, hidden_size), low),
            pltpu.VMEM((batch, hidden_size), low),
            pltpu.VMEM((hidden_size, batch), low),
            pltpu.VMEM((rows_all, batch), f32),
            pltpu.VMEM((rows_all, batch), f32),
            pltpu.VMEM((rows_all, batch), low),
            pltpu.VMEM((rows_all, batch), low),
            pltpu.VMEM((ny * rows_all, lanes), low),
            pltpu.VMEM((ny * hidden_size, depth), low),
            pltpu.VMEM((2, h, depth), low),
            pltpu.VMEM((8, capacity), jnp.int32),
            pltpu.VMEM((8, capacity), f32),
            pltpu.SMEM((8, capacity), jnp.int32),
            pltpu.SMEM((8, capacity), f32),
            dma((7,)),
            dma((len(GATHER_ORDERS), 6)),
            dma((len(GATHER_ORDERS), q)),
            dma((len(SCATTER_ORDERS),)),
            dma((sum(slot_counts),)),
            dma((6,)),
            dma((6,)),
        ]
        + [pltpu.VMEM(shape, low) for shape in slot_shapes],
        compiler_params=pltpu.CompilerParams(
            collective_id=0, has_side_effects=True, vmem_limit_bytes=64000 * 1024
        ),
        name="step",
    )(
        proposal_boxes[0],
        level_plan,
        first_weight.T,
        second_weight.T,
        upstream[0],
        fine_tile,
        coarse,
    )
    shift = share - 128 * min(share // 128, feats // 128 - bins)
    first, second = pl.pallas_call(
        functools.partial(finish_kernel, shift),
        out_shape=(
            jax.ShapeDtypeStruct((h, share), f32),
            jax.ShapeDtypeStruct((h, cores * depth), f32),
        ),
        in_specs=[vmem, vmem],
        out_specs=(vmem, vmem),
        name="finish",
    )(sums, sets)
    return (first.T, second.T)


def solution(mesh):
    placed = (
        P("dp", None, None),
        P("dp", None),
        P("dp", "tile", None, None),
        P("dp", "tile", None, None),
        P("tile", "dp"),
        P("tile", "dp"),
        P("dp", None, None),
    )
    grid = chip_grid(mesh)
    tiles = mesh.shape["tile"]
    body = per_device_by_bands
    if grid is not None and tiles == 2 and grid[1] <= 2 and grid[2] == 2:
        body = functools.partial(per_device_by_chips, (grid[0], grid[1], tiles, grid[2]))
    return jax.shard_map(
        body,
        mesh=mesh,
        in_specs=placed,
        out_specs=(P("tile", "dp"), P("tile", "dp")),
        check_vma=False,
    )
```

```python
import functools

import jax
import jax.numpy as jnp
from jax import lax
from jax.experimental import pallas as pl
from jax.experimental.pallas import tpu as pltpu
from jax.sharding import PartitionSpec as P

WIN = 16
BINS = 7
ROWS_PAD = 56
GROUP = 16


def from_ahead(block, axis, distance):
    if distance == 0:
        return block
    size = lax.axis_size(axis)
    return lax.ppermute(block, axis, [(i, (i - distance) % size) for i in range(size)])


def halo_from_next(block, axis):
    size = lax.axis_size(axis)
    return lax.ppermute(block, axis, [(i + 1, i) for i in range(size - 1)])


def gelu_parts(hidden):
    factor = 0.7978845608028654
    cubic_term = 0.044715
    inner_term = factor * (hidden + cubic_term * hidden * hidden * hidden)
    tangent = jnp.tanh(inner_term)
    gelu_value = 0.5 * hidden * (1.0 + tangent)
    gelu_slope = 0.5 * (1.0 + tangent) + 0.5 * hidden * (1.0 - tangent * tangent) * factor * (
        1.0 + 3.0 * cubic_term * hidden * hidden
    )
    return (gelu_value, gelu_slope)


def crop_kernel(starts, width, cells_ref, geo_ref, maps_ref, out_ref, wide, stage):
    step = pl.program_id(0)

    @pl.when(step == 0)
    def _():
        def widen(r, carry):
            wide[r] = maps_ref[r].astype(jnp.float32)
            return carry

        lax.fori_loop(0, maps_ref.shape[0], widen, 0)

    shape = (ROWS_PAD, WIN * WIN)
    k = lax.broadcasted_iota(jnp.int32, shape, 0).astype(jnp.float32)
    i_bin = jnp.floor((k + 0.5) * (1.0 / BINS))
    j_bin = k - BINS * i_bin
    i_mid = i_bin + 0.5
    j_mid = j_bin + 0.5
    lane = lax.broadcasted_iota(jnp.int32, shape, 1)
    r_cell = (lane >> 4).astype(jnp.float32)
    q_cell = (lane & 15).astype(jnp.float32)
    for p in range(GROUP):
        n = step * GROUP + p
        row = cells_ref[0, n]
        col = cells_ref[1, n]
        row_w = jnp.maximum(0.0, 1.0 - jnp.abs(i_mid * geo_ref[1, n] + geo_ref[0, n] - r_cell))
        col_w = jnp.maximum(0.0, 1.0 - jnp.abs(j_mid * geo_ref[3, n] + geo_ref[2, n] - q_cell))
        weights = (row_w * col_w).astype(jnp.bfloat16)
        window = jnp.concatenate(
            [wide[row + r, pl.ds(col, WIN), :] for r in range(WIN)], axis=0
        ).astype(jnp.bfloat16)
        crop = jnp.dot(weights, window, preferred_element_type=jnp.float32)
        stage[pl.ds(p, ROWS_PAD, stride=GROUP), :] = crop
    for t, first in enumerate(starts):
        for m in range(width):
            at = (first + m) * GROUP
            out_ref[t, :, m * 128 : (m + 1) * 128] = stage[at : at + GROUP, :].astype(jnp.bfloat16)


def make_crops(cells, geo, maps, starts, width, capacity):
    tiles = len(starts)
    lanes = width * 128
    return pl.pallas_call(
        functools.partial(crop_kernel, starts, width),
        grid=(capacity // GROUP,),
        out_shape=jax.ShapeDtypeStruct((tiles, capacity, lanes), jnp.bfloat16),
        in_specs=[
            pl.BlockSpec(memory_space=pltpu.SMEM),
            pl.BlockSpec(memory_space=pltpu.SMEM),
            pl.BlockSpec(maps.shape, lambda g: (0, 0, 0)),
        ],
        out_specs=pl.BlockSpec((tiles, GROUP, lanes), lambda g: (0, g, 0)),
        scratch_shapes=[
            pltpu.VMEM(maps.shape, jnp.float32),
            pltpu.VMEM((ROWS_PAD * GROUP, 128), jnp.float32),
        ],
        compiler_params=pltpu.CompilerParams(
            dimension_semantics=("arbitrary",), vmem_limit_bytes=48 * 1024 * 1024
        ),
        cost_estimate=pl.CostEstimate(
            flops=capacity * ROWS_PAD * WIN * WIN * 128 * 16,
            bytes_accessed=2 * maps.size + 2 * tiles * capacity * lanes,
            transcendentals=0,
        ),
        name="crops",
    )(cells, geo, maps)


def per_device_by_bands(
    proposal_boxes, level_plan, fine_map, coarse_map, first_weight, second_weight, upstream
):
    tile_count = lax.axis_size("tile")
    band = lax.axis_index("tile")
    num_props = level_plan.shape[1]
    capacity = max(num_props // 4, num_props // tile_count)
    fine_tile = fine_map[0]
    coarse = coarse_map[0]
    fine_rows, fine_cols, channels = fine_tile.shape
    coarse_rows, coarse_cols = (coarse.shape[0], coarse.shape[1])

    top_rows = jnp.concatenate([fine_tile[:WIN], coarse[:WIN]], axis=1)
    below_rows = halo_from_next(top_rows, "tile")

    share_feats = first_weight.shape[0]
    feats = share_feats * tile_count
    width = max(
        -(-((t + 1) * share_feats) // 128) - t * share_feats // 128 for t in range(tile_count)
    )
    starts = [min(t * share_feats // 128, feats // 128 - width) for t in range(tile_count)]
    lanes = width * 128
    feat_off = band * share_feats - 128 * jnp.minimum(
        band * share_feats // 128, feats // 128 - width
    )

    first_rows = lax.dynamic_update_slice(
        jnp.zeros((first_weight.shape[1], lanes), jnp.bfloat16),
        first_weight.T,
        (0, feat_off),
    )
    both = lax.all_gather(
        jnp.concatenate([first_rows, second_weight.T], axis=1), "dp", axis=0, tiled=True
    )
    first_all = both[:, :lanes]
    second_all = both[:, lanes:]

    fields = proposal_boxes[0]
    levels = level_plan[0]
    owner = fields[0] // (4 * fine_rows)
    members = (owner[:, None] == jnp.arange(tile_count, dtype=jnp.int32)[None, :]).astype(jnp.int32)
    rank = jnp.sum((jnp.cumsum(members, axis=0) - 1) * members, axis=1)
    relative = lax.rem(owner - band + tile_count, tile_count)
    slot_id = relative * capacity + rank
    slots = tile_count * capacity
    chosen = slot_id[None, :] == jnp.arange(slots, dtype=jnp.int32)[:, None]
    upstream_slots = jnp.dot(
        chosen.astype(jnp.bfloat16), upstream[0], preferred_element_type=jnp.float32
    ).astype(jnp.bfloat16)
    mine = chosen[:capacity].astype(jnp.int32)
    top, left, height, box_width = (
        jnp.sum(mine * fields[f][None, :], axis=1) for f in range(4)
    )
    level = jnp.sum(mine * levels[None, :], axis=1)

    stride = jnp.where(level == 0, 4, 8).astype(jnp.int32)
    is_fine = level == 0
    first_row = top // stride
    local_row = jnp.clip(
        first_row - band * jnp.where(is_fine, fine_rows, coarse_rows),
        0,
        jnp.where(is_fine, fine_rows, coarse_rows) - 1,
    )
    first_col = jnp.minimum(left // stride, jnp.where(is_fine, fine_cols, coarse_cols) - WIN)
    cells = jnp.stack(
        [local_row + jnp.where(is_fine, 0, fine_rows + WIN), first_col], axis=0
    ).astype(jnp.int32)
    stride_float = stride.astype(jnp.float32)
    geo = jnp.stack(
        [
            top.astype(jnp.float32) / stride_float - first_row.astype(jnp.float32),
            height.astype(jnp.float32) / (7.0 * stride_float),
            left.astype(jnp.float32) / stride_float - first_col.astype(jnp.float32),
            box_width.astype(jnp.float32) / (7.0 * stride_float),
        ],
        axis=0,
    )

    side = ((0, 0), (0, fine_cols - coarse_cols), (0, 0))
    maps = jnp.concatenate(
        [
            fine_tile,
            below_rows[:, :fine_cols],
            jnp.pad(coarse, side),
            jnp.pad(below_rows[:, fine_cols:], side),
        ],
        axis=0,
    )
    crop_blocks = make_crops(cells, geo, maps, starts, width, capacity)
    own_feats = jnp.concatenate(
        [
            from_ahead(
                lax.dynamic_index_in_dim(
                    crop_blocks, lax.rem(band - d + tile_count, tile_count), 0, keepdims=False
                ),
                "tile",
                d,
            )
            for d in range(tile_count)
        ],
        axis=0,
    )

    partial_hidden = lax.dot_general(
        own_feats, first_all, (((1,), (1,)), ((), ())), preferred_element_type=jnp.float32
    ).astype(jnp.bfloat16)
    share = second_weight.shape[0]

    def in_my_order(block, d):
        return jnp.roll(block, d * capacity, axis=0) if d else block

    hidden_own = 0.0
    for d in range(tile_count):
        to = lax.rem(band - d + tile_count, tile_count)
        piece = lax.dynamic_slice_in_dim(partial_hidden, to * share, share, axis=1)
        hidden_own = hidden_own + in_my_order(from_ahead(piece, "tile", d), d).astype(jnp.float32)
    gelu_value, gelu_slope = gelu_parts(hidden_own)
    activated = gelu_value.astype(jnp.bfloat16)
    back_grad = jnp.dot(upstream_slots, second_all, preferred_element_type=jnp.float32)
    pre_own = (back_grad * gelu_slope).astype(jnp.bfloat16)
    ahead = [in_my_order(from_ahead(pre_own, "tile", d), d) for d in range(tile_count)]
    twice = jnp.concatenate(ahead + ahead[:-1], axis=1)
    pre_grad = lax.dynamic_slice_in_dim(
        twice, lax.rem(tile_count - band, tile_count) * share, tile_count * share, axis=1
    )
    over_rows = (((0,), (0,)), ((), ()))
    second_part = lax.dot_general(
        upstream_slots, activated, over_rows, preferred_element_type=jnp.float32
    ).astype(jnp.bfloat16)
    first_part = lax.dot_general(
        pre_grad, own_feats, over_rows, preferred_element_type=jnp.float32
    ).astype(jnp.bfloat16)
    summed = lax.psum_scatter(
        jnp.concatenate([first_part, second_part], axis=1), "dp", scatter_dimension=0, tiled=True
    ).astype(jnp.float32)
    first_grad = lax.dynamic_slice_in_dim(summed[:, :lanes], feat_off, share_feats, axis=1).T
    second_grad = summed[:, lanes:].T
    return (first_grad, second_grad)


MESH = pl.DeviceIdType.MESH
REACH = 15
HALO = REACH - 1
NT = (((1,), (1,)), ((), ()))
NN = (((1,), (0,)), ((), ()))


def chip_grid(mesh):
    chips = [getattr(device, "coords", None) for device in mesh.devices[:, 0]]
    if chips[0] is None:
        return None
    cores = sum(1 for c in chips if tuple(c) == tuple(chips[0]))
    chips = [tuple(c) for c in chips[::cores]]
    if len(chips) == 1:
        return (1, 1, cores)
    axis = [a != b for a, b in zip(chips[0], chips[1])].index(True)
    fast = 1
    while fast < len(chips) and all(
        a == b or i == axis for i, (a, b) in enumerate(zip(chips[0], chips[fast]))
    ):
        fast += 1
    return (len(chips) // fast, fast, cores)


def offsets(size):
    if size == 1:
        return [0]
    if size == 2:
        return [0, 1]
    return [0] + [s * d for d in range(1, size) for s in (-1, 1)]


def steps_of(size):
    return {1: [], 2: [1]}.get(size, [-1, 1])


def moved(position, size, rel):
    if rel == 0 or size == 1:
        return position
    return 1 - position if size == 2 else position + rel


def last_axis(order, rel):
    used = [j for j in range(3) if rel[order[j]]]
    return used[-1] if used else -1


def onward(sizes, order, rel):
    last = last_axis(order, rel)
    hops = []
    if last >= 0:
        axis = order[last]
        if sizes[axis] > 2 and abs(rel[axis]) < sizes[axis] - 1:
            hops.append((last, axis, -1 if rel[axis] > 0 else 1))
    for j in range(last + 1, 3):
        hops.extend((j, order[j], step) for step in steps_of(sizes[order[j]]))
    return hops


def arrival_order(sizes, routes, extra):
    import heapq
    import itertools

    places = list(itertools.product(*(range(n) for n in sizes)))
    queue, waiting, busy = [], {}, set()
    seen, tick = {}, itertools.count()

    def start(link, now):
        if link not in busy and waiting.get(link):
            busy.add(link)
            load, arrival = waiting[link].pop(0)
            heapq.heappush(queue, (now + load, next(tick), link, arrival))

    def arrive(place, route, rel, now):
        seen.setdefault((route, rel), []).append(now)
        for _, axis, step in onward(sizes, routes[route][0], rel):
            target = list(place)
            target[axis] = moved(place[axis], sizes[axis], step)
            if not 0 <= target[axis] < sizes[axis]:
                continue
            there = list(rel)
            there[axis] = rel[axis] - step if sizes[axis] > 2 else 1
            link = (place, axis, step)
            waiting.setdefault(link, []).append(
                (routes[route][1], (tuple(target), route, tuple(there)))
            )
            start(link, now)

    first = {}
    for place in places:
        for route in extra[1]:
            arrive(place, route, (0, 0, 0), 0.0)
        if extra[0] and place[2] == 1:
            waiting.setdefault((place, 2, 1), []).append((extra[0], None))
            start((place, 2, 1), 0.0)
        for route in range(len(routes)):
            if route not in extra[1]:
                arrive(place, route, (0, 0, 0), 0.0)
    end = 0.0
    while queue:
        now, _, link, arrival = heapq.heappop(queue)
        end = now
        busy.discard(link)
        if arrival is not None:
            arrive(*arrival, now)
        start(link, now)
    key = {event: sum(t) / len(t) for event, t in seen.items()}
    for _ in range(sum(sizes)):
        for (route, rel) in list(key):
            for _, axis, step in onward(sizes, routes[route][0], rel):
                there = list(rel)
                there[axis] = rel[axis] - step if sizes[axis] > 2 else 1
                event = (route, tuple(there))
                if event in key:
                    key[event] = max(key[event], key[(route, rel)] + 1e-3)
    return sorted(key, key=lambda e: (key[e], e)), key, end


def slots_of(sizes, order):
    counts, before = [], 1
    for j in range(3):
        n = sizes[order[j]]
        counts.append(before * (2 * n if n > 2 else 1))
        before *= n
    return counts


def when(conds, body):
    if not conds:
        body()
        return
    total = conds[0]
    for cond in conds[1:]:
        total = jnp.logical_and(total, cond)
    pl.when(total)(body)


class Routes:
    def __init__(self, sizes, position, core, cores, orders):
        self.sizes, self.position = sizes, position
        self.core, self.cores = core, cores
        self.orders = orders
        self.slot_counts = [slots_of(sizes, order) for order in orders]
        self.slot_base = [sum(sum(c) for c in self.slot_counts[:i]) for i in range(len(orders))]

    def inside(self, axis, rel):
        if rel == 0 or self.sizes[axis] <= 2:
            return []
        p = self.position[axis]
        return [p < self.sizes[axis] - rel] if rel > 0 else [p >= -rel]

    def valid(self, rel):
        return sum((self.inside(axis, rel[axis]) for axis in range(3)), [])

    def at(self, rel):
        return [moved(self.position[a], self.sizes[a], rel[a]) for a in range(3)]

    def device(self, axis, step):
        there = list(self.position)
        there[axis] = moved(there[axis], self.sizes[axis], step)
        return ((there[0] * self.sizes[1] + there[1]) * self.cores + self.core, there[2])

    def back_step(self, order, rel):
        axis = order[last_axis(order, rel)]
        return axis, (1 if self.sizes[axis] == 2 or rel[axis] > 0 else -1)

    def number(self, place):
        return (place[0] * self.sizes[1] + place[1]) * self.sizes[2] + place[2]

    def direction(self, axis, step):
        return 2 * axis + (1 if step > 0 else 0)

    def drain(self, route, whole, unit, sems):
        order, before = self.orders[route], 1
        for axis in order:
            n, p = self.sizes[axis], self.position[axis]
            for step in steps_of(n):
                for at in range(n) if n > 2 else [0]:
                    sent = before * ((at + 1 if step > 0 else n - at) if n > 2 else 1)
                    if n > 2 and not 0 <= at + step < n:
                        continue

                    def wait(axis=axis, step=step, sent=sent):
                        part = whole(sent * unit)
                        pltpu.make_async_copy(
                            part, part, sems.at[route, self.direction(axis, step)]
                        ).wait()

                    when([p == at] if n > 2 else [], wait)
            before *= n

    def gather(self, route, rel, ref_of, send_sems, recv_sems):
        order = self.orders[route]

        def body():
            place = self.at(rel)
            ref = ref_of(place)
            q = self.number(place)

            def hop(axis, step):
                return pltpu.make_async_remote_copy(
                    src_ref=ref,
                    dst_ref=ref,
                    send_sem=send_sems.at[route, self.direction(axis, step)],
                    recv_sem=recv_sems.at[route, q],
                    device_id=self.device(axis, step),
                    device_id_type=MESH,
                )

            if last_axis(order, rel) >= 0:
                hop(*self.back_step(order, rel)).wait_recv()
            for _, axis, step in onward(self.sizes, order, rel):
                copy = hop(axis, step)
                when(self.inside(axis, step), copy.start)

        when(self.valid(rel), body)

    def slot(self, route, phase, side, place):
        order, counts = self.orders[route], self.slot_counts[route]
        index = 0
        for j in range(phase):
            index = index * self.sizes[order[j]] + place[order[j]]
        n = self.sizes[order[phase]]
        if n > 2:
            index = (index * n + place[order[phase]]) * 2 + (1 if side > 0 else 0)
        return sum(counts[:phase]) + index

    def scatter(self, route, rel, ref_of, slots, add, send_sems, recv_sems):
        order = self.orders[route]

        def body():
            place = self.at(rel)
            ref = ref_of(place)
            base = self.slot_base[route]
            for phase, axis, step in onward(self.sizes, order, rel):
                slot = self.slot(route, phase, step, place)

                def take(axis=axis, step=step, slot=slot):
                    pltpu.make_async_remote_copy(
                        src_ref=ref,
                        dst_ref=slots.at[slot],
                        send_sem=send_sems.at[route],
                        recv_sem=recv_sems.at[base + slot],
                        device_id=self.device(axis, step),
                        device_id_type=MESH,
                    ).wait_recv()
                    add(ref, slots.at[slot])

                when(self.inside(axis, step), take)
            phase = last_axis(order, rel)
            if phase >= 0:
                axis, step = self.back_step(order, rel)
                slot = self.slot(route, phase, 1 if self.sizes[axis] == 2 else -step, place)
                pltpu.make_async_remote_copy(
                    src_ref=ref,
                    dst_ref=slots.at[slot],
                    send_sem=send_sems.at[route],
                    recv_sem=recv_sems.at[base + slot],
                    device_id=self.device(axis, step),
                    device_id_type=MESH,
                ).start()

        when(self.valid(rel), body)


def cut(bins, shares):
    edges = [0]
    for i in range(1, len(shares) + 1):
        edges.append(round(bins * sum(shares[:i]) / sum(shares)))
    return [(a, b - a) for a, b in zip(edges, edges[1:])]


GATHER_ORDERS = ((2, 0, 1), (0, 1, 2), (1, 2, 0), (2, 0, 1), (0, 1, 2))
GATHER_SHARES = (13, 9, 3)
SCATTER_ORDERS = ((2, 0, 1), (0, 1, 2), (0, 1, 2), (1, 2, 0), (2, 0, 1))
SCATTER_SHARES = (6, 8, 8, 3)
HALO_AFTER = 2
EARLY, DURING = 15, 41
CROP_AT = (
        0, 1, 1, 1, 1, 2, 2, 2, 2, 2, 4, 4, 4, 4, 6, 6, 6, 6, 7, 7, 7, 8, 8, 8, 9, 9, 10, 10,
        10, 10, 10, 12, 12, 12, 12, 13, 13, 13, 14, 15, 15
)
GATHER_CODES = {
    (4, 2, 2): (
        0, 56, 84, 112, 28, 1, 120, 116, 32, 8, 128, 36, 58, 4, 124, 118, 136, 40, 132, 16, 12,
        38, 122, 34, 57, 85, 62, 86, 44, 9, 48, 20, 70, 24, 5, 60, 129, 64, 138, 52, 65, 134, 2,
        50, 13, 42, 59, 30, 68, 17, 66, 72, 125, 10, 41, 54, 37, 25, 21, 88, 14, 26, 46, 92, 80,
        119, 121, 74, 89, 11, 93, 133, 33, 82, 105, 63, 97, 18, 22, 61, 39, 78, 87, 6, 53, 73,
        130, 7, 29, 104, 96, 101, 109, 126, 113, 137, 71, 108, 100, 114, 69, 49, 139, 67, 19,
        76, 117, 55, 27, 51, 23, 45, 75, 15, 43, 3, 31, 123, 94, 47, 35, 103, 111, 131, 81, 77,
        135, 91, 107, 95, 79, 106, 127, 115, 90, 110, 99, 83, 102, 98
    ),
}
SCATTER_CODES = {
    (4, 2, 2): (
        6, 138, 110, 39, 106, 123, 35, 109, 108, 83, 22, 14, 107, 105, 51, 139, 27, 23, 75, 98,
        111, 131, 102, 55, 19, 130, 7, 135, 11, 101, 26, 134, 47, 94, 43, 137, 15, 99, 71, 37,
        73, 18, 100, 82, 53, 25, 103, 79, 127, 63, 93, 90, 41, 20, 136, 104, 97, 54, 12, 74, 21,
        49, 81, 33, 77, 91, 17, 96, 133, 129, 132, 10, 118, 3, 46, 115, 122, 125, 50, 126, 67,
        13, 24, 16, 119, 65, 78, 9, 42, 4, 128, 92, 59, 52, 70, 80, 89, 45, 114, 34, 121, 62,
        31, 95, 69, 66, 8, 72, 44, 5, 61, 57, 38, 85, 2, 120, 124, 117, 88, 87, 76, 1, 48, 116,
        113, 58, 68, 40, 64, 60, 86, 30, 32, 29, 36, 0, 84, 56, 112, 28
    ),
}


def unpack(codes, sizes):
    spans = [offsets(n) for n in sizes]
    events = []
    for code in codes:
        code, k = divmod(code, len(spans[2]))
        code, j = divmod(code, len(spans[1]))
        route, i = divmod(code, len(spans[0]))
        events.append((route, (spans[0][i], spans[1][j], spans[2][k])))
    return events


def step_kernel(grid, *refs):
    fields_ref, levels_ref, w1_ref, w2_ref, up_ref, fine_ref, coarse_ref = refs[:7]
    first_ref, second_ref = refs[7:9]
    (
        w_in,
        w2_in,
        w2_sets,
        wbuf,
        w2buf,
        fine_low,
        coarse_low,
        wide,
        stage,
        crops,
        up_all,
        upb,
        uptb,
        back,
        hidden,
        acts,
        pres,
        grads,
        seconds,
        swap,
        cells_v,
        geo_v,
        cells_ref,
        geo_ref,
        local_sems,
        send_sems,
        recv_sems,
        sum_send_sems,
        sum_recv_sems,
        core_send,
        core_recv,
    ) = refs[9:40]
    slot_refs = refs[40:]
    nz, nx, ny, cores = grid
    sizes = (nz, nx, ny)
    dp = lax.axis_index("dp")
    y = lax.axis_index("tile")
    core = dp % cores
    chip = dp // cores
    x = chip % nx
    z = chip // nx
    position = (z, x, y)
    other = 1 - core
    partner = (chip * cores + other, y)
    ways_in = Routes(sizes, position, core, cores, GATHER_ORDERS)
    ways_out = Routes(sizes, position, core, cores, SCATTER_ORDERS)
    h, share = w1_ref.shape
    lanes = wbuf.shape[1]
    bins = lanes // 128
    all_rows = nz * nx * h
    fine_rows, fine_cols, _ = fine_ref.shape
    coarse_rows, coarse_cols, _ = coarse_ref.shape
    batch, feats = crops.shape
    capacity = batch // cores
    depth = w2buf.shape[1]
    hidden_size = up_ref.shape[1]
    pair = cores * h
    starts = [min(t * share // 128, feats // 128 - bins) for t in range(ny)]
    shift = share - 128 * starts[1]
    parts_in = cut(bins, GATHER_SHARES)
    parts_out = cut(bins, SCATTER_SHARES)
    f32, low = jnp.float32, jnp.bfloat16

    barrier = pltpu.get_barrier_semaphore()
    pl.semaphore_signal(barrier, inc=1, device_id=partner, device_id_type=MESH)
    peers = 1
    for axis in range(3):
        for step in steps_of(sizes[axis]):

            def greet(axis=axis, step=step):
                pl.semaphore_signal(
                    barrier, inc=1, device_id=ways_in.device(axis, step), device_id_type=MESH
                )

            near = ways_in.inside(axis, step)
            when(near, greet)
            peers = peers + (near[0].astype(jnp.int32) if near else 1)

    def rows(start, size):
        return pl.ds(pl.multiple_of(start, size), size)

    def local(src, dst, i):
        copy = pltpu.make_async_copy(src, dst, local_sems.at[i])
        copy.start()
        return copy

    def remote(src, dst, i, device):
        return pltpu.make_async_remote_copy(
            src_ref=src,
            dst_ref=dst,
            send_sem=core_send.at[i],
            recv_sem=core_recv.at[i],
            device_id=device,
            device_id_type=MESH,
        )

    w_copy = local(w1_ref, w_in, 0)
    w2_copy = local(w2_ref, w2_in, 1)
    fine_copy = local(fine_ref, fine_low.at[pl.ds(0, fine_rows)], 2)
    coarse_copy = local(coarse_ref, coarse_low.at[pl.ds(0, coarse_rows)], 3)
    up_copy = local(up_ref, up_all, 4)
    halves = lax.broadcasted_iota(jnp.int32, (h, 128), 1)

    w_copy.wait()
    own_rows = pl.ds(pl.multiple_of(y * all_rows + chip * h, h), h)
    before = jnp.zeros((h, 128), f32)
    for i in range(bins):
        width = min(128, share - 128 * i)
        now = w_in[:, 128 * i : 128 * i + width].astype(f32)
        if width < 128:
            now = jnp.concatenate([now, jnp.zeros((h, 128 - width), f32)], axis=1)
        turned = pltpu.roll(now, shift, axis=1) if shift else now
        late = jnp.where(halves < shift, before, turned)
        before = turned
        wbuf[own_rows, 128 * i : 128 * (i + 1)] = jnp.where(y == 0, now, late).astype(low)

    pl.semaphore_wait(barrier, peers)

    last_in = len(GATHER_SHARES)
    last_out = len(SCATTER_SHARES)
    cols_in = depth // (len(GATHER_ORDERS) - last_in)
    cols_out = depth // (len(SCATTER_ORDERS) - last_out)
    loads_in = [
        (order, parts_in[i][1] if i < last_in else cols_in * pair // (h * 128))
        for i, order in enumerate(GATHER_ORDERS)
    ]
    loads_out = [
        (order, parts_out[i][1] if i < last_out else cols_out * pair // (h * 128))
        for i, order in enumerate(SCATTER_ORDERS)
    ]
    halo_load = HALO * (fine_cols + coarse_cols) // h
    if sizes in GATHER_CODES:
        events = unpack(GATHER_CODES[sizes], sizes)
        sum_events = unpack(SCATTER_CODES[sizes], sizes)
    else:
        events = arrival_order(sizes, loads_in, (halo_load, (0,)))[0]
        sum_events = arrival_order(sizes, loads_out, (0, ()))[0][::-1]

    def gather_ref(route):
        if route >= last_in:
            return lambda q: w2buf.at[
                rows(q[2] * hidden_size + (q[0] * nx + q[1]) * pair, pair),
                pl.ds((route - last_in) * cols_in, cols_in),
            ]
        first, count = parts_in[route]
        return lambda q: wbuf.at[
            rows(q[2] * all_rows + (q[0] * nx + q[1]) * h, h), pl.ds(first * 128, count * 128)
        ]

    def gather(event):
        route, rel = event
        ways_in.gather(route, rel, gather_ref(route), send_sems, recv_sems)

    below = ways_in.device(2, 1)
    fine_halo = remote(
        fine_ref.at[pl.ds(0, HALO)], fine_low.at[pl.ds(fine_rows, HALO)], 1, below
    )
    coarse_halo = remote(
        coarse_ref.at[pl.ds(0, HALO)], coarse_low.at[pl.ds(coarse_rows, HALO)], 2, below
    )
    own = [e for e in events if e[1] == (0, 0, 0)]
    todo = [e for e in events if e[1] != (0, 0, 0)]
    own.sort(key=lambda e: e[0] >= last_in)
    for n, event in enumerate(own[:last_in]):
        gather(event)
        if n + 1 == min(HALO_AFTER, last_in):

            @pl.when(y == 1)
            def _():
                fine_halo.start()
                coarse_halo.start()

    w2_copy.wait()
    for m in range(depth // 128):
        a = w2_in[:, 256 * m : 256 * m + 128].astype(f32)
        b = w2_in[:, 256 * m + 128 : 256 * m + 256].astype(f32)
        at = slice(128 * m, 128 * (m + 1))
        w2_sets[0, :, at] = jnp.where(halves < h, a, pltpu.roll(b, h, axis=1)).astype(low)
        w2_sets[1, :, at] = jnp.where(halves < h, pltpu.roll(a, h, axis=1), b).astype(low)
    w2_rows = pl.ds(pl.multiple_of(y * hidden_size + chip * pair + core * h, h), h)
    w2buf[w2_rows, :] = w2_sets[core]

    w2_swap = remote(w2_sets.at[other], w2buf.at[w2_rows, :], 0, partner)
    w2_swap.start()
    w2_swap.wait()
    for event in own[last_in:]:
        gather(event)

    events = own + todo

    member = jnp.logical_and(
        fields_ref[0:1, :] >= y * (4 * fine_rows), fields_ref[0:1, :] < (y + 1) * (4 * fine_rows)
    )
    props = fields_ref.shape[1]
    ones = jnp.broadcast_to(jnp.where(member, 1.0, 0.0), (8, props)).astype(low)
    upto = lax.broadcasted_iota(jnp.int32, (props, props), 0) <= lax.broadcasted_iota(
        jnp.int32, (props, props), 1
    )
    rank = jnp.dot(ones, jnp.where(upto, 1.0, 0.0).astype(low), preferred_element_type=f32)
    slot = jnp.where(member, rank[0:1, :] - 1.0, -1.0)
    slot_ids = lax.broadcasted_iota(jnp.int32, (capacity, props), 0).astype(f32)
    picks = jnp.where(slot == slot_ids, 1.0, 0.0).astype(low)

    def pick(ints):
        return lax.dot_general(
            ints.astype(f32).astype(low), picks, NT, preferred_element_type=f32
        )

    boxes = jnp.concatenate([fields_ref[...], fields_ref[...]], axis=0)
    values = 8.0 * pick(boxes >> 3) + pick(boxes & 7)
    level = pick(jnp.broadcast_to(levels_ref[...], (8, props)))[0:1, :]
    top, left, height, box_width = (values[i : i + 1, :] for i in range(4))
    is_fine = level < 0.5
    inverse = jnp.where(is_fine, 0.25, 0.125)
    span = jnp.where(is_fine, 28.0, 56.0)
    first_row = jnp.floor(top * inverse)
    band_rows = jnp.where(is_fine, 1.0 * fine_rows, 1.0 * coarse_rows)
    local_row = jnp.clip(first_row - y.astype(f32) * band_rows, 0.0, band_rows - 1.0)
    first_col = jnp.minimum(
        jnp.floor(left * inverse), jnp.where(is_fine, 1.0 * fine_cols, 1.0 * coarse_cols) - WIN
    )
    cells_v[0:1, :] = (local_row + jnp.where(is_fine, 0.0, 1.0 * (fine_rows + HALO))).astype(
        jnp.int32
    )
    cells_v[1:2, :] = first_col.astype(jnp.int32)
    geo_v[0:1, :] = top * inverse - first_row
    geo_v[1:2, :] = height / span
    geo_v[2:3, :] = left * inverse - first_col
    geo_v[3:4, :] = box_width / span
    up_copy.wait()
    half = rows(core * capacity, capacity)
    upb[half, :] = jnp.dot(picks, up_all[...], preferred_element_type=f32).astype(low)
    cells_copy = local(cells_v, cells_ref, 5)
    geo_copy = local(geo_v, geo_ref, 6)

    coarse_base = fine_rows + HALO

    def widen(source, first, count, base, cols):
        def one(r, carry):
            wide[base + r, 0:cols, :] = source[r].astype(f32)
            return carry

        lax.fori_loop(first, first + count, one, 0)

    fine_copy.wait()
    coarse_copy.wait()
    widen(fine_low, 0, fine_rows, 0, fine_cols)
    widen(coarse_low, 0, coarse_rows, coarse_base, coarse_cols)
    up_swap = remote(upb.at[half, :], upb.at[half, :], 3, partner)
    up_swap.start()

    for event in todo[:EARLY]:
        gather(event)
    up_swap.wait()

    def turn_up(i, carry):
        at = rows(i * 128, 128)
        uptb[at, :] = upb[:, at].astype(f32).T.astype(low)
        return carry

    lax.fori_loop(0, hidden_size // 128, turn_up, 0)

    @pl.when(y == 0)
    def _():
        fine_halo.wait_recv()
        coarse_halo.wait_recv()
        widen(fine_low, fine_rows, HALO, 0, fine_cols)
        widen(coarse_low, coarse_rows, HALO, coarse_base, coarse_cols)

    @pl.when(y == 1)
    def _():
        def clear(r, carry):
            wide[r] = jnp.zeros(wide.shape[1:], f32)
            return carry

        lax.fori_loop(fine_rows, fine_rows + HALO, clear, 0)
        lax.fori_loop(coarse_base + coarse_rows, coarse_base + coarse_rows + HALO, clear, 0)

    cells_copy.wait()
    geo_copy.wait()

    groups = capacity // GROUP
    during = todo[EARLY : EARLY + DURING]
    shape = (ROWS_PAD, REACH * WIN)
    k = lax.broadcasted_iota(jnp.int32, shape, 0).astype(f32)
    i_bin = jnp.floor((k + 0.5) * (1.0 / BINS))
    j_bin = k - BINS * i_bin
    i_mid = i_bin + 0.5
    j_mid = j_bin + 0.5
    lane = lax.broadcasted_iota(jnp.int32, shape, 1)
    r_cell = (lane >> 4).astype(f32)
    q_cell = (lane & 15).astype(f32)

    def crop_copy(first, count):
        crop_rows = pl.ds(pl.multiple_of(core * capacity + first, GROUP), count)
        return remote(crops.at[crop_rows, :], crops.at[crop_rows, :], 4, partner)

    def crop_group(g, carry):
        for n, event in enumerate(during):
            at = CROP_AT[n] if sizes in GATHER_CODES else n * groups // len(during)
            pl.when(g == min(at, groups - 1))(functools.partial(gather, event))
        for p in range(GROUP):
            n = g * GROUP + p
            row = jnp.clip(cells_ref[0, n], 0, wide.shape[0] - REACH)
            col = jnp.clip(cells_ref[1, n], 0, fine_cols - WIN)
            row_w = jnp.maximum(0.0, 1.0 - jnp.abs(i_mid * geo_ref[1, n] + geo_ref[0, n] - r_cell))
            col_w = jnp.maximum(0.0, 1.0 - jnp.abs(j_mid * geo_ref[3, n] + geo_ref[2, n] - q_cell))
            weights = (row_w * col_w).astype(low)
            window = jnp.concatenate(
                [wide[row + r, pl.ds(col, WIN), :] for r in range(REACH)], axis=0
            ).astype(low)
            crop = jnp.dot(weights, window, preferred_element_type=f32)
            stage[pl.ds(p, ROWS_PAD, stride=GROUP), :] = crop
        group_rows = rows(core * capacity + g * GROUP, GROUP)
        for m in range(feats // 128):
            crops[group_rows, m * 128 : (m + 1) * 128] = stage[
                m * GROUP : (m + 1) * GROUP, :
            ].astype(low)

        @pl.when(g > 0)
        def _():
            crop_copy((g - 1) * GROUP, GROUP).start()

        return carry

    lax.fori_loop(0, groups, crop_group, 0)
    crop_copy((groups - 1) * GROUP, GROUP).start()

    def hide(ahead, route, begun):
        t = y if ahead == 0 else 1 - y
        first, count = parts_in[route]
        from_at = (starts[0] + t * (starts[1] - starts[0]) + first) * 128
        part = lax.dot_general(
            wbuf[rows(t * all_rows, all_rows), first * 128 : (first + count) * 128],
            crops[:, pl.ds(pl.multiple_of(from_at, 128), count * 128)],
            NT,
            preferred_element_type=f32,
        )
        hidden[...] = hidden[...] + part if begun else part

    ends = {(rel[2], route): i for i, (route, rel) in enumerate(events) if route < last_in}
    ready = [(i, key) for key, i in ends.items()]
    passed = len(own) + EARLY + DURING
    waited, begun = False, False
    for i in range(passed - 1, len(events)):
        if i >= passed:
            gather(events[i])
        for key in [k for end, k in sorted(ready) if end == i or (i == passed - 1 and end < i)]:
            if not waited:
                waited = True
                crop_copy(0, capacity).wait()
            hide(*key, begun)
            begun = True
    for t in range(ny):
        part = jnp.dot(
            upb[...], w2buf[t * hidden_size : (t + 1) * hidden_size, :], preferred_element_type=f32
        )
        back[t * depth : (t + 1) * depth, :] = part.T

    def gelu(i, carry):
        at = rows(i * 32, 32)
        value, slope = gelu_parts(hidden[at, :])
        acts[at, :] = value.astype(low)
        pres[at, :] = (back[at, :] * slope).astype(low)
        return carry

    lax.fori_loop(0, hidden.shape[0] // 32, gelu, 0)

    def sum_ref(route):
        if route >= last_out:
            return lambda q: seconds.at[
                rows(q[2] * hidden_size + (q[0] * nx + q[1]) * pair, pair),
                pl.ds((route - last_out) * cols_out, cols_out),
            ]
        first, count = parts_out[route]
        return lambda q: grads.at[
            rows(q[2] * all_rows + (q[0] * nx + q[1]) * h, h), pl.ds(first * 128, count * 128)
        ]

    def add(ref, more):
        def one(i, carry):
            at = rows(i * 16, 16)
            ref[at, :] = (ref[at, :].astype(f32) + more[at, :].astype(f32)).astype(low)
            return carry

        lax.fori_loop(0, ref.shape[0] // 16, one, 0)

    def make_grads(t, part):
        first, count = parts_out[part]
        step = max(c for c in range(1, 7) if count % c == 0)

        def one(i, carry):
            at = pl.multiple_of((first + i * step) * 128, 128)
            from_at = pl.multiple_of((starts[0] + t * (starts[1] - starts[0])) * 128 + at, 128)
            grads[rows(t * all_rows, all_rows), pl.ds(at, step * 128)] = jnp.dot(
                pres[...], crops[:, pl.ds(from_at, step * 128)], preferred_element_type=f32
            ).astype(low)
            return carry

        lax.fori_loop(0, count // step, one, 0)

    def make_seconds():
        for t in range(ny):
            seconds[t * hidden_size : (t + 1) * hidden_size, :] = lax.dot_general(
                uptb[...], acts[t * depth : (t + 1) * depth, :], NT, preferred_element_type=f32
            ).astype(low)

    own_second = y * hidden_size + chip * pair
    made, ended, outs, swapped = set(), set(), [], False
    for route, rel in sum_events:
        need = (route, rel[2]) if route < last_out else last_out
        if need not in made:
            made.add(need)
            if route >= last_out:
                make_seconds()
            else:
                make_grads(y if rel[2] == 0 else 1 - y, route)
        ways_out.scatter(
            route, rel, sum_ref(route), slot_refs[route], add, sum_send_sems, sum_recv_sems
        )
        if rel != (0, 0, 0):
            continue
        ended.add(route)
        if route < last_out:
            first, count = parts_out[route]
            at = pl.ds(first * 128, count * 128)
            outs.append(local(grads.at[own_rows, at], first_ref.at[:, at], len(outs)))
        if not swapped and all(r in ended for r in range(last_out, len(SCATTER_ORDERS))):
            swapped = True
            swap[0] = seconds[pl.ds(pl.multiple_of(own_second + other * h, h), h), :]
            second_swap = remote(swap.at[0], swap.at[1], 5, partner)
            second_swap.start()
            mine = seconds.at[pl.ds(pl.multiple_of(own_second + core * h, h), h), :]
            outs.append(local(mine, second_ref.at[core], len(outs)))

    def whole(route, buf, other_buf, parts, last, cols):
        if route >= last:
            return lambda n: other_buf.at[pl.ds(0, n), pl.ds((route - last) * cols, cols)]
        first, count = parts[route]
        return lambda n: buf.at[pl.ds(0, n), pl.ds(first * 128, count * 128)]

    for route in range(len(GATHER_ORDERS)):
        unit = pair if route >= last_in else h
        part = whole(route, wbuf, w2buf, parts_in, last_in, cols_in)
        ways_in.drain(route, part, unit, send_sems)
    for route in range(len(SCATTER_ORDERS)):
        unit = pair if route >= last_out else h
        part = whole(route, grads, seconds, parts_out, last_out, cols_out)
        sent = part((nz * nx * ny - 1) * unit)
        pltpu.make_async_copy(sent, sent, sum_send_sems.at[route]).wait()

    @pl.when(y == 1)
    def _():
        fine_halo.wait_send()
        coarse_halo.wait_send()

    second_swap.wait()
    outs.append(local(swap.at[1], second_ref.at[other], len(outs)))
    for copy in outs:
        copy.wait()


def finish_kernel(shift, sums_ref, sets_ref, first_ref, second_ref):
    y = lax.axis_index("tile")
    h, share = first_ref.shape
    depth = sets_ref.shape[2]
    bins = sums_ref.shape[1] // 128
    f32 = jnp.float32
    halves = lax.broadcasted_iota(jnp.int32, (h, 128), 1)
    back_shift = (128 - shift) % 128

    def turned(i):
        tile = sums_ref[:, 128 * i : 128 * (i + 1)].astype(f32)
        return tile, pltpu.roll(tile, back_shift, axis=1)

    now = turned(0)
    for i in range(bins):
        width = min(128, share - 128 * i)
        following = turned(i + 1) if i + 1 < bins else now
        late = jnp.where(halves < 128 - shift, now[1], following[1])
        first_ref[:, 128 * i : 128 * i + width] = jnp.where(y == 0, now[0], late)[:, :width]
        now = following
    for m in range(depth // 128):
        at = slice(128 * m, 128 * (m + 1))
        set_0 = sets_ref[0, :, at].astype(f32)
        set_1 = sets_ref[1, :, at].astype(f32)
        second_ref[:, 256 * m : 256 * m + 128] = jnp.where(
            halves < h, set_0, pltpu.roll(set_1, h, axis=1)
        )
        second_ref[:, 256 * m + 128 : 256 * m + 256] = jnp.where(
            halves < h, pltpu.roll(set_0, h, axis=1), set_1
        )


def per_device_by_chips(
    grid, proposal_boxes, level_plan, fine_map, coarse_map, first_weight, second_weight, upstream
):
    nz, nx, ny, cores = grid
    chips = nz * nx
    props = level_plan.shape[1]
    capacity = props // ny
    fine_tile, coarse = fine_map[0], coarse_map[0]
    fine_rows, fine_cols, channels = fine_tile.shape
    coarse_rows = coarse.shape[0]
    share, h = first_weight.shape
    feats = share * ny
    bins = max(-(-((t + 1) * share) // 128) - t * share // 128 for t in range(ny))
    lanes = bins * 128
    hidden_size = upstream.shape[2]
    depth = second_weight.shape[0] // cores
    pair = cores * h
    low, f32 = jnp.bfloat16, jnp.float32
    sizes = (nz, nx, ny)
    parts_out = cut(bins, SCATTER_SHARES)
    slot_counts = [sum(slots_of(sizes, order)) for order in SCATTER_ORDERS]
    rows_all = chips * h
    batch = cores * capacity
    q = chips * ny
    dma = pltpu.SemaphoreType.DMA
    anywhere = pl.BlockSpec(memory_space=pl.ANY)
    vmem = pl.BlockSpec(memory_space=pltpu.VMEM)
    slot_shapes = [
        (n, h, parts_out[i][1] * 128)
        if i < len(parts_out)
        else (n, pair, depth // (len(SCATTER_ORDERS) - len(parts_out)))
        for i, n in enumerate(slot_counts)
    ]
    sums, sets = pl.pallas_call(
        functools.partial(step_kernel, grid),
        out_shape=(
            jax.ShapeDtypeStruct((h, lanes), low),
            jax.ShapeDtypeStruct((cores, h, depth), low),
        ),
        in_specs=[vmem, vmem] + [anywhere] * 5,
        out_specs=(anywhere, anywhere),
        scratch_shapes=[
            pltpu.VMEM((h, share), low),
            pltpu.VMEM((h, cores * depth), low),
            pltpu.VMEM((cores, h, depth), low),
            pltpu.VMEM((ny * rows_all, lanes), low),
            pltpu.VMEM((ny * hidden_size, depth), low),
            pltpu.VMEM((fine_rows + HALO, fine_cols, channels), low),
            pltpu.VMEM((coarse_rows + HALO, coarse.shape[1], channels), low),
            pltpu.VMEM((fine_rows + coarse_rows + 2 * HALO, fine_cols, channels), f32),
            pltpu.VMEM((ROWS_PAD * GROUP, 128), f32),
            pltpu.VMEM((batch, feats), low),
            pltpu.VMEM((props, hidden_size), low),
            pltpu.VMEM((batch, hidden_size), low),
            pltpu.VMEM((hidden_size, batch), low),
            pltpu.VMEM((rows_all, batch), f32),
            pltpu.VMEM((rows_all, batch), f32),
            pltpu.VMEM((rows_all, batch), low),
            pltpu.VMEM((rows_all, batch), low),
            pltpu.VMEM((ny * rows_all, lanes), low),
            pltpu.VMEM((ny * hidden_size, depth), low),
            pltpu.VMEM((2, h, depth), low),
            pltpu.VMEM((8, capacity), jnp.int32),
            pltpu.VMEM((8, capacity), f32),
            pltpu.SMEM((8, capacity), jnp.int32),
            pltpu.SMEM((8, capacity), f32),
            dma((max(7, len(SCATTER_ORDERS) + 2),)),
            dma((len(GATHER_ORDERS), 6)),
            dma((len(GATHER_ORDERS), q)),
            dma((len(SCATTER_ORDERS),)),
            dma((sum(slot_counts),)),
            dma((6,)),
            dma((6,)),
        ]
        + [pltpu.VMEM(shape, low) for shape in slot_shapes],
        compiler_params=pltpu.CompilerParams(
            collective_id=0, has_side_effects=True, vmem_limit_bytes=64000 * 1024
        ),
        name="step",
    )(
        proposal_boxes[0],
        level_plan,
        first_weight.T,
        second_weight.T,
        upstream[0],
        fine_tile,
        coarse,
    )
    shift = share - 128 * min(share // 128, feats // 128 - bins)
    first, second = pl.pallas_call(
        functools.partial(finish_kernel, shift),
        out_shape=(
            jax.ShapeDtypeStruct((h, share), f32),
            jax.ShapeDtypeStruct((h, cores * depth), f32),
        ),
        in_specs=[vmem, vmem],
        out_specs=(vmem, vmem),
        name="finish",
    )(sums, sets)
    return (first.T, second.T)


def solution(mesh):
    placed = (
        P("dp", None, None),
        P("dp", None),
        P("dp", "tile", None, None),
        P("dp", "tile", None, None),
        P("tile", "dp"),
        P("tile", "dp"),
        P("dp", None, None),
    )
    grid = chip_grid(mesh)
    tiles = mesh.shape["tile"]
    body = per_device_by_bands
    if grid is not None and tiles == 2 and grid[1] <= 2 and grid[2] == 2:
        body = functools.partial(per_device_by_chips, (grid[0], grid[1], tiles, grid[2]))
    return jax.shard_map(
        body,
        mesh=mesh,
        in_specs=placed,
        out_specs=(P("tile", "dp"), P("tile", "dp")),
        check_vma=False,
    )
```

```python
import functools

import jax
import jax.numpy as jnp
from jax import lax
from jax.experimental import pallas as pl
from jax.experimental.pallas import tpu as pltpu
from jax.sharding import PartitionSpec as P

WIN = 16
BINS = 7
ROWS_PAD = 56
GROUP = 16


def from_ahead(block, axis, distance):
    if distance == 0:
        return block
    size = lax.axis_size(axis)
    return lax.ppermute(block, axis, [(i, (i - distance) % size) for i in range(size)])


def halo_from_next(block, axis):
    size = lax.axis_size(axis)
    return lax.ppermute(block, axis, [(i + 1, i) for i in range(size - 1)])


def gelu_parts(hidden):
    factor = 0.7978845608028654
    cubic_term = 0.044715
    inner_term = factor * (hidden + cubic_term * hidden * hidden * hidden)
    tangent = jnp.tanh(inner_term)
    gelu_value = 0.5 * hidden * (1.0 + tangent)
    gelu_slope = 0.5 * (1.0 + tangent) + 0.5 * hidden * (1.0 - tangent * tangent) * factor * (
        1.0 + 3.0 * cubic_term * hidden * hidden
    )
    return (gelu_value, gelu_slope)


def crop_kernel(starts, width, cells_ref, geo_ref, maps_ref, out_ref, wide, stage):
    step = pl.program_id(0)

    @pl.when(step == 0)
    def _():
        def widen(r, carry):
            wide[r] = maps_ref[r].astype(jnp.float32)
            return carry

        lax.fori_loop(0, maps_ref.shape[0], widen, 0)

    shape = (ROWS_PAD, WIN * WIN)
    k = lax.broadcasted_iota(jnp.int32, shape, 0).astype(jnp.float32)
    i_bin = jnp.floor((k + 0.5) * (1.0 / BINS))
    j_bin = k - BINS * i_bin
    i_mid = i_bin + 0.5
    j_mid = j_bin + 0.5
    lane = lax.broadcasted_iota(jnp.int32, shape, 1)
    r_cell = (lane >> 4).astype(jnp.float32)
    q_cell = (lane & 15).astype(jnp.float32)
    for p in range(GROUP):
        n = step * GROUP + p
        row = cells_ref[0, n]
        col = cells_ref[1, n]
        row_w = jnp.maximum(0.0, 1.0 - jnp.abs(i_mid * geo_ref[1, n] + geo_ref[0, n] - r_cell))
        col_w = jnp.maximum(0.0, 1.0 - jnp.abs(j_mid * geo_ref[3, n] + geo_ref[2, n] - q_cell))
        weights = (row_w * col_w).astype(jnp.bfloat16)
        window = jnp.concatenate(
            [wide[row + r, pl.ds(col, WIN), :] for r in range(WIN)], axis=0
        ).astype(jnp.bfloat16)
        crop = jnp.dot(weights, window, preferred_element_type=jnp.float32)
        stage[pl.ds(p, ROWS_PAD, stride=GROUP), :] = crop
    for t, first in enumerate(starts):
        for m in range(width):
            at = (first + m) * GROUP
            out_ref[t, :, m * 128 : (m + 1) * 128] = stage[at : at + GROUP, :].astype(jnp.bfloat16)


def make_crops(cells, geo, maps, starts, width, capacity):
    tiles = len(starts)
    lanes = width * 128
    return pl.pallas_call(
        functools.partial(crop_kernel, starts, width),
        grid=(capacity // GROUP,),
        out_shape=jax.ShapeDtypeStruct((tiles, capacity, lanes), jnp.bfloat16),
        in_specs=[
            pl.BlockSpec(memory_space=pltpu.SMEM),
            pl.BlockSpec(memory_space=pltpu.SMEM),
            pl.BlockSpec(maps.shape, lambda g: (0, 0, 0)),
        ],
        out_specs=pl.BlockSpec((tiles, GROUP, lanes), lambda g: (0, g, 0)),
        scratch_shapes=[
            pltpu.VMEM(maps.shape, jnp.float32),
            pltpu.VMEM((ROWS_PAD * GROUP, 128), jnp.float32),
        ],
        compiler_params=pltpu.CompilerParams(
            dimension_semantics=("arbitrary",), vmem_limit_bytes=48 * 1024 * 1024
        ),
        cost_estimate=pl.CostEstimate(
            flops=capacity * ROWS_PAD * WIN * WIN * 128 * 16,
            bytes_accessed=2 * maps.size + 2 * tiles * capacity * lanes,
            transcendentals=0,
        ),
        name="crops",
    )(cells, geo, maps)


def per_device_by_bands(
    proposal_boxes, level_plan, fine_map, coarse_map, first_weight, second_weight, upstream
):
    tile_count = lax.axis_size("tile")
    band = lax.axis_index("tile")
    num_props = level_plan.shape[1]
    capacity = max(num_props // 4, num_props // tile_count)
    fine_tile = fine_map[0]
    coarse = coarse_map[0]
    fine_rows, fine_cols, channels = fine_tile.shape
    coarse_rows, coarse_cols = (coarse.shape[0], coarse.shape[1])

    top_rows = jnp.concatenate([fine_tile[:WIN], coarse[:WIN]], axis=1)
    below_rows = halo_from_next(top_rows, "tile")

    share_feats = first_weight.shape[0]
    feats = share_feats * tile_count
    width = max(
        -(-((t + 1) * share_feats) // 128) - t * share_feats // 128 for t in range(tile_count)
    )
    starts = [min(t * share_feats // 128, feats // 128 - width) for t in range(tile_count)]
    lanes = width * 128
    feat_off = band * share_feats - 128 * jnp.minimum(
        band * share_feats // 128, feats // 128 - width
    )

    first_rows = lax.dynamic_update_slice(
        jnp.zeros((first_weight.shape[1], lanes), jnp.bfloat16),
        first_weight.T,
        (0, feat_off),
    )
    both = lax.all_gather(
        jnp.concatenate([first_rows, second_weight.T], axis=1), "dp", axis=0, tiled=True
    )
    first_all = both[:, :lanes]
    second_all = both[:, lanes:]

    fields = proposal_boxes[0]
    levels = level_plan[0]
    owner = fields[0] // (4 * fine_rows)
    members = (owner[:, None] == jnp.arange(tile_count, dtype=jnp.int32)[None, :]).astype(jnp.int32)
    rank = jnp.sum((jnp.cumsum(members, axis=0) - 1) * members, axis=1)
    relative = lax.rem(owner - band + tile_count, tile_count)
    slot_id = relative * capacity + rank
    slots = tile_count * capacity
    chosen = slot_id[None, :] == jnp.arange(slots, dtype=jnp.int32)[:, None]
    upstream_slots = jnp.dot(
        chosen.astype(jnp.bfloat16), upstream[0], preferred_element_type=jnp.float32
    ).astype(jnp.bfloat16)
    mine = chosen[:capacity].astype(jnp.int32)
    top, left, height, box_width = (
        jnp.sum(mine * fields[f][None, :], axis=1) for f in range(4)
    )
    level = jnp.sum(mine * levels[None, :], axis=1)

    stride = jnp.where(level == 0, 4, 8).astype(jnp.int32)
    is_fine = level == 0
    first_row = top // stride
    local_row = jnp.clip(
        first_row - band * jnp.where(is_fine, fine_rows, coarse_rows),
        0,
        jnp.where(is_fine, fine_rows, coarse_rows) - 1,
    )
    first_col = jnp.minimum(left // stride, jnp.where(is_fine, fine_cols, coarse_cols) - WIN)
    cells = jnp.stack(
        [local_row + jnp.where(is_fine, 0, fine_rows + WIN), first_col], axis=0
    ).astype(jnp.int32)
    stride_float = stride.astype(jnp.float32)
    geo = jnp.stack(
        [
            top.astype(jnp.float32) / stride_float - first_row.astype(jnp.float32),
            height.astype(jnp.float32) / (7.0 * stride_float),
            left.astype(jnp.float32) / stride_float - first_col.astype(jnp.float32),
            box_width.astype(jnp.float32) / (7.0 * stride_float),
        ],
        axis=0,
    )

    side = ((0, 0), (0, fine_cols - coarse_cols), (0, 0))
    maps = jnp.concatenate(
        [
            fine_tile,
            below_rows[:, :fine_cols],
            jnp.pad(coarse, side),
            jnp.pad(below_rows[:, fine_cols:], side),
        ],
        axis=0,
    )
    crop_blocks = make_crops(cells, geo, maps, starts, width, capacity)
    own_feats = jnp.concatenate(
        [
            from_ahead(
                lax.dynamic_index_in_dim(
                    crop_blocks, lax.rem(band - d + tile_count, tile_count), 0, keepdims=False
                ),
                "tile",
                d,
            )
            for d in range(tile_count)
        ],
        axis=0,
    )

    partial_hidden = lax.dot_general(
        own_feats, first_all, (((1,), (1,)), ((), ())), preferred_element_type=jnp.float32
    ).astype(jnp.bfloat16)
    share = second_weight.shape[0]

    def in_my_order(block, d):
        return jnp.roll(block, d * capacity, axis=0) if d else block

    hidden_own = 0.0
    for d in range(tile_count):
        to = lax.rem(band - d + tile_count, tile_count)
        piece = lax.dynamic_slice_in_dim(partial_hidden, to * share, share, axis=1)
        hidden_own = hidden_own + in_my_order(from_ahead(piece, "tile", d), d).astype(jnp.float32)
    gelu_value, gelu_slope = gelu_parts(hidden_own)
    activated = gelu_value.astype(jnp.bfloat16)
    back_grad = jnp.dot(upstream_slots, second_all, preferred_element_type=jnp.float32)
    pre_own = (back_grad * gelu_slope).astype(jnp.bfloat16)
    ahead = [in_my_order(from_ahead(pre_own, "tile", d), d) for d in range(tile_count)]
    twice = jnp.concatenate(ahead + ahead[:-1], axis=1)
    pre_grad = lax.dynamic_slice_in_dim(
        twice, lax.rem(tile_count - band, tile_count) * share, tile_count * share, axis=1
    )
    over_rows = (((0,), (0,)), ((), ()))
    second_part = lax.dot_general(
        upstream_slots, activated, over_rows, preferred_element_type=jnp.float32
    ).astype(jnp.bfloat16)
    first_part = lax.dot_general(
        pre_grad, own_feats, over_rows, preferred_element_type=jnp.float32
    ).astype(jnp.bfloat16)
    summed = lax.psum_scatter(
        jnp.concatenate([first_part, second_part], axis=1), "dp", scatter_dimension=0, tiled=True
    ).astype(jnp.float32)
    first_grad = lax.dynamic_slice_in_dim(summed[:, :lanes], feat_off, share_feats, axis=1).T
    second_grad = summed[:, lanes:].T
    return (first_grad, second_grad)


MESH = pl.DeviceIdType.MESH
REACH = 15
HALO = REACH - 1
NT = (((1,), (1,)), ((), ()))
NN = (((1,), (0,)), ((), ()))


def chip_grid(mesh):
    chips = [getattr(device, "coords", None) for device in mesh.devices[:, 0]]
    if chips[0] is None:
        return None
    cores = sum(1 for c in chips if tuple(c) == tuple(chips[0]))
    chips = [tuple(c) for c in chips[::cores]]
    if len(chips) == 1:
        return (1, 1, cores)
    axis = [a != b for a, b in zip(chips[0], chips[1])].index(True)
    fast = 1
    while fast < len(chips) and all(
        a == b or i == axis for i, (a, b) in enumerate(zip(chips[0], chips[fast]))
    ):
        fast += 1
    return (len(chips) // fast, fast, cores)


def offsets(size):
    if size == 1:
        return [0]
    if size == 2:
        return [0, 1]
    return [0] + [s * d for d in range(1, size) for s in (-1, 1)]


def steps_of(size):
    return {1: [], 2: [1]}.get(size, [-1, 1])


def moved(position, size, rel):
    if rel == 0 or size == 1:
        return position
    return 1 - position if size == 2 else position + rel


def last_axis(order, rel):
    used = [j for j in range(3) if rel[order[j]]]
    return used[-1] if used else -1


def onward(sizes, order, rel):
    last = last_axis(order, rel)
    hops = []
    if last >= 0:
        axis = order[last]
        if sizes[axis] > 2 and abs(rel[axis]) < sizes[axis] - 1:
            hops.append((last, axis, -1 if rel[axis] > 0 else 1))
    for j in range(last + 1, 3):
        hops.extend((j, order[j], step) for step in steps_of(sizes[order[j]]))
    return hops


def arrival_order(sizes, routes, extra):
    import heapq
    import itertools

    places = list(itertools.product(*(range(n) for n in sizes)))
    queue, waiting, busy = [], {}, set()
    seen, tick = {}, itertools.count()

    def start(link, now):
        if link not in busy and waiting.get(link):
            busy.add(link)
            load, arrival = waiting[link].pop(0)
            heapq.heappush(queue, (now + load, next(tick), link, arrival))

    def arrive(place, route, rel, now):
        seen.setdefault((route, rel), []).append(now)
        for _, axis, step in onward(sizes, routes[route][0], rel):
            target = list(place)
            target[axis] = moved(place[axis], sizes[axis], step)
            if not 0 <= target[axis] < sizes[axis]:
                continue
            there = list(rel)
            there[axis] = rel[axis] - step if sizes[axis] > 2 else 1
            link = (place, axis, step)
            waiting.setdefault(link, []).append(
                (routes[route][1], (tuple(target), route, tuple(there)))
            )
            start(link, now)

    first = {}
    for place in places:
        for route in extra[1]:
            arrive(place, route, (0, 0, 0), 0.0)
        if extra[0] and place[2] == 1:
            waiting.setdefault((place, 2, 1), []).append((extra[0], None))
            start((place, 2, 1), 0.0)
        for route in range(len(routes)):
            if route not in extra[1]:
                arrive(place, route, (0, 0, 0), 0.0)
    end = 0.0
    while queue:
        now, _, link, arrival = heapq.heappop(queue)
        end = now
        busy.discard(link)
        if arrival is not None:
            arrive(*arrival, now)
        start(link, now)
    key = {event: sum(t) / len(t) for event, t in seen.items()}
    for _ in range(sum(sizes)):
        for (route, rel) in list(key):
            for _, axis, step in onward(sizes, routes[route][0], rel):
                there = list(rel)
                there[axis] = rel[axis] - step if sizes[axis] > 2 else 1
                event = (route, tuple(there))
                if event in key:
                    key[event] = max(key[event], key[(route, rel)] + 1e-3)
    return sorted(key, key=lambda e: (key[e], e)), key, end


def slots_of(sizes, order):
    counts, before = [], 1
    for j in range(3):
        n = sizes[order[j]]
        counts.append(before * (n + 1 if n > 2 else 1))
        before *= n
    return counts


def when(conds, body):
    if not conds:
        body()
        return
    total = conds[0]
    for cond in conds[1:]:
        total = jnp.logical_and(total, cond)
    pl.when(total)(body)


class Routes:
    def __init__(self, sizes, position, core, cores, orders):
        self.sizes, self.position = sizes, position
        self.core, self.cores = core, cores
        self.orders = orders
        self.slot_counts = [slots_of(sizes, order) for order in orders]
        self.slot_base = [sum(sum(c) for c in self.slot_counts[:i]) for i in range(len(orders))]

    def inside(self, axis, rel):
        if rel == 0 or self.sizes[axis] <= 2:
            return []
        p = self.position[axis]
        return [p < self.sizes[axis] - rel] if rel > 0 else [p >= -rel]

    def valid(self, rel):
        return sum((self.inside(axis, rel[axis]) for axis in range(3)), [])

    def at(self, rel):
        return [moved(self.position[a], self.sizes[a], rel[a]) for a in range(3)]

    def device(self, axis, step):
        there = list(self.position)
        there[axis] = moved(there[axis], self.sizes[axis], step)
        return ((there[0] * self.sizes[1] + there[1]) * self.cores + self.core, there[2])

    def back_step(self, order, rel):
        axis = order[last_axis(order, rel)]
        return axis, (1 if self.sizes[axis] == 2 or rel[axis] > 0 else -1)

    def number(self, place):
        return (place[0] * self.sizes[1] + place[1]) * self.sizes[2] + place[2]

    def direction(self, axis, step):
        return axis + 1 if axis else (1 if step > 0 else 0)

    def drain(self, route, whole, unit, sems):
        order, before = self.orders[route], 1
        for axis in order:
            n, p = self.sizes[axis], self.position[axis]
            for step in steps_of(n):
                for at in range(n) if n > 2 else [0]:
                    sent = before * ((at + 1 if step > 0 else n - at) if n > 2 else 1)
                    if n > 2 and not 0 <= at + step < n:
                        continue

                    def wait(axis=axis, step=step, sent=sent):
                        part = whole(sent * unit)
                        pltpu.make_async_copy(
                            part, part, sems.at[route, self.direction(axis, step)]
                        ).wait()

                    when([p == at] if n > 2 else [], wait)
            before *= n

    def gather(self, route, rel, ref_of, send_sems, recv_sems):
        order = self.orders[route]

        def body():
            place = self.at(rel)
            ref = ref_of(place)
            q = self.number(place)

            def hop(axis, step):
                return pltpu.make_async_remote_copy(
                    src_ref=ref,
                    dst_ref=ref,
                    send_sem=send_sems.at[route, self.direction(axis, step)],
                    recv_sem=recv_sems.at[route, q],
                    device_id=self.device(axis, step),
                    device_id_type=MESH,
                )

            if last_axis(order, rel) >= 0:
                hop(*self.back_step(order, rel)).wait_recv()
            for _, axis, step in onward(self.sizes, order, rel):
                copy = hop(axis, step)
                when(self.inside(axis, step), copy.start)

        when(self.valid(rel), body)

    def slot(self, route, phase, side, place, here):
        order, counts = self.orders[route], self.slot_counts[route]
        index = 0
        for j in range(phase):
            index = index * self.sizes[order[j]] + place[order[j]]
        n = self.sizes[order[phase]]
        if n > 2:
            index = index * (n + 1) + (n if here and side > 0 else place[order[phase]])
        return sum(counts[:phase]) + index

    def scatter(self, route, rel, ref_of, slots, add, send_sems, recv_sems):
        order = self.orders[route]

        def body():
            place = self.at(rel)
            ref = ref_of(place)
            base = self.slot_base[route]
            for phase, axis, step in onward(self.sizes, order, rel):
                slot = self.slot(route, phase, step, place, rel[axis] == 0)

                def take(axis=axis, step=step, slot=slot):
                    pltpu.make_async_remote_copy(
                        src_ref=ref,
                        dst_ref=slots.at[slot],
                        send_sem=send_sems.at[route],
                        recv_sem=recv_sems.at[base + slot],
                        device_id=self.device(axis, step),
                        device_id_type=MESH,
                    ).wait_recv()
                    add(ref, slots.at[slot])

                when(self.inside(axis, step), take)
            phase = last_axis(order, rel)
            if phase >= 0:
                axis, step = self.back_step(order, rel)
                here = rel[axis] - step == 0
                slot = self.slot(route, phase, -step, place, here)
                pltpu.make_async_remote_copy(
                    src_ref=ref,
                    dst_ref=slots.at[slot],
                    send_sem=send_sems.at[route],
                    recv_sem=recv_sems.at[base + slot],
                    device_id=self.device(axis, step),
                    device_id_type=MESH,
                ).start()

        when(self.valid(rel), body)


def cut(bins, shares):
    edges = [0]
    for i in range(1, len(shares) + 1):
        edges.append(round(bins * sum(shares[:i]) / sum(shares)))
    return [(a, b - a) for a, b in zip(edges, edges[1:])]


GATHER_ORDERS = ((2, 0, 1), (0, 1, 2), (1, 2, 0), (2, 0, 1), (0, 1, 2))
GATHER_SHARES = (12, 9, 4)
SCATTER_ORDERS = ((2, 0, 1), (2, 0, 1), (0, 1, 2), (0, 1, 2), (1, 2, 0), (2, 0, 1))
SCATTER_SHARES = (3, 3, 8, 8, 3)
HALO_AFTER = 3
EARLY, DURING = 13, 56
CROP_AT = (
        2, 2, 2, 2, 3, 3, 3, 3, 3, 4, 5, 6, 6, 7, 7, 7, 7, 7, 7, 8, 8, 8, 8, 9, 9, 9, 10, 11,
        11, 11, 11, 11, 12, 12, 13, 13, 13, 13, 13, 13, 13, 13, 13, 13, 13, 13, 14, 15, 15, 15,
        15, 15, 15, 15, 15, 15
)
GATHER_CODES = {
    (4, 2, 2): (
        0, 84, 112, 28, 56, 116, 4, 8, 36, 16, 120, 44, 1, 124, 32, 12, 58, 40, 24, 85, 52, 9,
        5, 48, 20, 64, 57, 54, 46, 18, 136, 118, 62, 128, 13, 66, 17, 113, 3, 125, 38, 93, 26,
        121, 45, 42, 60, 55, 132, 30, 22, 87, 21, 88, 2, 96, 25, 50, 34, 59, 29, 92, 49, 138,
        89, 126, 70, 6, 14, 33, 134, 137, 97, 74, 61, 68, 11, 47, 108, 37, 105, 23, 78, 100, 7,
        65, 63, 101, 72, 130, 104, 117, 67, 86, 10, 19, 53, 82, 122, 27, 69, 80, 109, 114, 73,
        51, 15, 107, 95, 110, 76, 90, 75, 31, 98, 106, 41, 71, 39, 35, 43, 91, 127, 135, 94,
        129, 77, 133, 81, 131, 139, 102, 123, 119, 111, 103, 99, 83, 79, 115
    ),
}
SCATTER_CODES = {
    (4, 2, 2): (
        43, 47, 137, 132, 55, 67, 81, 51, 71, 133, 134, 50, 35, 34, 138, 26, 89, 162, 49, 83,
        139, 23, 18, 107, 39, 105, 22, 147, 27, 163, 63, 131, 79, 42, 95, 126, 111, 15, 129,
        167, 103, 159, 53, 7, 14, 48, 69, 125, 19, 41, 155, 6, 46, 54, 33, 21, 20, 124, 130,
        161, 45, 160, 99, 135, 91, 166, 158, 136, 146, 117, 77, 106, 123, 121, 25, 13, 75, 128,
        38, 154, 12, 82, 62, 122, 151, 37, 165, 143, 61, 97, 116, 30, 109, 17, 164, 110, 40,
        118, 127, 5, 101, 150, 157, 152, 66, 78, 98, 102, 153, 11, 70, 87, 65, 52, 44, 24, 119,
        80, 156, 93, 4, 104, 90, 74, 144, 115, 73, 148, 94, 3, 10, 76, 108, 142, 145, 59, 31,
        96, 16, 149, 100, 85, 36, 2, 141, 68, 32, 9, 120, 88, 86, 72, 113, 8, 114, 92, 29, 60,
        1, 64, 57, 58, 140, 0, 112, 28, 84, 56
    ),
}


def unpack(codes, sizes):
    spans = [offsets(n) for n in sizes]
    events = []
    for code in codes:
        code, k = divmod(code, len(spans[2]))
        code, j = divmod(code, len(spans[1]))
        route, i = divmod(code, len(spans[0]))
        events.append((route, (spans[0][i], spans[1][j], spans[2][k])))
    return events


def step_kernel(grid, *refs):
    fields_ref, levels_ref, w1_ref, w2_ref, up_ref, fine_ref, coarse_ref = refs[:7]
    first_ref, second_ref = refs[7:9]
    (
        w_in,
        w2_in,
        w2_sets,
        wbuf,
        w2buf,
        fine_low,
        coarse_low,
        wide,
        stage,
        crops,
        up_all,
        upb,
        uptb,
        back,
        hidden,
        acts,
        pres,
        grads,
        seconds,
        swap,
        cells_v,
        geo_v,
        cells_ref,
        geo_ref,
        local_sems,
        send_sems,
        recv_sems,
        sum_send_sems,
        sum_recv_sems,
        core_send,
        core_recv,
    ) = refs[9:40]
    slot_refs = refs[40:]
    nz, nx, ny, cores = grid
    sizes = (nz, nx, ny)
    dp = lax.axis_index("dp")
    y = lax.axis_index("tile")
    core = dp % cores
    chip = dp // cores
    x = chip % nx
    z = chip // nx
    position = (z, x, y)
    other = 1 - core
    partner = (chip * cores + other, y)
    ways_in = Routes(sizes, position, core, cores, GATHER_ORDERS)
    ways_out = Routes(sizes, position, core, cores, SCATTER_ORDERS)
    h, share = w1_ref.shape
    lanes = wbuf.shape[1]
    bins = lanes // 128
    all_rows = nz * nx * h
    fine_rows, fine_cols, _ = fine_ref.shape
    coarse_rows, coarse_cols, _ = coarse_ref.shape
    batch, feats = crops.shape
    capacity = batch // cores
    depth = w2buf.shape[1]
    hidden_size = up_ref.shape[1]
    pair = cores * h
    starts = [min(t * share // 128, feats // 128 - bins) for t in range(ny)]
    shift = share - 128 * starts[1]
    parts_in = cut(bins, GATHER_SHARES)
    parts_out = cut(bins, SCATTER_SHARES)
    f32, low = jnp.float32, jnp.bfloat16

    barrier = pltpu.get_barrier_semaphore()
    pl.semaphore_signal(barrier, inc=1, device_id=partner, device_id_type=MESH)
    peers = 1
    for axis in range(3):
        for step in steps_of(sizes[axis]):

            def greet(axis=axis, step=step):
                pl.semaphore_signal(
                    barrier, inc=1, device_id=ways_in.device(axis, step), device_id_type=MESH
                )

            near = ways_in.inside(axis, step)
            when(near, greet)
            peers = peers + (near[0].astype(jnp.int32) if near else 1)

    def rows(start, size):
        return pl.ds(pl.multiple_of(start, size), size)

    def local(src, dst, i):
        copy = pltpu.make_async_copy(src, dst, local_sems.at[i])
        copy.start()
        return copy

    def remote(src, dst, i, device):
        return pltpu.make_async_remote_copy(
            src_ref=src,
            dst_ref=dst,
            send_sem=core_send.at[i],
            recv_sem=core_recv.at[i],
            device_id=device,
            device_id_type=MESH,
        )

    w_copy = local(w1_ref, w_in, 0)
    w2_copy = local(w2_ref, w2_in, 1)
    fine_copy = local(fine_ref, fine_low.at[pl.ds(0, fine_rows)], 2)
    coarse_copy = local(coarse_ref, coarse_low.at[pl.ds(0, coarse_rows)], 3)
    up_copy = local(up_ref, up_all, 4)
    halves = lax.broadcasted_iota(jnp.int32, (h, 128), 1)

    w_copy.wait()
    own_rows = pl.ds(pl.multiple_of(y * all_rows + chip * h, h), h)

    def turned(i):
        width = min(128, share - 128 * i) if i >= 0 else 0
        if width <= 0:
            return jnp.zeros((h, 128), f32), jnp.zeros((h, 128), f32)
        now = w_in[:, 128 * i : 128 * i + width].astype(f32)
        if width < 128:
            now = jnp.concatenate([now, jnp.zeros((h, 128 - width), f32)], axis=1)
        return now, (pltpu.roll(now, shift, axis=1) if shift else now)

    def turn(first, count):
        before = turned(first - 1)[1]
        for i in range(first, first + count):
            now, after = turned(i)
            late = jnp.where(halves < shift, before, after)
            before = after
            wbuf[own_rows, 128 * i : 128 * (i + 1)] = jnp.where(y == 0, now, late).astype(low)


    last_in = len(GATHER_SHARES)
    last_out = len(SCATTER_SHARES)
    cols_in = depth // (len(GATHER_ORDERS) - last_in)
    cols_out = depth // (len(SCATTER_ORDERS) - last_out)
    loads_in = [
        (order, parts_in[i][1] if i < last_in else cols_in * pair // (h * 128))
        for i, order in enumerate(GATHER_ORDERS)
    ]
    loads_out = [
        (order, parts_out[i][1] if i < last_out else cols_out * pair // (h * 128))
        for i, order in enumerate(SCATTER_ORDERS)
    ]
    halo_load = HALO * (fine_cols + coarse_cols) // h
    if sizes in GATHER_CODES:
        events = unpack(GATHER_CODES[sizes], sizes)
        sum_events = unpack(SCATTER_CODES[sizes], sizes)
    else:
        events = arrival_order(sizes, loads_in, (halo_load, (0,)))[0]
        sum_events = arrival_order(sizes, loads_out, (0, ()))[0][::-1]

    def gather_ref(route):
        if route >= last_in:
            return lambda q: w2buf.at[
                rows(q[2] * hidden_size + (q[0] * nx + q[1]) * pair, pair),
                pl.ds((route - last_in) * cols_in, cols_in),
            ]
        first, count = parts_in[route]
        return lambda q: wbuf.at[
            rows(q[2] * all_rows + (q[0] * nx + q[1]) * h, h), pl.ds(first * 128, count * 128)
        ]

    def gather(event):
        route, rel = event
        ways_in.gather(route, rel, gather_ref(route), send_sems, recv_sems)

    below = ways_in.device(2, 1)
    fine_halo = remote(
        fine_ref.at[pl.ds(0, HALO)], fine_low.at[pl.ds(fine_rows, HALO)], 1, below
    )
    coarse_halo = remote(
        coarse_ref.at[pl.ds(0, HALO)], coarse_low.at[pl.ds(coarse_rows, HALO)], 2, below
    )
    own = [e for e in events if e[1] == (0, 0, 0)]
    todo = [e for e in events if e[1] != (0, 0, 0)]
    own.sort(key=lambda e: e[0] >= last_in)
    for n, event in enumerate(own[:last_in]):
        turn(*parts_in[event[0]])
        if n == 0:
            pl.semaphore_wait(barrier, peers)
        gather(event)
        if n + 1 == min(HALO_AFTER, last_in):

            @pl.when(y == 1)
            def _():
                fine_halo.start()
                coarse_halo.start()

    w2_copy.wait()
    for m in range(depth // 128):
        a = w2_in[:, 256 * m : 256 * m + 128].astype(f32)
        b = w2_in[:, 256 * m + 128 : 256 * m + 256].astype(f32)
        at = slice(128 * m, 128 * (m + 1))
        w2_sets[0, :, at] = jnp.where(halves < h, a, pltpu.roll(b, h, axis=1)).astype(low)
        w2_sets[1, :, at] = jnp.where(halves < h, pltpu.roll(a, h, axis=1), b).astype(low)
    w2_rows = pl.ds(pl.multiple_of(y * hidden_size + chip * pair + core * h, h), h)
    w2buf[w2_rows, :] = w2_sets[core]

    w2_swap = remote(w2_sets.at[other], w2buf.at[w2_rows, :], 0, partner)
    w2_swap.start()
    w2_swap.wait()
    for event in own[last_in:]:
        gather(event)

    events = own + todo

    member = jnp.logical_and(
        fields_ref[0:1, :] >= y * (4 * fine_rows), fields_ref[0:1, :] < (y + 1) * (4 * fine_rows)
    )
    props = fields_ref.shape[1]
    ones = jnp.broadcast_to(jnp.where(member, 1.0, 0.0), (8, props)).astype(low)
    upto = lax.broadcasted_iota(jnp.int32, (props, props), 0) <= lax.broadcasted_iota(
        jnp.int32, (props, props), 1
    )
    rank = jnp.dot(ones, jnp.where(upto, 1.0, 0.0).astype(low), preferred_element_type=f32)
    slot = jnp.where(member, rank[0:1, :] - 1.0, -1.0)
    slot_ids = lax.broadcasted_iota(jnp.int32, (capacity, props), 0).astype(f32)
    picks = jnp.where(slot == slot_ids, 1.0, 0.0).astype(low)

    def pick(ints):
        return lax.dot_general(
            ints.astype(f32).astype(low), picks, NT, preferred_element_type=f32
        )

    boxes = jnp.concatenate([fields_ref[...], fields_ref[...]], axis=0)
    values = 8.0 * pick(boxes >> 3) + pick(boxes & 7)
    level = pick(jnp.broadcast_to(levels_ref[...], (8, props)))[0:1, :]
    top, left, height, box_width = (values[i : i + 1, :] for i in range(4))
    is_fine = level < 0.5
    inverse = jnp.where(is_fine, 0.25, 0.125)
    span = jnp.where(is_fine, 28.0, 56.0)
    first_row = jnp.floor(top * inverse)
    band_rows = jnp.where(is_fine, 1.0 * fine_rows, 1.0 * coarse_rows)
    local_row = jnp.clip(first_row - y.astype(f32) * band_rows, 0.0, band_rows - 1.0)
    first_col = jnp.minimum(
        jnp.floor(left * inverse), jnp.where(is_fine, 1.0 * fine_cols, 1.0 * coarse_cols) - WIN
    )
    cells_v[0:1, :] = (local_row + jnp.where(is_fine, 0.0, 1.0 * (fine_rows + HALO))).astype(
        jnp.int32
    )
    cells_v[1:2, :] = first_col.astype(jnp.int32)
    geo_v[0:1, :] = top * inverse - first_row
    geo_v[1:2, :] = height / span
    geo_v[2:3, :] = left * inverse - first_col
    geo_v[3:4, :] = box_width / span
    up_copy.wait()
    half = rows(core * capacity, capacity)
    upb[half, :] = jnp.dot(picks, up_all[...], preferred_element_type=f32).astype(low)
    cells_copy = local(cells_v, cells_ref, 5)
    geo_copy = local(geo_v, geo_ref, 6)

    coarse_base = fine_rows + HALO

    def widen(source, first, count, base, cols):
        def one(r, carry):
            wide[base + r, 0:cols, :] = source[r].astype(f32)
            return carry

        lax.fori_loop(first, first + count, one, 0)

    fine_copy.wait()
    coarse_copy.wait()
    widen(fine_low, 0, fine_rows, 0, fine_cols)
    widen(coarse_low, 0, coarse_rows, coarse_base, coarse_cols)
    up_swap = remote(upb.at[half, :], upb.at[half, :], 3, partner)
    up_swap.start()

    for event in todo[:EARLY]:
        gather(event)
    up_swap.wait()

    def turn_up(i, carry):
        at = rows(i * 128, 128)
        uptb[at, :] = upb[:, at].astype(f32).T.astype(low)
        return carry

    lax.fori_loop(0, hidden_size // 128, turn_up, 0)

    @pl.when(y == 0)
    def _():
        fine_halo.wait_recv()
        coarse_halo.wait_recv()
        widen(fine_low, fine_rows, HALO, 0, fine_cols)
        widen(coarse_low, coarse_rows, HALO, coarse_base, coarse_cols)

    @pl.when(y == 1)
    def _():
        def clear(r, carry):
            wide[r] = jnp.zeros(wide.shape[1:], f32)
            return carry

        lax.fori_loop(fine_rows, fine_rows + HALO, clear, 0)
        lax.fori_loop(coarse_base + coarse_rows, coarse_base + coarse_rows + HALO, clear, 0)

    cells_copy.wait()
    geo_copy.wait()

    groups = capacity // GROUP
    during = todo[EARLY : EARLY + DURING]
    shape = (ROWS_PAD, REACH * WIN)
    k = lax.broadcasted_iota(jnp.int32, shape, 0).astype(f32)
    i_bin = jnp.floor((k + 0.5) * (1.0 / BINS))
    j_bin = k - BINS * i_bin
    i_mid = i_bin + 0.5
    j_mid = j_bin + 0.5
    lane = lax.broadcasted_iota(jnp.int32, shape, 1)
    r_cell = (lane >> 4).astype(f32)
    q_cell = (lane & 15).astype(f32)

    def crop_copy(first, count):
        crop_rows = pl.ds(pl.multiple_of(core * capacity + first, GROUP), count)
        return remote(crops.at[crop_rows, :], crops.at[crop_rows, :], 4, partner)

    def crop_group(g, carry):
        for n, event in enumerate(during):
            at = CROP_AT[n] if sizes in GATHER_CODES else n * groups // len(during)
            pl.when(g == min(at, groups - 1))(functools.partial(gather, event))
        for p in range(GROUP):
            n = g * GROUP + p
            row = jnp.clip(cells_ref[0, n], 0, wide.shape[0] - REACH)
            col = jnp.clip(cells_ref[1, n], 0, fine_cols - WIN)
            row_w = jnp.maximum(0.0, 1.0 - jnp.abs(i_mid * geo_ref[1, n] + geo_ref[0, n] - r_cell))
            col_w = jnp.maximum(0.0, 1.0 - jnp.abs(j_mid * geo_ref[3, n] + geo_ref[2, n] - q_cell))
            weights = (row_w * col_w).astype(low)
            window = jnp.concatenate(
                [wide[row + r, pl.ds(col, WIN), :] for r in range(REACH)], axis=0
            ).astype(low)
            crop = jnp.dot(weights, window, preferred_element_type=f32)
            stage[pl.ds(p, ROWS_PAD, stride=GROUP), :] = crop
        group_rows = rows(core * capacity + g * GROUP, GROUP)
        for m in range(feats // 128):
            crops[group_rows, m * 128 : (m + 1) * 128] = stage[
                m * GROUP : (m + 1) * GROUP, :
            ].astype(low)

        @pl.when(g > 0)
        def _():
            crop_copy((g - 1) * GROUP, GROUP).start()

        return carry

    lax.fori_loop(0, groups, crop_group, 0)
    crop_copy((groups - 1) * GROUP, GROUP).start()

    def hide(ahead, route, begun):
        t = y if ahead == 0 else 1 - y
        first, count = parts_in[route]
        from_at = (starts[0] + t * (starts[1] - starts[0]) + first) * 128
        part = lax.dot_general(
            wbuf[rows(t * all_rows, all_rows), first * 128 : (first + count) * 128],
            crops[:, pl.ds(pl.multiple_of(from_at, 128), count * 128)],
            NT,
            preferred_element_type=f32,
        )
        hidden[...] = hidden[...] + part if begun else part

    def make_back(ahead):
        t = y if ahead == 0 else 1 - y
        part = jnp.dot(
            upb[...], w2buf[rows(t * hidden_size, hidden_size), :], preferred_element_type=f32
        )
        back[rows(t * depth, depth), :] = part.T

    ends = {
        (rel[2], route if route < last_in else -1): i for i, (route, rel) in enumerate(events)
    }
    ready = [(i, key) for key, i in ends.items()]
    passed = len(own) + EARLY + DURING
    waited, begun = False, False
    for i in range(passed - 1, len(events)):
        if i >= passed:
            gather(events[i])
        for key in [k for end, k in sorted(ready) if end == i or (i == passed - 1 and end < i)]:
            if key[1] < 0:
                make_back(key[0])
                continue
            if not waited:
                waited = True
                crop_copy(0, capacity).wait()
            hide(*key, begun)
            begun = True
    def gelu(i, carry):
        at = rows(i * 32, 32)
        value, slope = gelu_parts(hidden[at, :])
        acts[at, :] = value.astype(low)
        pres[at, :] = (back[at, :] * slope).astype(low)
        return carry

    lax.fori_loop(0, hidden.shape[0] // 32, gelu, 0)

    def sum_ref(route):
        if route >= last_out:
            return lambda q: seconds.at[
                rows(q[2] * hidden_size + (q[0] * nx + q[1]) * pair, pair),
                pl.ds((route - last_out) * cols_out, cols_out),
            ]
        first, count = parts_out[route]
        return lambda q: grads.at[
            rows(q[2] * all_rows + (q[0] * nx + q[1]) * h, h), pl.ds(first * 128, count * 128)
        ]

    def add(ref, more):
        def one(i, carry):
            at = rows(i * 16, 16)
            ref[at, :] = (ref[at, :].astype(f32) + more[at, :].astype(f32)).astype(low)
            return carry

        lax.fori_loop(0, ref.shape[0] // 16, one, 0)

    def make_grads(t, part):
        first, count = parts_out[part]
        step = max(c for c in range(1, 7) if count % c == 0)

        def one(i, carry):
            at = pl.multiple_of((first + i * step) * 128, 128)
            from_at = pl.multiple_of((starts[0] + t * (starts[1] - starts[0])) * 128 + at, 128)
            grads[rows(t * all_rows, all_rows), pl.ds(at, step * 128)] = jnp.dot(
                pres[...], crops[:, pl.ds(from_at, step * 128)], preferred_element_type=f32
            ).astype(low)
            return carry

        lax.fori_loop(0, count // step, one, 0)

    def make_seconds():
        for t in range(ny):
            seconds[t * hidden_size : (t + 1) * hidden_size, :] = lax.dot_general(
                uptb[...], acts[t * depth : (t + 1) * depth, :], NT, preferred_element_type=f32
            ).astype(low)

    own_second = y * hidden_size + chip * pair
    made, ended, outs, swapped = set(), set(), [], False
    for route, rel in sum_events:
        need = (route, rel[2]) if route < last_out else last_out
        if need not in made:
            made.add(need)
            if route >= last_out:
                make_seconds()
            else:
                make_grads(y if rel[2] == 0 else 1 - y, route)
        ways_out.scatter(
            route, rel, sum_ref(route), slot_refs[route], add, sum_send_sems, sum_recv_sems
        )
        if rel != (0, 0, 0):
            continue
        ended.add(route)
        if route < last_out:
            first, count = parts_out[route]
            at = pl.ds(first * 128, count * 128)
            outs.append(local(grads.at[own_rows, at], first_ref.at[:, at], len(outs)))
        if not swapped and all(r in ended for r in range(last_out, len(SCATTER_ORDERS))):
            swapped = True
            swap[0] = seconds[pl.ds(pl.multiple_of(own_second + other * h, h), h), :]
            second_swap = remote(swap.at[0], swap.at[1], 5, partner)
            second_swap.start()
            mine = seconds.at[pl.ds(pl.multiple_of(own_second + core * h, h), h), :]
            outs.append(local(mine, second_ref.at[core], len(outs)))

    def whole(route, buf, other_buf, parts, last, cols):
        if route >= last:
            return lambda n: other_buf.at[pl.ds(0, n), pl.ds((route - last) * cols, cols)]
        first, count = parts[route]
        return lambda n: buf.at[pl.ds(0, n), pl.ds(first * 128, count * 128)]

    for route in range(len(GATHER_ORDERS)):
        unit = pair if route >= last_in else h
        part = whole(route, wbuf, w2buf, parts_in, last_in, cols_in)
        ways_in.drain(route, part, unit, send_sems)
    for route in range(len(SCATTER_ORDERS)):
        unit = pair if route >= last_out else h
        part = whole(route, grads, seconds, parts_out, last_out, cols_out)
        sent = part((nz * nx * ny - 1) * unit)
        pltpu.make_async_copy(sent, sent, sum_send_sems.at[route]).wait()

    @pl.when(y == 1)
    def _():
        fine_halo.wait_send()
        coarse_halo.wait_send()

    second_swap.wait()
    outs.append(local(swap.at[1], second_ref.at[other], len(outs)))
    for copy in outs:
        copy.wait()


def finish_kernel(shift, sums_ref, sets_ref, first_ref, second_ref):
    y = lax.axis_index("tile")
    h, share = first_ref.shape
    depth = sets_ref.shape[2]
    bins = sums_ref.shape[1] // 128
    f32 = jnp.float32
    halves = lax.broadcasted_iota(jnp.int32, (h, 128), 1)
    back_shift = (128 - shift) % 128

    def turned(i):
        tile = sums_ref[:, 128 * i : 128 * (i + 1)].astype(f32)
        return tile, pltpu.roll(tile, back_shift, axis=1)

    now = turned(0)
    for i in range(bins):
        width = min(128, share - 128 * i)
        following = turned(i + 1) if i + 1 < bins else now
        late = jnp.where(halves < 128 - shift, now[1], following[1])
        first_ref[:, 128 * i : 128 * i + width] = jnp.where(y == 0, now[0], late)[:, :width]
        now = following
    for m in range(depth // 128):
        at = slice(128 * m, 128 * (m + 1))
        set_0 = sets_ref[0, :, at].astype(f32)
        set_1 = sets_ref[1, :, at].astype(f32)
        second_ref[:, 256 * m : 256 * m + 128] = jnp.where(
            halves < h, set_0, pltpu.roll(set_1, h, axis=1)
        )
        second_ref[:, 256 * m + 128 : 256 * m + 256] = jnp.where(
            halves < h, pltpu.roll(set_0, h, axis=1), set_1
        )


def per_device_by_chips(
    grid, proposal_boxes, level_plan, fine_map, coarse_map, first_weight, second_weight, upstream
):
    nz, nx, ny, cores = grid
    chips = nz * nx
    props = level_plan.shape[1]
    capacity = props // ny
    fine_tile, coarse = fine_map[0], coarse_map[0]
    fine_rows, fine_cols, channels = fine_tile.shape
    coarse_rows = coarse.shape[0]
    share, h = first_weight.shape
    feats = share * ny
    bins = max(-(-((t + 1) * share) // 128) - t * share // 128 for t in range(ny))
    lanes = bins * 128
    hidden_size = upstream.shape[2]
    depth = second_weight.shape[0] // cores
    pair = cores * h
    low, f32 = jnp.bfloat16, jnp.float32
    sizes = (nz, nx, ny)
    parts_out = cut(bins, SCATTER_SHARES)
    slot_counts = [sum(slots_of(sizes, order)) for order in SCATTER_ORDERS]
    rows_all = chips * h
    batch = cores * capacity
    q = chips * ny
    dma = pltpu.SemaphoreType.DMA
    anywhere = pl.BlockSpec(memory_space=pl.ANY)
    vmem = pl.BlockSpec(memory_space=pltpu.VMEM)
    slot_shapes = [
        (n, h, parts_out[i][1] * 128)
        if i < len(parts_out)
        else (n, pair, depth // (len(SCATTER_ORDERS) - len(parts_out)))
        for i, n in enumerate(slot_counts)
    ]
    sums, sets = pl.pallas_call(
        functools.partial(step_kernel, grid),
        out_shape=(
            jax.ShapeDtypeStruct((h, lanes), low),
            jax.ShapeDtypeStruct((cores, h, depth), low),
        ),
        in_specs=[vmem, vmem] + [anywhere] * 5,
        out_specs=(anywhere, anywhere),
        scratch_shapes=[
            pltpu.VMEM((h, share), low),
            pltpu.VMEM((h, cores * depth), low),
            pltpu.VMEM((cores, h, depth), low),
            pltpu.VMEM((ny * rows_all, lanes), low),
            pltpu.VMEM((ny * hidden_size, depth), low),
            pltpu.VMEM((fine_rows + HALO, fine_cols, channels), low),
            pltpu.VMEM((coarse_rows + HALO, coarse.shape[1], channels), low),
            pltpu.VMEM((fine_rows + coarse_rows + 2 * HALO, fine_cols, channels), f32),
            pltpu.VMEM((ROWS_PAD * GROUP, 128), f32),
            pltpu.VMEM((batch, feats), low),
            pltpu.VMEM((props, hidden_size), low),
            pltpu.VMEM((batch, hidden_size), low),
            pltpu.VMEM((hidden_size, batch), low),
            pltpu.VMEM((rows_all, batch), f32),
            pltpu.VMEM((rows_all, batch), f32),
            pltpu.VMEM((rows_all, batch), low),
            pltpu.VMEM((rows_all, batch), low),
            pltpu.VMEM((ny * rows_all, lanes), low),
            pltpu.VMEM((ny * hidden_size, depth), low),
            pltpu.VMEM((2, h, depth), low),
            pltpu.VMEM((8, capacity), jnp.int32),
            pltpu.VMEM((8, capacity), f32),
            pltpu.SMEM((8, capacity), jnp.int32),
            pltpu.SMEM((8, capacity), f32),
            dma((max(7, len(SCATTER_ORDERS) + 2),)),
            dma((len(GATHER_ORDERS), 4)),
            dma((len(GATHER_ORDERS), q)),
            dma((len(SCATTER_ORDERS),)),
            dma((sum(slot_counts),)),
            dma((6,)),
            dma((6,)),
        ]
        + [pltpu.VMEM(shape, low) for shape in slot_shapes],
        compiler_params=pltpu.CompilerParams(
            collective_id=0, has_side_effects=True, vmem_limit_bytes=64000 * 1024
        ),
        name="step",
    )(
        proposal_boxes[0],
        level_plan,
        first_weight.T,
        second_weight.T,
        upstream[0],
        fine_tile,
        coarse,
    )
    shift = share - 128 * min(share // 128, feats // 128 - bins)
    first, second = pl.pallas_call(
        functools.partial(finish_kernel, shift),
        out_shape=(
            jax.ShapeDtypeStruct((h, share), f32),
            jax.ShapeDtypeStruct((h, cores * depth), f32),
        ),
        in_specs=[vmem, vmem],
        out_specs=(vmem, vmem),
        name="finish",
    )(sums, sets)
    return (first.T, second.T)


def solution(mesh):
    placed = (
        P("dp", None, None),
        P("dp", None),
        P("dp", "tile", None, None),
        P("dp", "tile", None, None),
        P("tile", "dp"),
        P("tile", "dp"),
        P("dp", None, None),
    )
    grid = chip_grid(mesh)
    tiles = mesh.shape["tile"]
    body = per_device_by_bands
    if grid is not None and tiles == 2 and grid[1] <= 2 and grid[2] == 2:
        body = functools.partial(per_device_by_chips, (grid[0], grid[1], tiles, grid[2]))
    return jax.shard_map(
        body,
        mesh=mesh,
        in_specs=placed,
        out_specs=(P("tile", "dp"), P("tile", "dp")),
        check_vma=False,
    )
```

```python
import functools

import jax
import jax.numpy as jnp
from jax import lax
from jax.experimental import pallas as pl
from jax.experimental.pallas import tpu as pltpu
from jax.sharding import PartitionSpec as P

WIN = 16
BINS = 7
ROWS_PAD = 56
GROUP = 16


def from_ahead(block, axis, distance):
    if distance == 0:
        return block
    size = lax.axis_size(axis)
    return lax.ppermute(block, axis, [(i, (i - distance) % size) for i in range(size)])


def halo_from_next(block, axis):
    size = lax.axis_size(axis)
    return lax.ppermute(block, axis, [(i + 1, i) for i in range(size - 1)])


def gelu_parts(hidden):
    factor = 0.7978845608028654
    cubic_term = 0.044715
    inner_term = factor * (hidden + cubic_term * hidden * hidden * hidden)
    tangent = jnp.tanh(inner_term)
    gelu_value = 0.5 * hidden * (1.0 + tangent)
    gelu_slope = 0.5 * (1.0 + tangent) + 0.5 * hidden * (1.0 - tangent * tangent) * factor * (
        1.0 + 3.0 * cubic_term * hidden * hidden
    )
    return (gelu_value, gelu_slope)


def crop_kernel(starts, width, cells_ref, geo_ref, maps_ref, out_ref, wide, stage):
    step = pl.program_id(0)

    @pl.when(step == 0)
    def _():
        def widen(r, carry):
            wide[r] = maps_ref[r].astype(jnp.float32)
            return carry

        lax.fori_loop(0, maps_ref.shape[0], widen, 0)

    shape = (ROWS_PAD, WIN * WIN)
    k = lax.broadcasted_iota(jnp.int32, shape, 0).astype(jnp.float32)
    i_bin = jnp.floor((k + 0.5) * (1.0 / BINS))
    j_bin = k - BINS * i_bin
    i_mid = i_bin + 0.5
    j_mid = j_bin + 0.5
    lane = lax.broadcasted_iota(jnp.int32, shape, 1)
    r_cell = (lane >> 4).astype(jnp.float32)
    q_cell = (lane & 15).astype(jnp.float32)
    for p in range(GROUP):
        n = step * GROUP + p
        row = cells_ref[0, n]
        col = cells_ref[1, n]
        row_w = jnp.maximum(0.0, 1.0 - jnp.abs(i_mid * geo_ref[1, n] + geo_ref[0, n] - r_cell))
        col_w = jnp.maximum(0.0, 1.0 - jnp.abs(j_mid * geo_ref[3, n] + geo_ref[2, n] - q_cell))
        weights = (row_w * col_w).astype(jnp.bfloat16)
        window = jnp.concatenate(
            [wide[row + r, pl.ds(col, WIN), :] for r in range(WIN)], axis=0
        ).astype(jnp.bfloat16)
        crop = jnp.dot(weights, window, preferred_element_type=jnp.float32)
        stage[pl.ds(p, ROWS_PAD, stride=GROUP), :] = crop
    for t, first in enumerate(starts):
        for m in range(width):
            at = (first + m) * GROUP
            out_ref[t, :, m * 128 : (m + 1) * 128] = stage[at : at + GROUP, :].astype(jnp.bfloat16)


def make_crops(cells, geo, maps, starts, width, capacity):
    tiles = len(starts)
    lanes = width * 128
    return pl.pallas_call(
        functools.partial(crop_kernel, starts, width),
        grid=(capacity // GROUP,),
        out_shape=jax.ShapeDtypeStruct((tiles, capacity, lanes), jnp.bfloat16),
        in_specs=[
            pl.BlockSpec(memory_space=pltpu.SMEM),
            pl.BlockSpec(memory_space=pltpu.SMEM),
            pl.BlockSpec(maps.shape, lambda g: (0, 0, 0)),
        ],
        out_specs=pl.BlockSpec((tiles, GROUP, lanes), lambda g: (0, g, 0)),
        scratch_shapes=[
            pltpu.VMEM(maps.shape, jnp.float32),
            pltpu.VMEM((ROWS_PAD * GROUP, 128), jnp.float32),
        ],
        compiler_params=pltpu.CompilerParams(
            dimension_semantics=("arbitrary",), vmem_limit_bytes=48 * 1024 * 1024
        ),
        cost_estimate=pl.CostEstimate(
            flops=capacity * ROWS_PAD * WIN * WIN * 128 * 16,
            bytes_accessed=2 * maps.size + 2 * tiles * capacity * lanes,
            transcendentals=0,
        ),
        name="crops",
    )(cells, geo, maps)


def per_device_by_bands(
    proposal_boxes, level_plan, fine_map, coarse_map, first_weight, second_weight, upstream
):
    tile_count = lax.axis_size("tile")
    band = lax.axis_index("tile")
    num_props = level_plan.shape[1]
    capacity = max(num_props // 4, num_props // tile_count)
    fine_tile = fine_map[0]
    coarse = coarse_map[0]
    fine_rows, fine_cols, channels = fine_tile.shape
    coarse_rows, coarse_cols = (coarse.shape[0], coarse.shape[1])

    top_rows = jnp.concatenate([fine_tile[:WIN], coarse[:WIN]], axis=1)
    below_rows = halo_from_next(top_rows, "tile")

    share_feats = first_weight.shape[0]
    feats = share_feats * tile_count
    width = max(
        -(-((t + 1) * share_feats) // 128) - t * share_feats // 128 for t in range(tile_count)
    )
    starts = [min(t * share_feats // 128, feats // 128 - width) for t in range(tile_count)]
    lanes = width * 128
    feat_off = band * share_feats - 128 * jnp.minimum(
        band * share_feats // 128, feats // 128 - width
    )

    first_rows = lax.dynamic_update_slice(
        jnp.zeros((first_weight.shape[1], lanes), jnp.bfloat16),
        first_weight.T,
        (0, feat_off),
    )
    both = lax.all_gather(
        jnp.concatenate([first_rows, second_weight.T], axis=1), "dp", axis=0, tiled=True
    )
    first_all = both[:, :lanes]
    second_all = both[:, lanes:]

    fields = proposal_boxes[0]
    levels = level_plan[0]
    owner = fields[0] // (4 * fine_rows)
    members = (owner[:, None] == jnp.arange(tile_count, dtype=jnp.int32)[None, :]).astype(jnp.int32)
    rank = jnp.sum((jnp.cumsum(members, axis=0) - 1) * members, axis=1)
    relative = lax.rem(owner - band + tile_count, tile_count)
    slot_id = relative * capacity + rank
    slots = tile_count * capacity
    chosen = slot_id[None, :] == jnp.arange(slots, dtype=jnp.int32)[:, None]
    upstream_slots = jnp.dot(
        chosen.astype(jnp.bfloat16), upstream[0], preferred_element_type=jnp.float32
    ).astype(jnp.bfloat16)
    mine = chosen[:capacity].astype(jnp.int32)
    top, left, height, box_width = (
        jnp.sum(mine * fields[f][None, :], axis=1) for f in range(4)
    )
    level = jnp.sum(mine * levels[None, :], axis=1)

    stride = jnp.where(level == 0, 4, 8).astype(jnp.int32)
    is_fine = level == 0
    first_row = top // stride
    local_row = jnp.clip(
        first_row - band * jnp.where(is_fine, fine_rows, coarse_rows),
        0,
        jnp.where(is_fine, fine_rows, coarse_rows) - 1,
    )
    first_col = jnp.minimum(left // stride, jnp.where(is_fine, fine_cols, coarse_cols) - WIN)
    cells = jnp.stack(
        [local_row + jnp.where(is_fine, 0, fine_rows + WIN), first_col], axis=0
    ).astype(jnp.int32)
    stride_float = stride.astype(jnp.float32)
    geo = jnp.stack(
        [
            top.astype(jnp.float32) / stride_float - first_row.astype(jnp.float32),
            height.astype(jnp.float32) / (7.0 * stride_float),
            left.astype(jnp.float32) / stride_float - first_col.astype(jnp.float32),
            box_width.astype(jnp.float32) / (7.0 * stride_float),
        ],
        axis=0,
    )

    side = ((0, 0), (0, fine_cols - coarse_cols), (0, 0))
    maps = jnp.concatenate(
        [
            fine_tile,
            below_rows[:, :fine_cols],
            jnp.pad(coarse, side),
            jnp.pad(below_rows[:, fine_cols:], side),
        ],
        axis=0,
    )
    crop_blocks = make_crops(cells, geo, maps, starts, width, capacity)
    own_feats = jnp.concatenate(
        [
            from_ahead(
                lax.dynamic_index_in_dim(
                    crop_blocks, lax.rem(band - d + tile_count, tile_count), 0, keepdims=False
                ),
                "tile",
                d,
            )
            for d in range(tile_count)
        ],
        axis=0,
    )

    partial_hidden = lax.dot_general(
        own_feats, first_all, (((1,), (1,)), ((), ())), preferred_element_type=jnp.float32
    ).astype(jnp.bfloat16)
    share = second_weight.shape[0]

    def in_my_order(block, d):
        return jnp.roll(block, d * capacity, axis=0) if d else block

    hidden_own = 0.0
    for d in range(tile_count):
        to = lax.rem(band - d + tile_count, tile_count)
        piece = lax.dynamic_slice_in_dim(partial_hidden, to * share, share, axis=1)
        hidden_own = hidden_own + in_my_order(from_ahead(piece, "tile", d), d).astype(jnp.float32)
    gelu_value, gelu_slope = gelu_parts(hidden_own)
    activated = gelu_value.astype(jnp.bfloat16)
    back_grad = jnp.dot(upstream_slots, second_all, preferred_element_type=jnp.float32)
    pre_own = (back_grad * gelu_slope).astype(jnp.bfloat16)
    ahead = [in_my_order(from_ahead(pre_own, "tile", d), d) for d in range(tile_count)]
    twice = jnp.concatenate(ahead + ahead[:-1], axis=1)
    pre_grad = lax.dynamic_slice_in_dim(
        twice, lax.rem(tile_count - band, tile_count) * share, tile_count * share, axis=1
    )
    over_rows = (((0,), (0,)), ((), ()))
    second_part = lax.dot_general(
        upstream_slots, activated, over_rows, preferred_element_type=jnp.float32
    ).astype(jnp.bfloat16)
    first_part = lax.dot_general(
        pre_grad, own_feats, over_rows, preferred_element_type=jnp.float32
    ).astype(jnp.bfloat16)
    summed = lax.psum_scatter(
        jnp.concatenate([first_part, second_part], axis=1), "dp", scatter_dimension=0, tiled=True
    ).astype(jnp.float32)
    first_grad = lax.dynamic_slice_in_dim(summed[:, :lanes], feat_off, share_feats, axis=1).T
    second_grad = summed[:, lanes:].T
    return (first_grad, second_grad)


MESH = pl.DeviceIdType.MESH
REACH = 15
HALO = REACH - 1
NT = (((1,), (1,)), ((), ()))
NN = (((1,), (0,)), ((), ()))


def chip_grid(mesh):
    chips = [getattr(device, "coords", None) for device in mesh.devices[:, 0]]
    if chips[0] is None:
        return None
    cores = sum(1 for c in chips if tuple(c) == tuple(chips[0]))
    chips = [tuple(c) for c in chips[::cores]]
    if len(chips) == 1:
        return (1, 1, cores)
    axis = [a != b for a, b in zip(chips[0], chips[1])].index(True)
    fast = 1
    while fast < len(chips) and all(
        a == b or i == axis for i, (a, b) in enumerate(zip(chips[0], chips[fast]))
    ):
        fast += 1
    return (len(chips) // fast, fast, cores)


def offsets(size):
    if size == 1:
        return [0]
    if size == 2:
        return [0, 1]
    return [0] + [s * d for d in range(1, size) for s in (-1, 1)]


def steps_of(size):
    return {1: [], 2: [1]}.get(size, [-1, 1])


def moved(position, size, rel):
    if rel == 0 or size == 1:
        return position
    return 1 - position if size == 2 else position + rel


def last_axis(order, rel):
    used = [j for j in range(3) if rel[order[j]]]
    return used[-1] if used else -1


def onward(sizes, order, rel):
    last = last_axis(order, rel)
    hops = []
    if last >= 0:
        axis = order[last]
        if sizes[axis] > 2 and abs(rel[axis]) < sizes[axis] - 1:
            hops.append((last, axis, -1 if rel[axis] > 0 else 1))
    for j in range(last + 1, 3):
        hops.extend((j, order[j], step) for step in steps_of(sizes[order[j]]))
    return hops


def arrival_order(sizes, routes, extra):
    import heapq
    import itertools

    places = list(itertools.product(*(range(n) for n in sizes)))
    queue, waiting, busy = [], {}, set()
    seen, tick = {}, itertools.count()

    def start(link, now):
        if link not in busy and waiting.get(link):
            busy.add(link)
            load, arrival = waiting[link].pop(0)
            heapq.heappush(queue, (now + load, next(tick), link, arrival))

    def arrive(place, route, rel, now):
        seen.setdefault((route, rel), []).append(now)
        for _, axis, step in onward(sizes, routes[route][0], rel):
            target = list(place)
            target[axis] = moved(place[axis], sizes[axis], step)
            if not 0 <= target[axis] < sizes[axis]:
                continue
            there = list(rel)
            there[axis] = rel[axis] - step if sizes[axis] > 2 else 1
            link = (place, axis, step)
            waiting.setdefault(link, []).append(
                (routes[route][1], (tuple(target), route, tuple(there)))
            )
            start(link, now)

    first = {}
    for place in places:
        for route in extra[1]:
            arrive(place, route, (0, 0, 0), 0.0)
        if extra[0] and place[2] == 1:
            waiting.setdefault((place, 2, 1), []).append((extra[0], None))
            start((place, 2, 1), 0.0)
        for route in range(len(routes)):
            if route not in extra[1]:
                arrive(place, route, (0, 0, 0), 0.0)
    end = 0.0
    while queue:
        now, _, link, arrival = heapq.heappop(queue)
        end = now
        busy.discard(link)
        if arrival is not None:
            arrive(*arrival, now)
        start(link, now)
    key = {event: sum(t) / len(t) for event, t in seen.items()}
    for _ in range(sum(sizes)):
        for (route, rel) in list(key):
            for _, axis, step in onward(sizes, routes[route][0], rel):
                there = list(rel)
                there[axis] = rel[axis] - step if sizes[axis] > 2 else 1
                event = (route, tuple(there))
                if event in key:
                    key[event] = max(key[event], key[(route, rel)] + 1e-3)
    return sorted(key, key=lambda e: (key[e], e)), key, end


def slots_of(sizes, order):
    counts, before = [], 1
    for j in range(3):
        n = sizes[order[j]]
        counts.append(before * (n + 1 if n > 2 else 1))
        before *= n
    return counts


def when(conds, body):
    if not conds:
        body()
        return
    total = conds[0]
    for cond in conds[1:]:
        total = jnp.logical_and(total, cond)
    pl.when(total)(body)


class Routes:
    def __init__(self, sizes, position, core, cores, orders):
        self.sizes, self.position = sizes, position
        self.core, self.cores = core, cores
        self.orders = orders
        self.slot_counts = [slots_of(sizes, order) for order in orders]
        self.slot_base = [sum(sum(c) for c in self.slot_counts[:i]) for i in range(len(orders))]

    def inside(self, axis, rel):
        if rel == 0 or self.sizes[axis] <= 2:
            return []
        p = self.position[axis]
        return [p < self.sizes[axis] - rel] if rel > 0 else [p >= -rel]

    def valid(self, rel):
        return sum((self.inside(axis, rel[axis]) for axis in range(3)), [])

    def at(self, rel):
        return [moved(self.position[a], self.sizes[a], rel[a]) for a in range(3)]

    def device(self, axis, step):
        there = list(self.position)
        there[axis] = moved(there[axis], self.sizes[axis], step)
        return ((there[0] * self.sizes[1] + there[1]) * self.cores + self.core, there[2])

    def back_step(self, order, rel):
        axis = order[last_axis(order, rel)]
        return axis, (1 if self.sizes[axis] == 2 or rel[axis] > 0 else -1)

    def number(self, place):
        return (place[0] * self.sizes[1] + place[1]) * self.sizes[2] + place[2]

    def direction(self, axis, step):
        return axis + 1 if axis else (1 if step > 0 else 0)

    def drain(self, route, whole, unit, sems):
        order, before = self.orders[route], 1
        for axis in order:
            n, p = self.sizes[axis], self.position[axis]
            for step in steps_of(n):
                for at in range(n) if n > 2 else [0]:
                    sent = before * ((at + 1 if step > 0 else n - at) if n > 2 else 1)
                    if n > 2 and not 0 <= at + step < n:
                        continue

                    def wait(axis=axis, step=step, sent=sent):
                        part = whole(sent * unit)
                        pltpu.make_async_copy(
                            part, part, sems.at[route, self.direction(axis, step)]
                        ).wait()

                    when([p == at] if n > 2 else [], wait)
            before *= n

    def gather(self, route, rel, ref_of, send_sems, recv_sems):
        order = self.orders[route]

        def body():
            place = self.at(rel)
            ref = ref_of(place)
            q = self.number(place)

            def hop(axis, step):
                return pltpu.make_async_remote_copy(
                    src_ref=ref,
                    dst_ref=ref,
                    send_sem=send_sems.at[route, self.direction(axis, step)],
                    recv_sem=recv_sems.at[route, q],
                    device_id=self.device(axis, step),
                    device_id_type=MESH,
                )

            if last_axis(order, rel) >= 0:
                hop(*self.back_step(order, rel)).wait_recv()
            for _, axis, step in onward(self.sizes, order, rel):
                copy = hop(axis, step)
                when(self.inside(axis, step), copy.start)

        when(self.valid(rel), body)

    def slot(self, route, phase, side, place, here):
        order, counts = self.orders[route], self.slot_counts[route]
        index = 0
        for j in range(phase):
            index = index * self.sizes[order[j]] + place[order[j]]
        n = self.sizes[order[phase]]
        if n > 2:
            index = index * (n + 1) + (n if here and side > 0 else place[order[phase]])
        return sum(counts[:phase]) + index

    def scatter(self, route, rel, ref_of, slots, add, send_sems, recv_sems):
        order = self.orders[route]

        def body():
            place = self.at(rel)
            ref = ref_of(place)
            base = self.slot_base[route]
            for phase, axis, step in onward(self.sizes, order, rel):
                slot = self.slot(route, phase, step, place, rel[axis] == 0)

                def take(axis=axis, step=step, slot=slot):
                    pltpu.make_async_remote_copy(
                        src_ref=ref,
                        dst_ref=slots.at[slot],
                        send_sem=send_sems.at[route],
                        recv_sem=recv_sems.at[base + slot],
                        device_id=self.device(axis, step),
                        device_id_type=MESH,
                    ).wait_recv()
                    add(ref, slots.at[slot])

                when(self.inside(axis, step), take)
            phase = last_axis(order, rel)
            if phase >= 0:
                axis, step = self.back_step(order, rel)
                here = rel[axis] - step == 0
                slot = self.slot(route, phase, -step, place, here)
                pltpu.make_async_remote_copy(
                    src_ref=ref,
                    dst_ref=slots.at[slot],
                    send_sem=send_sems.at[route],
                    recv_sem=recv_sems.at[base + slot],
                    device_id=self.device(axis, step),
                    device_id_type=MESH,
                ).start()

        when(self.valid(rel), body)


def cut(bins, shares):
    edges = [0]
    for i in range(1, len(shares) + 1):
        edges.append(round(bins * sum(shares[:i]) / sum(shares)))
    return [(a, b - a) for a, b in zip(edges, edges[1:])]


GATHER_ORDERS = ((2, 0, 1), (0, 1, 2), (1, 2, 0), (2, 0, 1), (0, 1, 2))
GATHER_SHARES = (12, 9, 4)
SCATTER_ORDERS = ((2, 0, 1), (0, 1, 2), (0, 1, 2), (1, 2, 0), (2, 0, 1))
SCATTER_SHARES = (6, 8, 8, 3)
HALO_AFTER = 3
EARLY, DURING = 13, 56
CROP_AT = (
        2, 2, 2, 2, 3, 3, 3, 3, 3, 4, 5, 6, 6, 7, 7, 7, 7, 7, 7, 8, 8, 8, 8, 9, 9, 9, 10, 11,
        11, 11, 11, 11, 12, 12, 13, 13, 13, 13, 13, 13, 13, 13, 13, 13, 13, 13, 14, 15, 15, 15,
        15, 15, 15, 15, 15, 15
)
GATHER_CODES = {
    (4, 2, 2): (
        0, 84, 112, 28, 56, 116, 4, 8, 36, 16, 120, 44, 1, 124, 32, 12, 58, 40, 24, 85, 52, 9,
        5, 48, 20, 64, 57, 54, 46, 18, 136, 118, 62, 128, 13, 66, 17, 113, 3, 125, 38, 93, 26,
        121, 45, 42, 60, 55, 132, 30, 22, 87, 21, 88, 2, 96, 25, 50, 34, 59, 29, 92, 49, 138,
        89, 126, 70, 6, 14, 33, 134, 137, 97, 74, 61, 68, 11, 47, 108, 37, 105, 23, 78, 100, 7,
        65, 63, 101, 72, 130, 104, 117, 67, 86, 10, 19, 53, 82, 122, 27, 69, 80, 109, 114, 73,
        51, 15, 107, 95, 110, 76, 90, 75, 31, 98, 106, 41, 71, 39, 35, 43, 91, 127, 135, 94,
        129, 77, 133, 81, 131, 139, 102, 123, 119, 111, 103, 99, 83, 79, 115
    ),
}
SCATTER_CODES = {
    (4, 2, 2): (
        6, 138, 110, 39, 106, 123, 35, 109, 108, 83, 22, 14, 107, 105, 51, 139, 27, 23, 75, 98,
        111, 131, 102, 55, 19, 130, 7, 135, 11, 101, 26, 134, 47, 94, 43, 137, 15, 99, 71, 37,
        73, 18, 100, 82, 53, 25, 103, 79, 127, 63, 93, 90, 41, 20, 136, 104, 97, 54, 12, 74, 21,
        49, 81, 33, 77, 91, 17, 96, 133, 129, 132, 10, 118, 3, 46, 115, 122, 125, 50, 126, 67,
        13, 24, 16, 119, 65, 78, 9, 42, 4, 128, 92, 59, 52, 70, 80, 89, 45, 114, 34, 121, 62,
        31, 95, 69, 66, 8, 72, 44, 5, 61, 57, 38, 85, 2, 120, 124, 117, 88, 87, 76, 1, 48, 116,
        113, 58, 68, 40, 64, 60, 86, 30, 32, 29, 36, 0, 84, 56, 112, 28
    ),
}


def unpack(codes, sizes):
    spans = [offsets(n) for n in sizes]
    events = []
    for code in codes:
        code, k = divmod(code, len(spans[2]))
        code, j = divmod(code, len(spans[1]))
        route, i = divmod(code, len(spans[0]))
        events.append((route, (spans[0][i], spans[1][j], spans[2][k])))
    return events


def step_kernel(grid, *refs):
    fields_ref, levels_ref, w1_ref, w2_ref, up_ref, fine_ref, coarse_ref = refs[:7]
    first_ref, second_ref = refs[7:9]
    (
        w_in,
        w2_in,
        w2_sets,
        wbuf,
        w2buf,
        fine_low,
        coarse_low,
        wide,
        stage,
        crops,
        up_all,
        upb,
        uptb,
        back,
        hidden,
        acts,
        pres,
        grads,
        seconds,
        swap,
        cells_v,
        geo_v,
        cells_ref,
        geo_ref,
        local_sems,
        send_sems,
        recv_sems,
        sum_send_sems,
        sum_recv_sems,
        core_send,
        core_recv,
    ) = refs[9:40]
    slot_refs = refs[40:]
    nz, nx, ny, cores = grid
    sizes = (nz, nx, ny)
    dp = lax.axis_index("dp")
    y = lax.axis_index("tile")
    core = dp % cores
    chip = dp // cores
    x = chip % nx
    z = chip // nx
    position = (z, x, y)
    other = 1 - core
    partner = (chip * cores + other, y)
    ways_in = Routes(sizes, position, core, cores, GATHER_ORDERS)
    ways_out = Routes(sizes, position, core, cores, SCATTER_ORDERS)
    h, share = w1_ref.shape
    lanes = wbuf.shape[1]
    bins = lanes // 128
    all_rows = nz * nx * h
    fine_rows, fine_cols, _ = fine_ref.shape
    coarse_rows, coarse_cols, _ = coarse_ref.shape
    batch, feats = crops.shape
    capacity = batch // cores
    depth = w2buf.shape[1]
    hidden_size = up_ref.shape[1]
    pair = cores * h
    starts = [min(t * share // 128, feats // 128 - bins) for t in range(ny)]
    shift = share - 128 * starts[1]
    parts_in = cut(bins, GATHER_SHARES)
    parts_out = cut(bins, SCATTER_SHARES)
    f32, low = jnp.float32, jnp.bfloat16

    barrier = pltpu.get_barrier_semaphore()
    pl.semaphore_signal(barrier, inc=1, device_id=partner, device_id_type=MESH)
    peers = 1
    for axis in range(3):
        for step in steps_of(sizes[axis]):

            def greet(axis=axis, step=step):
                pl.semaphore_signal(
                    barrier, inc=1, device_id=ways_in.device(axis, step), device_id_type=MESH
                )

            near = ways_in.inside(axis, step)
            when(near, greet)
            peers = peers + (near[0].astype(jnp.int32) if near else 1)

    def rows(start, size):
        return pl.ds(pl.multiple_of(start, size), size)

    def local(src, dst, i):
        copy = pltpu.make_async_copy(src, dst, local_sems.at[i])
        copy.start()
        return copy

    def remote(src, dst, i, device):
        return pltpu.make_async_remote_copy(
            src_ref=src,
            dst_ref=dst,
            send_sem=core_send.at[i],
            recv_sem=core_recv.at[i],
            device_id=device,
            device_id_type=MESH,
        )

    w_copy = local(w1_ref, w_in, 0)
    w2_copy = local(w2_ref, w2_in, 1)
    fine_copy = local(fine_ref, fine_low.at[pl.ds(0, fine_rows)], 2)
    coarse_copy = local(coarse_ref, coarse_low.at[pl.ds(0, coarse_rows)], 3)
    up_copy = local(up_ref, up_all, 4)
    halves = lax.broadcasted_iota(jnp.int32, (h, 128), 1)

    w_copy.wait()
    own_rows = pl.ds(pl.multiple_of(y * all_rows + chip * h, h), h)

    def turned(i):
        width = min(128, share - 128 * i) if i >= 0 else 0
        if width <= 0:
            return jnp.zeros((h, 128), f32), jnp.zeros((h, 128), f32)
        now = w_in[:, 128 * i : 128 * i + width].astype(f32)
        if width < 128:
            now = jnp.concatenate([now, jnp.zeros((h, 128 - width), f32)], axis=1)
        return now, (pltpu.roll(now, shift, axis=1) if shift else now)

    def turn(first, count):
        before = turned(first - 1)[1]
        for i in range(first, first + count):
            now, after = turned(i)
            late = jnp.where(halves < shift, before, after)
            before = after
            wbuf[own_rows, 128 * i : 128 * (i + 1)] = jnp.where(y == 0, now, late).astype(low)


    last_in = len(GATHER_SHARES)
    last_out = len(SCATTER_SHARES)
    cols_in = depth // (len(GATHER_ORDERS) - last_in)
    cols_out = depth // (len(SCATTER_ORDERS) - last_out)
    loads_in = [
        (order, parts_in[i][1] if i < last_in else cols_in * pair // (h * 128))
        for i, order in enumerate(GATHER_ORDERS)
    ]
    loads_out = [
        (order, parts_out[i][1] if i < last_out else cols_out * pair // (h * 128))
        for i, order in enumerate(SCATTER_ORDERS)
    ]
    halo_load = HALO * (fine_cols + coarse_cols) // h
    if sizes in GATHER_CODES:
        events = unpack(GATHER_CODES[sizes], sizes)
        sum_events = unpack(SCATTER_CODES[sizes], sizes)
    else:
        events = arrival_order(sizes, loads_in, (halo_load, (0,)))[0]
        sum_events = arrival_order(sizes, loads_out, (0, ()))[0][::-1]

    def gather_ref(route):
        if route >= last_in:
            return lambda q: w2buf.at[
                rows(q[2] * hidden_size + (q[0] * nx + q[1]) * pair, pair),
                pl.ds((route - last_in) * cols_in, cols_in),
            ]
        first, count = parts_in[route]
        return lambda q: wbuf.at[
            rows(q[2] * all_rows + (q[0] * nx + q[1]) * h, h), pl.ds(first * 128, count * 128)
        ]

    def gather(event):
        route, rel = event
        ways_in.gather(route, rel, gather_ref(route), send_sems, recv_sems)

    below = ways_in.device(2, 1)
    fine_halo = remote(
        fine_ref.at[pl.ds(0, HALO)], fine_low.at[pl.ds(fine_rows, HALO)], 1, below
    )
    coarse_halo = remote(
        coarse_ref.at[pl.ds(0, HALO)], coarse_low.at[pl.ds(coarse_rows, HALO)], 2, below
    )
    own = [e for e in events if e[1] == (0, 0, 0)]
    todo = [e for e in events if e[1] != (0, 0, 0)]
    own.sort(key=lambda e: e[0] >= last_in)
    for n, event in enumerate(own[:last_in]):
        turn(*parts_in[event[0]])
        if n == 0:
            pl.semaphore_wait(barrier, peers)
        gather(event)
        if n + 1 == min(HALO_AFTER, last_in):

            @pl.when(y == 1)
            def _():
                fine_halo.start()
                coarse_halo.start()

    w2_copy.wait()
    for m in range(depth // 128):
        a = w2_in[:, 256 * m : 256 * m + 128].astype(f32)
        b = w2_in[:, 256 * m + 128 : 256 * m + 256].astype(f32)
        at = slice(128 * m, 128 * (m + 1))
        w2_sets[0, :, at] = jnp.where(halves < h, a, pltpu.roll(b, h, axis=1)).astype(low)
        w2_sets[1, :, at] = jnp.where(halves < h, pltpu.roll(a, h, axis=1), b).astype(low)
    w2_rows = pl.ds(pl.multiple_of(y * hidden_size + chip * pair + core * h, h), h)
    w2buf[w2_rows, :] = w2_sets[core]

    w2_swap = remote(w2_sets.at[other], w2buf.at[w2_rows, :], 0, partner)
    w2_swap.start()
    w2_swap.wait()
    for event in own[last_in:]:
        gather(event)

    events = own + todo

    member = jnp.logical_and(
        fields_ref[0:1, :] >= y * (4 * fine_rows), fields_ref[0:1, :] < (y + 1) * (4 * fine_rows)
    )
    props = fields_ref.shape[1]
    ones = jnp.broadcast_to(jnp.where(member, 1.0, 0.0), (8, props)).astype(low)
    upto = lax.broadcasted_iota(jnp.int32, (props, props), 0) <= lax.broadcasted_iota(
        jnp.int32, (props, props), 1
    )
    rank = jnp.dot(ones, jnp.where(upto, 1.0, 0.0).astype(low), preferred_element_type=f32)
    slot = jnp.where(member, rank[0:1, :] - 1.0, -1.0)
    slot_ids = lax.broadcasted_iota(jnp.int32, (capacity, props), 0).astype(f32)
    picks = jnp.where(slot == slot_ids, 1.0, 0.0).astype(low)

    def pick(ints):
        return lax.dot_general(
            ints.astype(f32).astype(low), picks, NT, preferred_element_type=f32
        )

    boxes = jnp.concatenate([fields_ref[...], fields_ref[...]], axis=0)
    values = 8.0 * pick(boxes >> 3) + pick(boxes & 7)
    level = pick(jnp.broadcast_to(levels_ref[...], (8, props)))[0:1, :]
    top, left, height, box_width = (values[i : i + 1, :] for i in range(4))
    is_fine = level < 0.5
    inverse = jnp.where(is_fine, 0.25, 0.125)
    span = jnp.where(is_fine, 28.0, 56.0)
    first_row = jnp.floor(top * inverse)
    band_rows = jnp.where(is_fine, 1.0 * fine_rows, 1.0 * coarse_rows)
    local_row = jnp.clip(first_row - y.astype(f32) * band_rows, 0.0, band_rows - 1.0)
    first_col = jnp.minimum(
        jnp.floor(left * inverse), jnp.where(is_fine, 1.0 * fine_cols, 1.0 * coarse_cols) - WIN
    )
    cells_v[0:1, :] = (local_row + jnp.where(is_fine, 0.0, 1.0 * (fine_rows + HALO))).astype(
        jnp.int32
    )
    cells_v[1:2, :] = first_col.astype(jnp.int32)
    geo_v[0:1, :] = top * inverse - first_row
    geo_v[1:2, :] = height / span
    geo_v[2:3, :] = left * inverse - first_col
    geo_v[3:4, :] = box_width / span
    up_copy.wait()
    half = rows(core * capacity, capacity)
    upb[half, :] = jnp.dot(picks, up_all[...], preferred_element_type=f32).astype(low)
    cells_copy = local(cells_v, cells_ref, 5)
    geo_copy = local(geo_v, geo_ref, 6)

    coarse_base = fine_rows + HALO

    def widen(source, first, count, base, cols):
        def one(r, carry):
            wide[base + r, 0:cols, :] = source[r].astype(f32)
            return carry

        lax.fori_loop(first, first + count, one, 0)

    fine_copy.wait()
    coarse_copy.wait()
    widen(fine_low, 0, fine_rows, 0, fine_cols)
    widen(coarse_low, 0, coarse_rows, coarse_base, coarse_cols)
    up_swap = remote(upb.at[half, :], upb.at[half, :], 3, partner)
    up_swap.start()

    for event in todo[:EARLY]:
        gather(event)
    up_swap.wait()

    def turn_up(i, carry):
        at = rows(i * 128, 128)
        uptb[at, :] = upb[:, at].astype(f32).T.astype(low)
        return carry

    lax.fori_loop(0, hidden_size // 128, turn_up, 0)

    @pl.when(y == 0)
    def _():
        fine_halo.wait_recv()
        coarse_halo.wait_recv()
        widen(fine_low, fine_rows, HALO, 0, fine_cols)
        widen(coarse_low, coarse_rows, HALO, coarse_base, coarse_cols)

    @pl.when(y == 1)
    def _():
        def clear(r, carry):
            wide[r] = jnp.zeros(wide.shape[1:], f32)
            return carry

        lax.fori_loop(fine_rows, fine_rows + HALO, clear, 0)
        lax.fori_loop(coarse_base + coarse_rows, coarse_base + coarse_rows + HALO, clear, 0)

    cells_copy.wait()
    geo_copy.wait()

    groups = capacity // GROUP
    during = todo[EARLY : EARLY + DURING]
    shape = (ROWS_PAD, REACH * WIN)
    k = lax.broadcasted_iota(jnp.int32, shape, 0).astype(f32)
    i_bin = jnp.floor((k + 0.5) * (1.0 / BINS))
    j_bin = k - BINS * i_bin
    i_mid = i_bin + 0.5
    j_mid = j_bin + 0.5
    lane = lax.broadcasted_iota(jnp.int32, shape, 1)
    r_cell = (lane >> 4).astype(f32)
    q_cell = (lane & 15).astype(f32)

    def crop_copy(first, count):
        crop_rows = pl.ds(pl.multiple_of(core * capacity + first, GROUP), count)
        return remote(crops.at[crop_rows, :], crops.at[crop_rows, :], 4, partner)

    def crop_group(g, carry):
        for n, event in enumerate(during):
            at = CROP_AT[n] if sizes in GATHER_CODES else n * groups // len(during)
            pl.when(g == min(at, groups - 1))(functools.partial(gather, event))
        for p in range(GROUP):
            n = g * GROUP + p
            row = jnp.clip(cells_ref[0, n], 0, wide.shape[0] - REACH)
            col = jnp.clip(cells_ref[1, n], 0, fine_cols - WIN)
            row_w = jnp.maximum(0.0, 1.0 - jnp.abs(i_mid * geo_ref[1, n] + geo_ref[0, n] - r_cell))
            col_w = jnp.maximum(0.0, 1.0 - jnp.abs(j_mid * geo_ref[3, n] + geo_ref[2, n] - q_cell))
            weights = (row_w * col_w).astype(low)
            window = jnp.concatenate(
                [wide[row + r, pl.ds(col, WIN), :] for r in range(REACH)], axis=0
            ).astype(low)
            crop = jnp.dot(weights, window, preferred_element_type=f32)
            stage[pl.ds(p, ROWS_PAD, stride=GROUP), :] = crop
        group_rows = rows(core * capacity + g * GROUP, GROUP)
        for m in range(feats // 128):
            crops[group_rows, m * 128 : (m + 1) * 128] = stage[
                m * GROUP : (m + 1) * GROUP, :
            ].astype(low)

        @pl.when(g > 0)
        def _():
            crop_copy((g - 1) * GROUP, GROUP).start()

        return carry

    lax.fori_loop(0, groups, crop_group, 0)
    crop_copy((groups - 1) * GROUP, GROUP).start()

    def hide(ahead, route, begun):
        t = y if ahead == 0 else 1 - y
        first, count = parts_in[route]
        from_at = (starts[0] + t * (starts[1] - starts[0]) + first) * 128
        part = lax.dot_general(
            wbuf[rows(t * all_rows, all_rows), first * 128 : (first + count) * 128],
            crops[:, pl.ds(pl.multiple_of(from_at, 128), count * 128)],
            NT,
            preferred_element_type=f32,
        )
        hidden[...] = hidden[...] + part if begun else part

    def make_back(ahead):
        t = y if ahead == 0 else 1 - y
        part = jnp.dot(
            upb[...], w2buf[rows(t * hidden_size, hidden_size), :], preferred_element_type=f32
        )
        back[rows(t * depth, depth), :] = part.T

    ends = {
        (rel[2], route if route < last_in else -1): i for i, (route, rel) in enumerate(events)
    }
    ready = [(i, key) for key, i in ends.items()]
    passed = len(own) + EARLY + DURING
    waited, begun = False, False
    for i in range(passed - 1, len(events)):
        if i >= passed:
            gather(events[i])
        for key in [k for end, k in sorted(ready) if end == i or (i == passed - 1 and end < i)]:
            if key[1] < 0:
                make_back(key[0])
                continue
            if not waited:
                waited = True
                crop_copy(0, capacity).wait()
            hide(*key, begun)
            begun = True
    def gelu(i, carry):
        at = rows(i * 32, 32)
        value, slope = gelu_parts(hidden[at, :])
        acts[at, :] = value.astype(low)
        pres[at, :] = (back[at, :] * slope).astype(low)
        return carry

    lax.fori_loop(0, hidden.shape[0] // 32, gelu, 0)

    def sum_ref(route):
        if route >= last_out:
            return lambda q: seconds.at[
                rows(q[2] * hidden_size + (q[0] * nx + q[1]) * pair, pair),
                pl.ds((route - last_out) * cols_out, cols_out),
            ]
        first, count = parts_out[route]
        return lambda q: grads.at[
            rows(q[2] * all_rows + (q[0] * nx + q[1]) * h, h), pl.ds(first * 128, count * 128)
        ]

    def add(ref, more):
        def one(i, carry):
            at = rows(i * 16, 16)
            ref[at, :] = (ref[at, :].astype(f32) + more[at, :].astype(f32)).astype(low)
            return carry

        lax.fori_loop(0, ref.shape[0] // 16, one, 0)

    def make_grads(t, part):
        first, count = parts_out[part]
        step = max(c for c in range(1, 7) if count % c == 0)

        def one(i, carry):
            at = pl.multiple_of((first + i * step) * 128, 128)
            from_at = pl.multiple_of((starts[0] + t * (starts[1] - starts[0])) * 128 + at, 128)
            grads[rows(t * all_rows, all_rows), pl.ds(at, step * 128)] = jnp.dot(
                pres[...], crops[:, pl.ds(from_at, step * 128)], preferred_element_type=f32
            ).astype(low)
            return carry

        lax.fori_loop(0, count // step, one, 0)

    def make_seconds():
        for t in range(ny):
            seconds[t * hidden_size : (t + 1) * hidden_size, :] = lax.dot_general(
                uptb[...], acts[t * depth : (t + 1) * depth, :], NT, preferred_element_type=f32
            ).astype(low)

    own_second = y * hidden_size + chip * pair
    made, ended, outs, swapped = set(), set(), [], False
    for route, rel in sum_events:
        need = (route, rel[2]) if route < last_out else last_out
        if need not in made:
            made.add(need)
            if route >= last_out:
                make_seconds()
            else:
                make_grads(y if rel[2] == 0 else 1 - y, route)
        ways_out.scatter(
            route, rel, sum_ref(route), slot_refs[route], add, sum_send_sems, sum_recv_sems
        )
        if rel != (0, 0, 0):
            continue
        ended.add(route)
        if route < last_out:
            first, count = parts_out[route]
            at = pl.ds(first * 128, count * 128)
            outs.append(local(grads.at[own_rows, at], first_ref.at[:, at], len(outs)))
        if not swapped and all(r in ended for r in range(last_out, len(SCATTER_ORDERS))):
            swapped = True
            swap[0] = seconds[pl.ds(pl.multiple_of(own_second + other * h, h), h), :]
            second_swap = remote(swap.at[0], swap.at[1], 5, partner)
            second_swap.start()
            mine = seconds.at[pl.ds(pl.multiple_of(own_second + core * h, h), h), :]
            outs.append(local(mine, second_ref.at[core], len(outs)))

    def whole(route, buf, other_buf, parts, last, cols):
        if route >= last:
            return lambda n: other_buf.at[pl.ds(0, n), pl.ds((route - last) * cols, cols)]
        first, count = parts[route]
        return lambda n: buf.at[pl.ds(0, n), pl.ds(first * 128, count * 128)]

    for route in range(len(GATHER_ORDERS)):
        unit = pair if route >= last_in else h
        part = whole(route, wbuf, w2buf, parts_in, last_in, cols_in)
        ways_in.drain(route, part, unit, send_sems)
    for route in range(len(SCATTER_ORDERS)):
        unit = pair if route >= last_out else h
        part = whole(route, grads, seconds, parts_out, last_out, cols_out)
        sent = part((nz * nx * ny - 1) * unit)
        pltpu.make_async_copy(sent, sent, sum_send_sems.at[route]).wait()

    @pl.when(y == 1)
    def _():
        fine_halo.wait_send()
        coarse_halo.wait_send()

    second_swap.wait()
    outs.append(local(swap.at[1], second_ref.at[other], len(outs)))
    for copy in outs:
        copy.wait()


def finish_kernel(
    shift, sums_ref, sets_ref, first_ref, second_ref, sums, sets, first, second, come, gone
):
    y = lax.axis_index("tile")
    h, share = first_ref.shape
    depth = sets_ref.shape[2]
    bins = sums_ref.shape[1] // 128
    f32 = jnp.float32
    chunks = come.shape[0] - 1
    size = h // chunks
    halves = lax.broadcasted_iota(jnp.int32, (size, 128), 1)
    whole = lax.broadcasted_iota(jnp.int32, (h, 128), 1)
    back_shift = (128 - shift) % 128
    parts = [slice(c * size, (c + 1) * size) for c in range(chunks)]
    loads = [
        pltpu.make_async_copy(sums_ref.at[part, :], sums.at[part, :], come.at[c])
        for c, part in enumerate(parts)
    ]
    loads.append(pltpu.make_async_copy(sets_ref, sets, come.at[chunks]))
    for copy in loads:
        copy.start()
    stores = []
    for c, part in enumerate(parts):
        loads[c].wait()

        def turned(i, part=part):
            tile = sums[part, 128 * i : 128 * (i + 1)].astype(f32)
            return tile, pltpu.roll(tile, back_shift, axis=1)

        now = turned(0)
        for i in range(bins):
            width = min(128, share - 128 * i)
            following = turned(i + 1) if i + 1 < bins else now
            late = jnp.where(halves < 128 - shift, now[1], following[1])
            first[part, 128 * i : 128 * i + width] = jnp.where(y == 0, now[0], late)[:, :width]
            now = following
        stores.append(pltpu.make_async_copy(first.at[part, :], first_ref.at[part, :], gone.at[c]))
        stores[-1].start()
    loads[chunks].wait()
    for m in range(depth // 128):
        at = slice(128 * m, 128 * (m + 1))
        set_0 = sets[0, :, at].astype(f32)
        set_1 = sets[1, :, at].astype(f32)
        second[:, 256 * m : 256 * m + 128] = jnp.where(
            whole < h, set_0, pltpu.roll(set_1, h, axis=1)
        )
        second[:, 256 * m + 128 : 256 * m + 256] = jnp.where(
            whole < h, pltpu.roll(set_0, h, axis=1), set_1
        )
    stores.append(pltpu.make_async_copy(second, second_ref, gone.at[chunks]))
    stores[-1].start()
    for copy in stores:
        copy.wait()


def per_device_by_chips(
    grid, proposal_boxes, level_plan, fine_map, coarse_map, first_weight, second_weight, upstream
):
    nz, nx, ny, cores = grid
    chips = nz * nx
    props = level_plan.shape[1]
    capacity = props // ny
    fine_tile, coarse = fine_map[0], coarse_map[0]
    fine_rows, fine_cols, channels = fine_tile.shape
    coarse_rows = coarse.shape[0]
    share, h = first_weight.shape
    feats = share * ny
    bins = max(-(-((t + 1) * share) // 128) - t * share // 128 for t in range(ny))
    lanes = bins * 128
    hidden_size = upstream.shape[2]
    depth = second_weight.shape[0] // cores
    pair = cores * h
    low, f32 = jnp.bfloat16, jnp.float32
    sizes = (nz, nx, ny)
    parts_out = cut(bins, SCATTER_SHARES)
    slot_counts = [sum(slots_of(sizes, order)) for order in SCATTER_ORDERS]
    rows_all = chips * h
    batch = cores * capacity
    q = chips * ny
    dma = pltpu.SemaphoreType.DMA
    anywhere = pl.BlockSpec(memory_space=pl.ANY)
    vmem = pl.BlockSpec(memory_space=pltpu.VMEM)
    slot_shapes = [
        (n, h, parts_out[i][1] * 128)
        if i < len(parts_out)
        else (n, pair, depth // (len(SCATTER_ORDERS) - len(parts_out)))
        for i, n in enumerate(slot_counts)
    ]
    sums, sets = pl.pallas_call(
        functools.partial(step_kernel, grid),
        out_shape=(
            jax.ShapeDtypeStruct((h, lanes), low),
            jax.ShapeDtypeStruct((cores, h, depth), low),
        ),
        in_specs=[vmem, vmem] + [anywhere] * 5,
        out_specs=(anywhere, anywhere),
        scratch_shapes=[
            pltpu.VMEM((h, share), low),
            pltpu.VMEM((h, cores * depth), low),
            pltpu.VMEM((cores, h, depth), low),
            pltpu.VMEM((ny * rows_all, lanes), low),
            pltpu.VMEM((ny * hidden_size, depth), low),
            pltpu.VMEM((fine_rows + HALO, fine_cols, channels), low),
            pltpu.VMEM((coarse_rows + HALO, coarse.shape[1], channels), low),
            pltpu.VMEM((fine_rows + coarse_rows + 2 * HALO, fine_cols, channels), f32),
            pltpu.VMEM((ROWS_PAD * GROUP, 128), f32),
            pltpu.VMEM((batch, feats), low),
            pltpu.VMEM((props, hidden_size), low),
            pltpu.VMEM((batch, hidden_size), low),
            pltpu.VMEM((hidden_size, batch), low),
            pltpu.VMEM((rows_all, batch), f32),
            pltpu.VMEM((rows_all, batch), f32),
            pltpu.VMEM((rows_all, batch), low),
            pltpu.VMEM((rows_all, batch), low),
            pltpu.VMEM((ny * rows_all, lanes), low),
            pltpu.VMEM((ny * hidden_size, depth), low),
            pltpu.VMEM((2, h, depth), low),
            pltpu.VMEM((8, capacity), jnp.int32),
            pltpu.VMEM((8, capacity), f32),
            pltpu.SMEM((8, capacity), jnp.int32),
            pltpu.SMEM((8, capacity), f32),
            dma((max(7, len(SCATTER_ORDERS) + 2),)),
            dma((len(GATHER_ORDERS), 4)),
            dma((len(GATHER_ORDERS), q)),
            dma((len(SCATTER_ORDERS),)),
            dma((sum(slot_counts),)),
            dma((6,)),
            dma((6,)),
        ]
        + [pltpu.VMEM(shape, low) for shape in slot_shapes],
        compiler_params=pltpu.CompilerParams(
            collective_id=0, has_side_effects=True, vmem_limit_bytes=64000 * 1024
        ),
        name="step",
    )(
        proposal_boxes[0],
        level_plan,
        first_weight.T,
        second_weight.T,
        upstream[0],
        fine_tile,
        coarse,
    )
    shift = share - 128 * min(share // 128, feats // 128 - bins)
    first, second = pl.pallas_call(
        functools.partial(finish_kernel, shift),
        out_shape=(
            jax.ShapeDtypeStruct((h, share), f32),
            jax.ShapeDtypeStruct((h, cores * depth), f32),
        ),
        in_specs=[anywhere, anywhere],
        out_specs=(anywhere, anywhere),
        scratch_shapes=[
            pltpu.VMEM((h, lanes), low),
            pltpu.VMEM((cores, h, depth), low),
            pltpu.VMEM((h, share), f32),
            pltpu.VMEM((h, cores * depth), f32),
            dma((h // 16 + 1,)),
            dma((h // 16 + 1,)),
        ],
        name="finish",
    )(sums, sets)
    return (first.T, second.T)


def solution(mesh):
    placed = (
        P("dp", None, None),
        P("dp", None),
        P("dp", "tile", None, None),
        P("dp", "tile", None, None),
        P("tile", "dp"),
        P("tile", "dp"),
        P("dp", None, None),
    )
    grid = chip_grid(mesh)
    tiles = mesh.shape["tile"]
    body = per_device_by_bands
    if grid is not None and tiles == 2 and grid[1] <= 2 and grid[2] == 2:
        body = functools.partial(per_device_by_chips, (grid[0], grid[1], tiles, grid[2]))
    return jax.shard_map(
        body,
        mesh=mesh,
        in_specs=placed,
        out_specs=(P("tile", "dp"), P("tile", "dp")),
        check_vma=False,
    )
```
